32 devices in a mesh: wide: 8 (over y, x, core), tp: 4 (over z).
Axes of the slice: x: 2, y: 2, z: 4, core: 2. Of those that a mesh axis runs over, the one named last changes fastest.
Arguments:
- tokens: bfloat16 [16384, 1536], P(('wide', 'tp')), may hold values from -6 to 6
- segment_ids: int32 [16384], P('wide'), may hold values from 0 to 15, never falling along the last dimension, each value on 1 to 2048 neighbouring positions
- out_cotangent: bfloat16 [16384, 1536], P(('wide', 'tp')), may hold values from -6 to 6
- norm_gain: bfloat16 [1536], replicated, may hold values from 0.5 to 1.5
- z_weight: bfloat16 [1536, 3072], P('wide', 'tp'), may hold values from -0.15625 to 0.15625
- x_weight: bfloat16 [1536, 3072], P('wide', 'tp'), may hold values from -0.15625 to 0.15625
- bc_weight: bfloat16 [1536, 256], P('wide', 'tp'), may hold values from -0.15625 to 0.15625
- dt_weight: bfloat16 [1536, 48], P('wide', 'tp'), may hold values from -0.15625 to 0.15625
- x_conv: bfloat16 [4, 3072], replicated, may hold values from -3 to 3
- x_bias: bfloat16 [3072], replicated, may hold values from -3 to 3
- bc_conv: bfloat16 [4, 256], replicated, may hold values from -3 to 3
- bc_bias: bfloat16 [256], replicated, may hold values from -3 to 3
- dt_bias: bfloat16 [48], replicated, may hold values from -6 to -2
- decay_log: bfloat16 [48], replicated, may hold values from -1 to 2
- skip_gain: bfloat16 [48], replicated, may hold values from 0.5 to 1.5
- gate_gain: bfloat16 [3072], replicated, may hold values from 0.5 to 1.5
- out_weight: bfloat16 [3072, 1536], P('tp', 'wide'), may hold values from -0.109375 to 0.109375
Outputs:
- block_out: bfloat16 [16384, 1536], P(('wide', 'tp'))
- grad_x: float32 [16384, 1536], P(('wide', 'tp'))
- norm_gain_grad: float32 [1536], replicated
- z_weight_grad: float32 [1536, 3072], P('wide', 'tp')
- x_weight_grad: float32 [1536, 3072], P('wide', 'tp')
- bc_weight_grad: float32 [1536, 256], P('wide', 'tp')
- dt_weight_grad: float32 [1536, 48], P('wide', 'tp')
- x_conv_grad: float32 [4, 3072], replicated
- x_bias_grad: float32 [3072], replicated
- bc_conv_grad: float32 [4, 256], replicated
- bc_bias_grad: float32 [256], replicated
- dt_bias_grad: float32 [48], replicated
- decay_log_grad: float32 [48], replicated
- skip_gain_grad: float32 [48], replicated
- gate_gain_grad: float32 [3072], replicated
- out_weight_grad: float32 [3072, 1536], P('tp', 'wide')
The draws below stay inside these ranges and needn't reach their ends.
Inputs may be any that keep to these rules, and one draw needn't show every extreme that they name: `segment_ids`: segment numbers never fall along the stream; each segment holds at most 2048 tokens, and one holds exactly 2048.
All inputs are finite; a program needn't handle non-finite values.
Results may differ from the reference program's by a relative error of at most 0.023.
Values may be sent and summed in bfloat16 or wider, within the bound.
A program may use at most 192 MiB of HBM per device.

```python
import math
import jax
import jax.numpy as jnp
import numpy as np
from jax import lax

D = 1536
HEADS = 48
HEAD_DIM = 64
STATE = 128
CONV = 4
GROUP = 256
DOC_MAX = 2048
INNER = 3072
TOKENS = 16384


def block_scale(stream_key, extent, pieces, least, high):
    loudness = 1.0
    for axis_at, blocks in pieces:
        draws = jax.random.uniform(jax.random.fold_in(jax.random.fold_in(stream_key, 6), axis_at), (blocks,), jnp.float32, least / len(pieces), high / len(pieces))
        loudness = loudness * jnp.repeat(jnp.exp(draws), extent[axis_at] // blocks).reshape((-1,) + (1,) * (len(extent) - 1 - axis_at))
    return loudness


def split_up(number_of, total, most, slope):
    weights = [(1 << 20) // math.isqrt(grade ** slope) + 1 for grade in range(2, number_of + 1)]
    spare, counts = total - most - (number_of - 1), [1] * (number_of - 1)
    while spare > 0:
        movable = [i for i in range(number_of - 1) if counts[i] < most]
        whole, budget = sum([weights[i] for i in movable]), spare
        for i in movable:
            addition = min(most - counts[i], max(1, budget * weights[i] // whole), spare)
            counts[i] = counts[i] + addition
            spare = spare - addition
    return np.array([most] + counts)


def uneven_parts(own_key, amount, total, limit, lean):
    if amount == 2:
        one = jax.random.randint(own_key, (), max(1, total - limit), min(limit, total - 1) + 1)
        return jnp.stack([one, total - one])
    sizes = jnp.asarray(split_up(amount, total, limit, lean), jnp.int32)
    pairs = (amount - 1) // 2
    giver, receiver = sizes[1:1 + 2 * pairs:2], sizes[2:2 + 2 * pairs:2]
    room = jnp.minimum(giver - 1, limit - receiver)
    shifted = jax.random.randint(jax.random.fold_in(own_key, 1), (pairs,), 0, 1 << 20) % (room + 1)
    sizes = sizes.at[1:1 + 2 * pairs:2].set(giver - shifted).at[2:2 + 2 * pairs:2].set(receiver + shifted)
    return sizes[jax.random.permutation(jax.random.fold_in(own_key, 2), amount)]


def centred(rng, dims, scale, limit, pieces=(), kind=jnp.bfloat16):
    entries = scale * jax.random.normal(rng, dims, jnp.float32)
    if pieces:
        entries = entries * block_scale(rng, dims, pieces, -0.22, 0.18)
    return jnp.clip(entries, -limit, limit).astype(kind)


def setup_inputs(seed: int = 0) -> dict:
    key_of = jax.random.split(jax.random.key(seed), 18)
    tokens = centred(key_of[0], (TOKENS, D), 1.0, 6.0, ((0, 32),))
    segment_ids = jnp.searchsorted(jnp.cumsum(uneven_parts(key_of[1], TOKENS // (DOC_MAX // 2), TOKENS, DOC_MAX, 0)), jnp.arange(TOKENS), side="right").astype(jnp.int32)
    out_cotangent = centred(key_of[2], (TOKENS, D), 1.0, 6.0, ((0, 32),))
    norm_gain = jnp.clip(1.0 + 0.1 * jax.random.normal(key_of[3], (D,), jnp.float32), 0.5, 1.5).astype(jnp.bfloat16)
    z_weight = centred(key_of[4], (D, INNER), D ** -0.5, 0.15625, ((0, 8), (1, 4)))
    x_weight = centred(key_of[5], (D, INNER), D ** -0.5, 0.15625, ((0, 8), (1, 4)))
    bc_weight = centred(key_of[6], (D, 2 * STATE), D ** -0.5, 0.15625, ((0, 8), (1, 4)))
    dt_weight = centred(key_of[7], (D, HEADS), D ** -0.5, 0.15625, ((0, 8), (1, 4)))
    x_conv = centred(key_of[8], (CONV, INNER), CONV ** -0.5, 3.0)
    x_bias = centred(key_of[9], (INNER,), 0.5, 3.0)
    bc_conv = centred(key_of[10], (CONV, 2 * STATE), CONV ** -0.5, 3.0)
    bc_bias = centred(key_of[11], (2 * STATE,), 0.5, 3.0)
    dt_bias = jnp.clip(jax.random.uniform(key_of[12], (HEADS,), jnp.float32, -6.0, -2.0), -6.0, -2.0).astype(jnp.bfloat16)
    decay_log = jnp.clip(jax.random.uniform(key_of[13], (HEADS,), jnp.float32, -1.0, 2.0), -1.0, 2.0).astype(jnp.bfloat16)
    skip_gain = jnp.clip(jax.random.uniform(key_of[14], (HEADS,), jnp.float32, 0.5, 1.5), 0.5, 1.5).astype(jnp.bfloat16)
    gate_gain = jnp.clip(1.0 + 0.1 * jax.random.normal(key_of[15], (INNER,), jnp.float32), 0.5, 1.5).astype(jnp.bfloat16)
    out_weight = centred(key_of[16], (INNER, D), INNER ** -0.5, 0.109375, ((0, 4), (1, 8)))
    return dict(tokens=tokens, segment_ids=segment_ids, out_cotangent=out_cotangent, norm_gain=norm_gain, z_weight=z_weight, x_weight=x_weight, bc_weight=bc_weight, dt_weight=dt_weight, x_conv=x_conv, x_bias=x_bias, bc_conv=bc_conv, bc_bias=bc_bias, dt_bias=dt_bias, decay_log=decay_log, skip_gain=skip_gain, gate_gain=gate_gain, out_weight=out_weight)


@jax.custom_vjp
def low(v):
    return lax.optimization_barrier(v.astype(jnp.bfloat16)).astype(jnp.float32)

@jax.custom_vjp
def low_back(v):
    return v

def low_keep(v):
    return (low(v), None)

def low_pass(kept, grad):
    return (grad,)

def back_keep(v):
    return (v, None)

def back_low(kept, grad):
    return (low(grad),)
low.defvjp(low_keep, low_pass)
low_back.defvjp(back_keep, back_low)
EPS = 1e-05
HIGH = lax.Precision.HIGHEST

def matmul(left, right):
    return jnp.dot(left, right, precision=HIGH)

def rms_norm(values, gain):
    return values * lax.rsqrt(lax.optimization_barrier(jnp.mean(values * values, axis=-1, keepdims=True)) + EPS) * gain

def causal_conv(values, rim, segments, rim_segments, weight, bias):
    extended = jnp.concatenate([rim, values], axis=0)
    ext_segments = jnp.concatenate([rim_segments, segments], axis=0)
    length = values.shape[0]
    total = jnp.zeros_like(values) + bias[None, :]
    for lag in range(CONV):
        offset = CONV - 1 - lag
        same = (ext_segments[offset:offset + length] == segments).astype(jnp.float32)
        total = total + weight[lag][None, :] * extended[offset:offset + length] * same[:, None]
    return total

def group_state(signal, bmat, step, rate, segments, before):
    cumulative = jnp.cumsum(rate, axis=0)
    inputs = signal * step[:, :, None]
    keep_last = (segments == segments[-1]).astype(jnp.float32)
    weights = jnp.exp(cumulative[-1][None, :] - cumulative) * keep_last[:, None]
    factor = jnp.exp(cumulative[-1]) * (segments[-1] == before).astype(jnp.float32)
    contribution = jnp.einsum('jh,jhp,jn->hpn', weights, inputs, bmat, precision=HIGH)
    return (factor, contribution)

def group_output(signal, bmat, cmat, step, rate, state, segments, before):
    length = segments.shape[0]
    cumulative = jnp.cumsum(rate, axis=0)
    position = jnp.arange(length)
    within = ((segments[:, None] == segments[None, :]) & (position[None, :] <= position[:, None])).astype(jnp.float32)
    gaps = cumulative[:, None, :] - cumulative[None, :, :]
    decays = jnp.exp(jnp.where(within[:, :, None] > 0, gaps, 0.0)) * within[:, :, None]
    scores = jnp.dot(cmat, bmat.T, precision=HIGH)
    inputs = signal * step[:, :, None]
    result = jnp.einsum('ijh,jhp->ihp', scores[:, :, None] * decays, inputs, precision=HIGH)
    entering = jnp.exp(cumulative) * (segments == before).astype(jnp.float32)[:, None]
    result = result + jnp.einsum('in,hpn->ihp', cmat, state, precision=HIGH) * entering[:, :, None]
    factor, contribution = group_state(signal, bmat, step, rate, segments, before)
    return (result, factor[:, None, None] * state + contribution)

def layer(params, segment_ids):
    tokens, norm_gain, z_weight, x_weight, bc_weight, dt_weight, x_conv, x_bias, bc_conv, bc_bias, dt_bias, decay_log, skip_gain, gate_gain, out_weight = params
    rows = math.gcd(TOKENS, 4096)
    blocks = TOKENS // rows
    groups = rows // GROUP
    padded_ids = jnp.concatenate([jnp.full((CONV - 1,), -1, jnp.int32), segment_ids.astype(jnp.int32)])
    offsets = (jnp.arange(blocks)[:, None] * rows + jnp.arange(CONV - 1)[None, :]).astype(jnp.int32)
    rim_ids = padded_ids[offsets]

    def group_step(state, item):
        signal, bmat, cmat, step, rate, segments, before = item
        result, new_state = group_output(signal, bmat, cmat, step, rate, state, segments, before)
        return (new_state, result)

    def block(carry, item):
        state, rim_x, rim_bc = carry
        rows_in, segments, rim_segments = item
        normed = low(rms_norm(rows_in, norm_gain))
        gate_z = low(low_back(matmul(normed, z_weight)))
        x_raw = low(low_back(matmul(normed, x_weight)))
        bc_raw = low(low_back(matmul(normed, bc_weight)))
        dt_raw = low(low_back(matmul(normed, dt_weight)))
        signal = low(jax.nn.silu(causal_conv(x_raw, rim_x, segments, rim_segments, x_conv, x_bias)))
        bc_act = low(jax.nn.silu(causal_conv(bc_raw, rim_bc, segments, rim_segments, bc_conv, bc_bias)))
        step = jax.nn.softplus(dt_raw + dt_bias[None, :])
        rate = -jnp.exp(decay_log)[None, :] * step
        befores = jnp.concatenate([rim_segments[CONV - 2:], segments[GROUP - 1::GROUP][:-1]])
        items = (signal.reshape(groups, GROUP, HEADS, HEAD_DIM), bc_act[:, :STATE].reshape(groups, GROUP, STATE), bc_act[:, STATE:].reshape(groups, GROUP, STATE), step.reshape(groups, GROUP, HEADS), rate.reshape(groups, GROUP, HEADS), segments.reshape(groups, GROUP), befores)
        state, results = lax.scan(jax.checkpoint(group_step), state, items)
        heads_out = results.reshape(rows, HEADS, HEAD_DIM) + skip_gain[None, :, None] * signal.reshape(rows, HEADS, HEAD_DIM)
        gated = heads_out.reshape(rows, INNER) * jax.nn.silu(gate_z)
        normed_out = low(rms_norm(gated, gate_gain))
        result = rows_in + matmul(normed_out, out_weight)
        return ((state, x_raw[rows - CONV + 1:], bc_raw[rows - CONV + 1:]), result)
    start = (jnp.zeros((HEADS, HEAD_DIM, STATE), jnp.float32), jnp.zeros((CONV - 1, INNER), jnp.float32), jnp.zeros((CONV - 1, 2 * STATE), jnp.float32))
    final, outputs = lax.scan(jax.checkpoint(block), start, (tokens.reshape(blocks, rows, D), segment_ids.reshape(blocks, rows), rim_ids))
    return outputs.reshape(TOKENS, D)

def reference(tokens, segment_ids, out_cotangent, norm_gain, z_weight, x_weight, bc_weight, dt_weight, x_conv, x_bias, bc_conv, bc_bias, dt_bias, decay_log, skip_gain, gate_gain, out_weight):
    params = tuple((a.astype(jnp.float32) for a in (tokens, norm_gain, z_weight, x_weight, bc_weight, dt_weight, x_conv, x_bias, bc_conv, bc_bias, dt_bias, decay_log, skip_gain, gate_gain, out_weight)))

    def forward(*arrays):
        return layer(arrays, segment_ids)
    result, pull = jax.vjp(forward, *params)
    grads = pull(out_cotangent.astype(jnp.float32))
    return (result.astype(jnp.bfloat16), grads[0], grads[1], grads[2], grads[3], grads[4], grads[5], grads[6], grads[7], grads[8], grads[9], grads[10], grads[11], grads[12], grads[13], grads[14])
```

```python
import functools

import jax
import jax.numpy as jnp
from jax import lax
from jax.experimental import pallas as pl
from jax.experimental.pallas import tpu as pltpu
from jax.sharding import PartitionSpec as P

HEADS = 48
HEAD_DIM = 64
STATE = 128
CONV = 4
INNER = 3072
DOC_MAX = 2048
EPS = 1e-05
HALO = 16
Q = 128
LANES = 256
GROUP_HEADS = LANES // HEAD_DIM
F32 = jnp.float32
BF = jnp.bfloat16
HIGH = lax.Precision.HIGHEST
NN = ((1,), (0,))
NT = ((1,), (1,))
TN = ((0,), (0,))
SDS = jax.ShapeDtypeStruct


def mm(a, b, dims=NN, precision=None):
    return lax.dot_general(a, b, (dims, ((), ())), precision=precision, preferred_element_type=F32)


def sigmoid(v):
    return 1.0 / (1.0 + jnp.exp(-v))


def iota(shape, axis):
    return lax.broadcasted_iota(jnp.int32, shape, axis)


def params(vmem_mb=60, **kw):
    return pltpu.CompilerParams(vmem_limit_bytes=vmem_mb * 1024 * 1024, **kw)


def cost(flops, read):
    return pl.CostEstimate(flops=int(flops), bytes_accessed=int(read), transcendentals=0)


def proj_kernel(tok, gain, weight, x_out, misc_out, normed):
    @pl.when(pl.program_id(0) == 0)
    def _():
        raw = tok[...].astype(F32)
        inv = lax.rsqrt(jnp.mean(raw * raw, axis=-1, keepdims=True) + EPS)
        normed[...] = (raw * inv * gain[...]).astype(BF)

    depth, cols = tok.shape[1], weight.shape[3]
    result = mm(normed[...], weight[...].reshape(depth, cols))
    block = x_out.shape[1]
    x_out[...] = result[:, :block].astype(BF)
    misc_out[0] = result[:, block:].astype(BF)


def project(tokens_ext, gain, weights):
    rows, depth = tokens_ext.shape
    nw, nt, k, cols = weights.shape
    block = INNER // nt
    misc = cols - block
    return pl.pallas_call(
        proj_kernel,
        grid=(nt,),
        in_specs=[
            pl.BlockSpec((rows, depth), lambda t: (0, 0)),
            pl.BlockSpec((1, depth), lambda t: (0, 0)),
            pl.BlockSpec((nw, 1, k, cols), lambda t: (0, t, 0, 0)),
        ],
        out_specs=[
            pl.BlockSpec((rows, block), lambda t: (0, t)),
            pl.BlockSpec((1, rows, misc), lambda t: (t, 0, 0)),
            pl.BlockSpec((rows, depth), lambda t: (0, 0)),
        ],
        out_shape=[
            SDS((rows, INNER), BF),
            SDS((nt, rows, misc), BF),
            SDS((rows, depth), BF),
        ],
        compiler_params=params(),
        cost_estimate=cost(2 * rows * depth * nt * cols, 2 * depth * nt * cols),
        name="project",
    )(tokens_ext, gain, weights)


def plain_kernel(left, weight, out):
    depth, cols = left.shape[1], weight.shape[3]
    out[...] = mm(left[...], weight[...].reshape(depth, cols)).astype(BF)


def plain(left, weights, which, name):
    rows, depth = left.shape
    nw, nt, k, _ = weights.shape
    block = INNER // nt
    return pl.pallas_call(
        plain_kernel,
        grid=(nt,),
        in_specs=[
            pl.BlockSpec((rows, depth), lambda t: (0, 0)),
            pl.BlockSpec((nw, 1, k, block), lambda t: (0, t, 0, which)),
        ],
        out_specs=pl.BlockSpec((rows, block), lambda t: (0, t)),
        out_shape=SDS((rows, INNER), BF),
        compiler_params=params(),
        cost_estimate=cost(2 * rows * depth * INNER, 2 * depth * INNER),
        name=name,
    )(left, weights)


def select_columns(t, heads, bc_cols, rows, cols):
    lane, col = iota((rows, cols), 0), iota((rows, cols), 1)
    first = (lane < bc_cols) & (col == lane + t * bc_cols)
    second = (
        (lane >= bc_cols)
        & (lane < bc_cols + heads)
        & (col == lane - bc_cols + 2 * STATE + t * heads)
    )
    return jnp.where(first | second, 1.0, 0.0).astype(BF)


def conv_of(ext, taps, bias, info):
    total = bias + taps[0:1] * ext[HALO:]
    for k in range(1, CONV):
        total = total + taps[k : k + 1] * pltpu.roll(ext, k, 0)[HALO:] * info[:, k - 1 : k]
    return total


def head_lanes(group, lanes):
    return jnp.where(
        iota((128, lanes), 0) == group * GROUP_HEADS + iota((128, lanes), 1) // HEAD_DIM, 1.0, 0.0
    ).astype(BF)


def expand(values, selection):
    high = values.astype(BF)
    low = (values - high.astype(F32)).astype(BF)
    return mm(high, selection) + mm(low, selection)


def prepare(misc, info, row_ids, bc_taps, bc_bias, dt_bias, decay, bcu, bc, bt, ct, scores, pre, step, rate, cum, cum_t, enter, leave, factor):
    nt, rows_ext, width = misc.shape
    rows = rows_ext - HALO
    chunks = rows // Q
    bc_cols, heads = 2 * STATE // nt, HEADS // nt
    total = None
    for t in range(nt):
        part = mm(misc[t], select_columns(t, heads, bc_cols, width, 2 * STATE + 128))
        total = part if total is None else total + part
    marks = info[...]
    bc_ext = total[:, : 2 * STATE]
    u = conv_of(bc_ext, bc_taps[...], bc_bias[...], marks)
    if bcu is not None:
        bcu[...] = bc_ext
    act = (u * sigmoid(u)).astype(BF)
    bc[...] = act
    before = total[HALO:, 2 * STATE :] + dt_bias[...]
    steps = jnp.maximum(before, 0.0) + jnp.log1p(jnp.exp(-jnp.abs(before)))
    rates = -jnp.exp(decay[...]) * steps
    rates = jnp.where(iota(rates.shape, 1) < HEADS, rates, 0.0)
    if pre is not None:
        pre[...] = before
        rate[...] = rates
    step[...] = steps
    upper = iota((Q, Q), 0) >= iota((Q, Q), 1)
    lower = jnp.where(upper, 1.0, 0.0)
    for c in range(chunks):
        at = slice(c * Q, (c + 1) * Q)
        sums = mm(lower, rates[at], NN, HIGH)
        cum[at] = sums
        cum_t[c] = sums.T
        last = sums[Q - 1 : Q]
        enter[at] = jnp.exp(sums) * marks[at, 4:5]
        leave[at] = jnp.exp(last - sums) * marks[at, 5:6]
        factor[c : c + 1] = jnp.exp(last) * marks[c * Q : c * Q + 1, 7:8]
        bb, cc = act[at, :STATE], act[at, STATE:]
        within = upper & (marks[at, 3:4] == row_ids[0:1, at])
        scores[c] = jnp.where(within, mm(cc, bb, NT), 0.0)
        bt[c] = bb.T
        if ct is not None:
            ct[c] = cc.T


def decay_of(turned, cum_t, c, group, k):
    row = cum_t[c, pl.ds(group * GROUP_HEADS + k, 1), :]
    return jnp.exp(jnp.minimum(turned[:, k : k + 1] - row, 0.0))


def turned_sums(cum, at, group):
    return pltpu.roll(cum[at], (128 - group * GROUP_HEADS) % 128, 1)


def halves(pair):
    left = iota(pair.shape, 1) < HEAD_DIM
    zero = jnp.zeros_like(pair)
    return jnp.concatenate([jnp.where(left, pair, zero), jnp.where(left, zero, pair)], axis=0)


def ssd_kernel(x, misc, info, row_ids, taps, bias, bc_taps, bc_bias, dt_bias, decay, signal, y, state, ent, bc_out, bt, scores, step, cum, cum_t, enter, leave, factor):
    group = pl.program_id(0)
    rows = signal.shape[0]
    chunks = rows // Q

    @pl.when(group == 0)
    def _():
        factor[...] = jnp.zeros_like(factor)
        prepare(misc, info, row_ids, bc_taps, bc_bias, dt_bias, decay, None, bc_out, bt, None, scores, None, step, None, cum, cum_t, enter, leave, factor)
        base = jnp.zeros((1, 128), F32)
        for c in range(chunks):
            at = slice(c * Q, (c + 1) * Q)
            ent[at] = jnp.exp(cum[at] + base) * info[at, 6:7]
            base = base + cum[c * Q + Q - 1 : c * Q + Q]

    u = conv_of(x[...].astype(F32), taps[...], bias[...], info[...])
    act = (u * sigmoid(u)).astype(BF)
    signal[...] = act
    pick = head_lanes(group, LANES)
    inputs = act.astype(F32) * expand(step[...], pick)
    inputs_b = inputs.astype(BF)
    weighted = (inputs * expand(leave[...], pick)).astype(BF)
    entering = expand(enter[...], pick)
    factors = expand(factor[...], pick)
    now = jnp.zeros((STATE, LANES), F32)
    whole = jnp.ones((1, LANES), F32)
    for c in range(chunks):
        at = slice(c * Q, (c + 1) * Q)
        turned = turned_sums(cum, at, group)
        pieces = []
        for p in range(LANES // 128):
            ma = (scores[c] * decay_of(turned, cum_t, c, group, 2 * p)).astype(BF)
            mb = (scores[c] * decay_of(turned, cum_t, c, group, 2 * p + 1)).astype(BF)
            pieces.append(mm(jnp.concatenate([ma, mb], axis=1), halves(inputs_b[at, p * 128 : p * 128 + 128])))
        result = jnp.concatenate(pieces, axis=1)
        if c:
            result = result + entering[at] * mm(bc_out[at, STATE:], now.astype(BF))
        y[at] = result.astype(BF)
        now = factors[c : c + 1] * now + mm(bt[c], weighted[at])
        whole = whole * factors[c : c + 1]
    state[0:STATE] = now.astype(BF)
    state[STATE:] = jnp.broadcast_to(whole, (16, LANES)).astype(BF)


def whole_spec(shape):
    return pl.BlockSpec(shape, lambda *_: (0,) * len(shape))


def column_spec(rows):
    return pl.BlockSpec((rows, LANES), lambda g: (0, g))


def ssd_forward(x_ext, misc, info, row_ids, taps, bias, bc_taps, bc_bias, dt_bias, decay):
    rows = x_ext.shape[0] - HALO
    chunks = rows // Q
    return pl.pallas_call(
        ssd_kernel,
        grid=(INNER // LANES,),
        in_specs=[
            column_spec(rows + HALO),
            whole_spec(misc.shape),
            whole_spec(info.shape),
            whole_spec(row_ids.shape),
            column_spec(8),
            column_spec(1),
            whole_spec(bc_taps.shape),
            whole_spec(bc_bias.shape),
            whole_spec(dt_bias.shape),
            whole_spec(decay.shape),
        ],
        out_specs=[
            column_spec(rows),
            column_spec(rows),
            column_spec(STATE + 16),
            whole_spec((rows, 128)),
            whole_spec((rows, 2 * STATE)),
        ],
        out_shape=[
            SDS((rows, INNER), BF),
            SDS((rows, INNER), BF),
            SDS((STATE + 16, INNER), BF),
            SDS((rows, 128), F32),
            SDS((rows, 2 * STATE), BF),
        ],
        scratch_shapes=[
            pltpu.VMEM((chunks, STATE, Q), BF),
            pltpu.VMEM((chunks, Q, Q), F32),
            pltpu.VMEM((rows, 128), F32),
            pltpu.VMEM((rows, 128), F32),
            pltpu.VMEM((chunks, 128, Q), F32),
            pltpu.VMEM((rows, 128), F32),
            pltpu.VMEM((rows, 128), F32),
            pltpu.VMEM((8, 128), F32),
        ],
        compiler_params=params(),
        cost_estimate=cost(20e9, 12e6),
        name="ssd_forward",
    )(x_ext, misc, info, row_ids, taps, bias, bc_taps, bc_bias, dt_bias, decay)


GATE_LANES = 512


def gate_kernel(y, signal, gate, dno, bc, ent, incoming, skip, gain, normed_out, d_y, d_gate, adjoint, sums, y_sum, gated_sum, acc):
    block = pl.program_id(0)
    rows = y.shape[0]
    width = GATE_LANES
    pieces = INNER // width

    @pl.when(block == 0)
    def _():
        acc[...] = jnp.zeros_like(acc)
        sums[...] = jnp.zeros_like(sums)

    cc = bc[:, STATE:]
    cc_t = cc.T
    ent_hi = ent[...].astype(BF)
    ent_lo = (ent[...] - ent_hi.astype(F32)).astype(BF)

    def lanes_of(i):
        pick = jnp.where(
            iota((128, width), 0) == i * (width // HEAD_DIM) + iota((128, width), 1) // HEAD_DIM, 1.0, 0.0
        ).astype(BF)
        return mm(ent_hi, pick) + mm(ent_lo, pick)

    def first(i, carry):
        squares, dots = carry
        at = pl.ds(pl.multiple_of(i * width, width), width)
        total = y[:, at].astype(F32) + skip[:, at] * signal[:, at].astype(F32)
        total = total + lanes_of(i) * mm(cc, incoming[0:STATE, at])
        z = gate[:, at].astype(F32)
        gated = total * (z * sigmoid(z))
        y_sum[:, at] = total
        gated_sum[:, at] = gated
        squares = squares + jnp.sum(gated * gated, axis=-1, keepdims=True)
        dots = dots + jnp.sum(dno[:, at].astype(F32) * gain[:, at] * gated, axis=-1, keepdims=True)
        return squares, dots

    zero = jnp.zeros((rows, 1), F32)
    squares, dots = lax.fori_loop(0, pieces, first, (zero, zero))
    inv = lax.rsqrt(squares / INNER + EPS)
    pull = inv * inv * inv * (dots / INNER)

    def second(i, carry):
        at = pl.ds(pl.multiple_of(i * width, width), width)
        total, gated = y_sum[:, at], gated_sum[:, at]
        z = gate[:, at].astype(F32)
        logistic = sigmoid(z)
        d_out = dno[:, at].astype(F32)
        scaled = gated * inv
        normed_out[:, at] = (scaled * gain[:, at]).astype(BF)
        d_gated = inv * (d_out * gain[:, at]) - gated * pull
        dy = d_gated * (z * logistic)
        d_y[:, at] = dy.astype(BF)
        d_gate[:, at] = (d_gated * total * logistic * (1.0 + z * (1.0 - logistic))).astype(BF)
        acc[:, at] += mm(cc_t, (dy * lanes_of(i)).astype(BF))
        sums[0:1, at] += jnp.sum(d_out * scaled, axis=0, keepdims=True)
        sums[1:2, at] += jnp.sum(dy * signal[:, at].astype(F32), axis=0, keepdims=True)
        return carry

    lax.fori_loop(0, pieces, second, 0)

    @pl.when(block == pl.num_programs(0) - 1)
    def _():
        adjoint[...] = acc[...].astype(BF)


def gate_norm(y, signal, gate, dno, bc, ent, incoming, skip, gain):
    rows = y.shape[0]
    size = min(rows, 128)
    row = lambda cols: pl.BlockSpec((size, cols), lambda i: (i, 0))
    return pl.pallas_call(
        gate_kernel,
        grid=(rows // size,),
        in_specs=[
            row(INNER), row(INNER), row(INNER), row(INNER), row(2 * STATE), row(128),
            whole_spec(incoming.shape), whole_spec((1, INNER)), whole_spec((1, INNER)),
        ],
        out_specs=[row(INNER), row(INNER), row(INNER), whole_spec((STATE, INNER)), whole_spec((8, INNER))],
        out_shape=[
            SDS((rows, INNER), BF), SDS((rows, INNER), BF), SDS((rows, INNER), BF),
            SDS((STATE, INNER), BF), SDS((8, INNER), F32),
        ],
        scratch_shapes=[
            pltpu.VMEM((size, INNER), F32), pltpu.VMEM((size, INNER), F32), pltpu.VMEM((STATE, INNER), F32),
        ],
        compiler_params=params(),
        cost_estimate=cost(10e9, 25e6),
        name="gate_norm",
    )(y, signal, gate, dno, bc, ent, incoming, skip, gain)


def conv_back(du, ext, taps, info):
    grads = []
    zero = jnp.zeros((HALO, du.shape[1]), F32)
    back = None
    for k in range(CONV):
        part = du if k == 0 else du * info[:, k - 1 : k]
        moved = ext if k == 0 else pltpu.roll(ext, k, 0)
        grads.append(jnp.sum(part * moved[HALO:], axis=0, keepdims=True))
        term = jnp.concatenate([zero, part * taps[k : k + 1]], axis=0)
        if k:
            term = pltpu.roll(term, term.shape[0] - k, 0)
        back = term if back is None else back + term
    grads.append(jnp.sum(du, axis=0, keepdims=True))
    grads.append(jnp.zeros((3, du.shape[1]), F32))
    return back, jnp.concatenate(grads, axis=0)


def slope_of(u):
    logistic = sigmoid(u)
    return logistic * (1.0 + u * (1.0 - logistic))


def ssd_back_kernel(
    x, signal, dy, misc, info, row_ids, taps, bias, bc_taps, bc_bias, dt_bias, decay, skip, incoming, after,
    dx, tail, rim, conv_grad, d_bc, rim_bc, bc_grad, d_dt, head_grad,
    bcu, bc, bt, ct, scores, pre, step, rate, cum, cum_t, enter, leave, factor,
    d_scores, d_b, d_c, d_direct, d_enter, d_leave, d_rows, d_cols, d_factor,
):
    group = pl.program_id(0)
    rows = signal.shape[0]
    chunks = rows // Q

    @pl.when(group == 0)
    def _():
        factor[...] = jnp.zeros_like(factor)
        prepare(misc, info, row_ids, bc_taps, bc_bias, dt_bias, decay, bcu, bc, bt, ct, scores, pre, step, rate, cum, cum_t, enter, leave, factor)
        for ref in (d_scores, d_b, d_c, d_direct, d_enter, d_leave, d_rows, d_cols, d_factor):
            ref[...] = jnp.zeros_like(ref)

    pick = head_lanes(group, LANES)
    gather = jnp.where(
        iota((LANES, 128), 1) == group * GROUP_HEADS + iota((LANES, 128), 0) // HEAD_DIM, 1.0, 0.0
    ).astype(BF)
    act = signal[...].astype(F32)
    steps = expand(step[...], pick)
    inputs = act * steps
    inputs_b = inputs.astype(BF)
    leaving = expand(leave[...], pick)
    weighted = inputs * leaving
    weighted_b = weighted.astype(BF)
    cot = dy[...].astype(F32)
    cot_in = cot * expand(enter[...], pick)
    cot_in_b = cot_in.astype(BF)
    factors = expand(factor[...], pick)
    now = incoming[0:STATE].astype(F32)
    states = []
    for c in range(chunks):
        at = slice(c * Q, (c + 1) * Q)
        states.append(now.astype(BF))
        if c < chunks - 1:
            now = factors[c : c + 1] * now + mm(bt[c], weighted_b[at])
    adj = after[0:STATE].astype(F32)
    lane = iota((Q, 128), 1)
    d_signal = [None] * chunks
    for c in reversed(range(chunks)):
        at = slice(c * Q, (c + 1) * Q)
        bb, cc = bc[at, :STATE], bc[at, STATE:]
        adj_b = adj.astype(BF)
        from_state = mm(cc, states[c])
        from_adj = mm(bb, adj_b)
        d_c[at] += mm(cot_in_b[at], states[c], NT)
        d_b[at] += mm(weighted_b[at], adj_b, NT)
        crossing = factors[c : c + 1] * jnp.sum(adj * states[c].astype(F32), axis=0, keepdims=True)
        d_factor[c] += mm(jnp.broadcast_to(crossing, (8, LANES)).astype(BF), gather)
        turned = turned_sums(cum, at, group)
        masked = scores[c]
        pieces = []
        score_sum = None
        row_sum = jnp.zeros((Q, 128), F32)
        for p in range(LANES // 128):
            lanes = slice(p * 128, p * 128 + 128)
            cots = halves(dy[at, lanes])
            d_pair = mm(cots, inputs_b[at, lanes], NT)
            both = []
            for j in range(2):
                k = 2 * p + j
                decays = decay_of(turned, cum_t, c, group, k)
                both.append((masked * decays).astype(BF))
                through = d_pair[j * Q : (j + 1) * Q] * decays
                score_sum = through if score_sum is None else score_sum + through
                product = through * masked
                row_sum = jnp.where(
                    lane == group * GROUP_HEADS + k, jnp.sum(product, axis=1, keepdims=True), row_sum
                )
                d_cols[c, pl.ds(group * GROUP_HEADS + k, 1), :] = jnp.sum(product, axis=0, keepdims=True)
            pieces.append(mm(jnp.concatenate(both, axis=0), cots, TN))
        d_scores[c] += score_sum
        d_rows[at] += row_sum
        d_inputs = jnp.concatenate(pieces, axis=1) + leaving[at] * from_adj
        d_direct[at] += mm((act[at] * d_inputs).astype(BF), gather)
        d_enter[at] += mm((cot_in[at] * from_state).astype(BF), gather)
        d_leave[at] += mm((weighted[at] * from_adj).astype(BF), gather)
        d_signal[c] = steps[at] * d_inputs + skip[...] * cot[at]
        if c:
            adj = factors[c : c + 1] * adj + mm(ct[c], cot_in_b[at])
    ext = x[...].astype(F32)
    du = jnp.concatenate(d_signal, axis=0) * slope_of(conv_of(ext, taps[...], bias[...], info[...]))
    back, grads = conv_back(du, ext, taps[...], info[...])
    dx[...] = back[HALO:].astype(BF)
    tail[...] = back[rows + HALO - 8 :]
    rim[...] = back[HALO - 8 : HALO]
    conv_grad[...] = grads

    @pl.when(group == pl.num_programs(0) - 1)
    def _():
        after_eq = jnp.where(iota((Q, Q), 1) >= iota((Q, Q), 0), 1.0, 0.0)
        before_ne = jnp.where(iota((Q, Q), 1) < iota((Q, Q), 0), 1.0, 0.0)
        grow = -jnp.exp(decay[...])
        dec_sum = jnp.zeros((1, 128), F32)
        bias_sum = jnp.zeros((1, 128), F32)
        valid = iota((Q, 128), 1) < HEADS
        parts = []
        for c in range(chunks):
            at = slice(c * Q, (c + 1) * Q)
            bb, cc = bc[at, :STATE], bc[at, STATE:]
            within = (iota((Q, Q), 0) >= iota((Q, Q), 1)) & (info[at, 3:4] == row_ids[0:1, at])
            ds = jnp.where(within, d_scores[c], 0.0).astype(BF)
            parts.append(jnp.concatenate([d_b[at] + mm(ds, cc, TN), d_c[at] + mm(ds, bb)], axis=1))
            d_rate = mm(after_eq, d_rows[at] + d_enter[at] - d_cols[c].T, NN, HIGH)
            d_rate = d_rate + mm(before_ne, d_leave[at], NN, HIGH) + d_factor[c][0:1]
            d_step = d_direct[at] + grow * d_rate
            d_pre = jnp.where(valid, d_step * sigmoid(pre[at]), 0.0)
            d_dt[at] = d_pre.astype(BF)
            bias_sum = bias_sum + jnp.sum(d_pre, axis=0, keepdims=True)
            dec_sum = dec_sum + jnp.sum(jnp.where(valid, d_rate * rate[at], 0.0), axis=0, keepdims=True)
        ext_bc = bcu[...]
        du_bc = jnp.concatenate(parts, axis=0)
        du_bc = du_bc * slope_of(conv_of(ext_bc, bc_taps[...], bc_bias[...], info[...]))
        back_bc, grads_bc = conv_back(du_bc, ext_bc, bc_taps[...], info[...])
        d_bc[...] = back_bc[HALO:]
        rim_bc[...] = back_bc[HALO - 8 : HALO]
        bc_grad[...] = grads_bc
        head_grad[...] = jnp.concatenate([bias_sum, dec_sum, jnp.zeros((6, 128), F32)], axis=0)


def ssd_backward(x_ext, signal, dy, misc, info, row_ids, taps, bias, bc_taps, bc_bias, dt_bias, decay, skip, incoming, after):
    rows = signal.shape[0]
    chunks = rows // Q
    vm = pltpu.VMEM
    return pl.pallas_call(
        ssd_back_kernel,
        grid=(INNER // LANES,),
        in_specs=[
            column_spec(rows + HALO),
            column_spec(rows),
            column_spec(rows),
            whole_spec(misc.shape),
            whole_spec(info.shape),
            whole_spec(row_ids.shape),
            column_spec(8),
            column_spec(1),
            whole_spec(bc_taps.shape),
            whole_spec(bc_bias.shape),
            whole_spec(dt_bias.shape),
            whole_spec(decay.shape),
            column_spec(1),
            column_spec(incoming.shape[0]),
            column_spec(after.shape[0]),
        ],
        out_specs=[
            column_spec(rows),
            column_spec(8),
            column_spec(8),
            column_spec(8),
            whole_spec((rows, 2 * STATE)),
            whole_spec((8, 2 * STATE)),
            whole_spec((8, 2 * STATE)),
            whole_spec((rows, 128)),
            whole_spec((8, 128)),
        ],
        out_shape=[
            SDS((rows, INNER), BF),
            SDS((8, INNER), F32),
            SDS((8, INNER), F32),
            SDS((8, INNER), F32),
            SDS((rows, 2 * STATE), F32),
            SDS((8, 2 * STATE), F32),
            SDS((8, 2 * STATE), F32),
            SDS((rows, 128), BF),
            SDS((8, 128), F32),
        ],
        scratch_shapes=[
            vm((rows + HALO, 2 * STATE), F32),
            vm((rows, 2 * STATE), BF),
            vm((chunks, STATE, Q), BF),
            vm((chunks, STATE, Q), BF),
            vm((chunks, Q, Q), F32),
            vm((rows, 128), F32),
            vm((rows, 128), F32),
            vm((rows, 128), F32),
            vm((rows, 128), F32),
            vm((chunks, 128, Q), F32),
            vm((rows, 128), F32),
            vm((rows, 128), F32),
            vm((8, 128), F32),
            vm((chunks, Q, Q), F32),
            vm((rows, 128), F32),
            vm((rows, 128), F32),
            vm((rows, 128), F32),
            vm((rows, 128), F32),
            vm((rows, 128), F32),
            vm((rows, 128), F32),
            vm((chunks, 128, Q), F32),
            vm((chunks, 8, 128), F32),
        ],
        compiler_params=params(),
        cost_estimate=cost(40e9, 15e6),
        name="ssd_backward",
    )(x_ext, signal, dy, misc, info, row_ids, taps, bias, bc_taps, bc_bias, dt_bias, decay, skip, incoming, after)


def weight_grad_kernel(left, right, out):
    nt, cols = out.shape[1], out.shape[3]
    result = mm(left[...], right[...])
    for t in range(nt):
        out[0, t] = result[:, t * cols : (t + 1) * cols].astype(BF)


def weight_grad(left_t, right, nw, nt, name):
    depth, rows = left_t.shape
    k, cols = depth // nw, INNER // nt
    return pl.pallas_call(
        weight_grad_kernel,
        grid=(nw,),
        in_specs=[
            pl.BlockSpec((k, rows), lambda w: (w, 0)),
            whole_spec(right.shape),
        ],
        out_specs=pl.BlockSpec((1, nt, k, cols), lambda w: (w, 0, 0, 0)),
        out_shape=SDS((nw, nt, k, cols), BF),
        compiler_params=params(),
        cost_estimate=cost(2 * depth * rows * INNER, 3 * depth * INNER),
        name=name,
    )(left_t, right)


def input_grad_kernel(left, right, d_bc, d_dt, out):
    nt, cols = out.shape[1], out.shape[3]
    block = INNER // nt
    result = mm(left[...], right[...])
    small = mm(left[...], jnp.concatenate([d_bc[...], d_dt[...]], axis=1)).astype(BF)
    bc_cols, heads = 2 * STATE // nt, HEADS // nt
    for t in range(nt):
        out[0, t, :, :block] = result[:, t * block : (t + 1) * block].astype(BF)
        pick = select_columns(t, heads, bc_cols, cols - block, 2 * STATE + 128)
        out[0, t, :, block:] = mm(small, pick, NT).astype(BF)


def input_grad(left_t, right, d_bc, d_dt, nw, nt, cols):
    depth, rows = left_t.shape
    k = depth // nw
    return pl.pallas_call(
        input_grad_kernel,
        grid=(nw,),
        in_specs=[
            pl.BlockSpec((k, rows), lambda w: (w, 0)),
            whole_spec(right.shape),
            whole_spec(d_bc.shape),
            whole_spec(d_dt.shape),
        ],
        out_specs=pl.BlockSpec((1, nt, k, cols), lambda w: (w, 0, 0, 0)),
        out_shape=SDS((nw, nt, k, cols), BF),
        compiler_params=params(),
        cost_estimate=cost(2 * depth * rows * INNER, 3 * depth * INNER),
        name="input_grad",
    )(left_t, right, d_bc, d_dt)


def out_kernel(left, weight, tokens, out, acc):
    t = pl.program_id(0)
    depth = out.shape[1]
    part = mm(left[...], weight[...].reshape(depth, weight.shape[3]), NT)

    @pl.when(t == 0)
    def _():
        acc[...] = tokens[...].astype(F32) + part

    @pl.when(t > 0)
    def _():
        acc[...] += part

    @pl.when(t == pl.num_programs(0) - 1)
    def _():
        out[...] = acc[...].astype(BF)


def out_project(left, weights, which, tokens):
    rows, depth = tokens.shape
    nw, nt, k, _ = weights.shape
    block = INNER // nt
    return pl.pallas_call(
        out_kernel,
        grid=(nt,),
        in_specs=[
            pl.BlockSpec((rows, block), lambda t: (0, t)),
            pl.BlockSpec((nw, 1, k, block), lambda t: (0, t, 0, which)),
            whole_spec(tokens.shape),
        ],
        out_specs=whole_spec(tokens.shape),
        out_shape=SDS(tokens.shape, BF),
        scratch_shapes=[pltpu.VMEM((rows, depth), F32)],
        compiler_params=params(),
        cost_estimate=cost(2 * rows * depth * INNER, 2 * depth * INNER),
        name="out_project",
    )(left, weights, tokens)


def gate_part_kernel(left, weight, out):
    t = pl.program_id(0)
    depth = out.shape[1]
    part = mm(left[...], weight[...].reshape(depth, weight.shape[3]), NT)

    @pl.when(t == 0)
    def _():
        out[...] = part

    @pl.when(t > 0)
    def _():
        out[...] += part


def gate_part(left, weights, which, depth):
    rows = left.shape[0]
    nw, nt, k, _ = weights.shape
    block = INNER // nt
    return pl.pallas_call(
        gate_part_kernel,
        grid=(nt,),
        in_specs=[
            pl.BlockSpec((rows, block), lambda t: (0, t)),
            pl.BlockSpec((nw, 1, k, block), lambda t: (0, t, 0, which)),
        ],
        out_specs=whole_spec((rows, depth)),
        out_shape=SDS((rows, depth), F32),
        compiler_params=params(),
        cost_estimate=cost(2 * rows * depth * INNER, 2 * depth * INNER),
        name="gate_part",
    )(left, weights)


def rows_kernel(dx, d_bc, d_dt, weight, so_far, tokens, cot, gain, grad, gain_grad, acc):
    t = pl.program_id(0)
    rows, depth = tokens.shape
    block = dx.shape[1]
    cols = weight.shape[3]
    nt = INNER // block
    w = weight[...].reshape(depth, cols)
    pick = select_columns(t, HEADS // nt, 2 * STATE // nt, cols - block, 2 * STATE + 128)
    small = mm(jnp.concatenate([d_bc[...], d_dt[...]], axis=1), pick, NT).astype(BF)
    part = mm(jnp.concatenate([dx[...], small], axis=1), w, NT)

    @pl.when(t == 0)
    def _():
        acc[...] = so_far[...] + part

    @pl.when(t > 0)
    def _():
        acc[...] += part

    @pl.when(t == pl.num_programs(0) - 1)
    def _():
        raw = tokens[...].astype(F32)
        inv = lax.rsqrt(jnp.mean(raw * raw, axis=-1, keepdims=True) + EPS)
        unit = raw * inv
        d_normed = acc[...]
        gain_grad[...] = jnp.sum(d_normed * unit, axis=0, keepdims=True)
        d_unit = d_normed * gain[...]
        grad[...] = cot[...].astype(F32) + inv * (d_unit - unit * jnp.mean(d_unit * unit, axis=-1, keepdims=True))


def rows_grad(dx, d_bc, d_dt, weights, so_far, tokens, cot, gain):
    rows, depth = tokens.shape
    nw, nt, k, cols = weights.shape
    block = INNER // nt
    return pl.pallas_call(
        rows_kernel,
        grid=(nt,),
        in_specs=[
            pl.BlockSpec((rows, block), lambda t: (0, t)),
            whole_spec(d_bc.shape),
            whole_spec(d_dt.shape),
            pl.BlockSpec((nw, 1, k, cols), lambda t: (0, t, 0, 0)),
            whole_spec(so_far.shape),
            whole_spec(tokens.shape),
            whole_spec(cot.shape),
            whole_spec((1, depth)),
        ],
        out_specs=[whole_spec((rows, depth)), whole_spec((1, depth))],
        out_shape=[SDS((rows, depth), F32), SDS((1, depth), F32)],
        scratch_shapes=[pltpu.VMEM((rows, depth), F32)],
        compiler_params=params(),
        cost_estimate=cost(2 * rows * depth * INNER, 2 * depth * INNER),
        name="rows_grad",
    )(dx, d_bc, d_dt, weights, so_far, tokens, cot, gain)


BOTH = ("wide", "tp")


def shift(value, steps):
    count = lax.axis_size("wide") * lax.axis_size("tp")
    first, last = max(0, -steps), min(count, count - steps)
    return lax.ppermute(value, BOTH, [(i, i + steps) for i in range(first, last)])


def carry_states(own, span, direction):
    reach = (DOC_MAX - 2) // span + 1
    held, size = own, 1
    while 2 * size < reach:
        other = shift(held, direction * size)
        held = combine(held, other)
        size *= 2
    near = shift(held, direction)
    if size >= reach:
        return near
    return combine(near, shift(held, direction * (1 + size)))


def combine(near, far):
    decay = near[STATE : STATE + 1].astype(F32)
    state = near[:STATE].astype(F32) + decay * far[:STATE].astype(F32)
    whole = near[STATE:].astype(F32) * far[STATE:].astype(F32)
    return jnp.concatenate([state, whole], axis=0).astype(BF)


def sum_everywhere(value):
    for axis in ("wide", "tp"):
        count = lax.axis_size(axis)
        bit = 1
        while bit < count:
            value = value + lax.ppermute(value, axis, [(i, i ^ bit) for i in range(count)])
            bit *= 2
    return value


def per_device(
    tokens, segment_ids, out_cotangent, norm_gain, z_weight, x_weight, bc_weight, dt_weight, x_conv, x_bias,
    bc_conv, bc_bias, dt_bias, decay_log, skip_gain, gate_gain, out_weight,
):
    nw, nt = lax.axis_size("wide"), lax.axis_size("tp")
    rank = lax.axis_index("tp")
    rows, depth = tokens.shape
    k = depth // nw
    block = INNER // nt
    chunks = rows // Q

    def lane_row(v, width):
        return jnp.pad(v.astype(F32), (0, width - v.shape[0]))[None, :]

    small = jnp.concatenate([bc_weight, dt_weight], axis=1)
    small = jnp.pad(small, ((0, 0), (0, 128 - small.shape[1])))
    own_x = jnp.concatenate([x_weight, small], axis=1)
    own_zo = jnp.concatenate([z_weight, out_weight.T], axis=1)
    wx = lax.all_gather(own_x, BOTH).reshape(nw, nt, k, block + 128)
    wzo = lax.all_gather(own_zo, BOTH).reshape(nw, nt, k, 2 * block)

    own_ids = lax.dynamic_slice_in_dim(segment_ids, rank * rows, rows, 0)
    halo_rows = shift(tokens[rows - HALO :], 1)
    halo_ids = shift(own_ids[rows - HALO :] + 1, 1) - 1
    ids_ext = jnp.concatenate([halo_ids, own_ids])
    ids = own_ids
    grouped = ids.reshape(chunks, Q)
    lasts = grouped[:, Q - 1]
    befores = jnp.concatenate([halo_ids[HALO - 1 :], lasts[:-1]])
    spread = lambda v: jnp.repeat(v, Q)
    info = jnp.stack(
        [(ids == ids_ext[HALO - j : HALO - j + rows]) for j in range(1, CONV)]
        + [ids]
        + [ids == spread(befores), ids == spread(lasts), ids == halo_ids[HALO - 1], spread(lasts == befores)],
        axis=1,
    ).astype(F32)
    row_ids = jnp.broadcast_to(ids.astype(F32)[None, :], (8, rows))
    tokens_ext = jnp.concatenate([halo_rows, tokens], axis=0)

    taps = jnp.pad(x_conv.astype(F32), ((0, 8 - CONV), (0, 0)))
    bias = x_bias.astype(F32)[None, :]
    bc_taps = jnp.pad(bc_conv.astype(F32), ((0, 8 - CONV), (0, 0)))
    bc_offset = bc_bias.astype(F32)[None, :]
    dt_offset = lane_row(dt_bias, 128)
    decay = lane_row(decay_log, 128)
    skip = jnp.repeat(skip_gain.astype(F32), HEAD_DIM)[None, :]
    out_gain = gate_gain.astype(F32)[None, :]
    in_gain = norm_gain.astype(F32)[None, :]

    x_ext, misc, normed_ext = project(tokens_ext, in_gain, wx)
    signal, y, own_state, ent, bc = ssd_forward(
        x_ext, misc, info, row_ids, taps, bias, bc_taps, bc_offset, dt_offset, decay
    )
    incoming = carry_states(own_state, rows, 1)
    normed = normed_ext[HALO:]
    normed_t = normed.T
    cot_t = out_cotangent.T
    gate = plain(normed, wzo, 0, "gate_project")
    dno = plain(out_cotangent, wzo, 1, "cot_project")
    normed_out, dy, d_gate, adjoint, sums = gate_norm(y, signal, gate, dno, bc, ent, incoming, skip, out_gain)
    own_adjoint = jnp.concatenate([adjoint, own_state[STATE:]], axis=0)
    after = carry_states(own_adjoint, rows, -1)
    block_out = out_project(normed_out, wzo, 1, tokens)
    o_grad = weight_grad(cot_t, normed_out, nw, nt, "out_grad")
    z_grad = weight_grad(normed_t, d_gate, nw, nt, "gate_grad")
    so_far = gate_part(d_gate, wzo, 0, depth)
    dx, tail, rim, conv_grad, d_bc, rim_bc, bc_grad, d_dt, head_grad = ssd_backward(
        x_ext, signal, dy, misc, info, row_ids, taps, bias, bc_taps, bc_offset, dt_offset, decay, skip, incoming, after
    )
    from_next = shift(jnp.concatenate([rim, rim_bc], axis=1), -1)
    dx = lax.dynamic_update_slice_in_dim(dx, (tail + from_next[:, :INNER]).astype(BF), rows - 8, 0)
    d_bc = jnp.concatenate([d_bc[: rows - 8], d_bc[rows - 8 :] + from_next[:, INNER:]], axis=0).astype(BF)
    x_grad = input_grad(normed_t, dx, d_bc, d_dt, nw, nt, block + 128)
    grad_x, gain_grad = rows_grad(dx, d_bc, d_dt, wx, so_far, tokens, out_cotangent, in_gain)

    def scatter(v):
        return lax.psum_scatter(v.reshape(nw * nt, k, v.shape[3]), BOTH, scatter_dimension=0, tiled=False).astype(F32)

    out_weight_grad = scatter(o_grad).T
    z_weight_grad = scatter(z_grad)
    own_x_grad = scatter(x_grad)
    x_weight_grad = own_x_grad[:, :block]
    bc_cols, heads = bc_weight.shape[1], dt_weight.shape[1]
    bc_weight_grad = own_x_grad[:, block : block + bc_cols]
    dt_weight_grad = own_x_grad[:, block + bc_cols : block + bc_cols + heads]

    packed = [conv_grad[: CONV + 1], sums[:2], bc_grad[: CONV + 1], head_grad[:2], gain_grad]
    flat = jnp.concatenate([v.reshape(-1, 128) for v in packed], axis=0)
    flat = sum_everywhere(flat)
    pieces, at = [], 0
    for v in packed:
        size = v.size // 128
        pieces.append(flat[at : at + size].reshape(v.shape))
        at += size
    conv_all, sums_all, bc_all, head_all, gain_all = pieces
    return (
        block_out,
        grad_x,
        gain_all[0],
        z_weight_grad,
        x_weight_grad,
        bc_weight_grad,
        dt_weight_grad,
        conv_all[:CONV],
        conv_all[CONV],
        bc_all[:CONV],
        bc_all[CONV],
        head_all[0, :HEADS],
        head_all[1, :HEADS],
        sums_all[1].reshape(HEADS, HEAD_DIM).sum(axis=1),
        sums_all[0],
        out_weight_grad,
    )


def solution(mesh):
    rows, shard, out_shard = P(("wide", "tp"), None), P("wide", "tp"), P("tp", "wide")
    return jax.shard_map(
        per_device,
        mesh=mesh,
        in_specs=(rows, P("wide"), rows, P(), shard, shard, shard, shard) + (P(),) * 8 + (out_shard,),
        out_specs=(rows, rows, P(), shard, shard, shard, shard) + (P(),) * 8 + (out_shard,),
        check_vma=False,
    )
```

```python
import functools

import jax
import jax.numpy as jnp
from jax import lax
from jax.experimental import pallas as pl
from jax.experimental.pallas import tpu as pltpu
from jax.sharding import PartitionSpec as P


HEADS = 48
HEAD_DIM = 64
STATE = 128
CONV = 4
INNER = 3072
DOC_MAX = 2048
EPS = 1e-05
HALO = 16
Q = 128
LANES = 256
GROUP_HEADS = LANES // HEAD_DIM
F32 = jnp.float32
BF = jnp.bfloat16
HIGH = lax.Precision.HIGHEST
NN = ((1,), (0,))
NT = ((1,), (1,))
TN = ((0,), (0,))
SDS = jax.ShapeDtypeStruct


def mm(a, b, dims=NN, precision=None):
    return lax.dot_general(a, b, (dims, ((), ())), precision=precision, preferred_element_type=F32)


def sigmoid(v):
    return 1.0 / (1.0 + jnp.exp(-v))


def iota(shape, axis):
    return lax.broadcasted_iota(jnp.int32, shape, axis)


def params(vmem_mb=60, **kw):
    return pltpu.CompilerParams(vmem_limit_bytes=vmem_mb * 1024 * 1024, **kw)


def cost(flops, read):
    return pl.CostEstimate(flops=int(flops), bytes_accessed=int(read), transcendentals=0)


def marks_of(ids, halo_ids):
    rows = ids.shape[1]
    here = ids.T
    row, lane = iota(here.shape, 0), iota(here.shape, 1)
    before = [jnp.broadcast_to(halo_ids[0:1, 128 - j : 129 - j], here.shape) for j in range(1, CONV)]
    same = []
    for k in range(1, CONV):
        past = pltpu.roll(here, k, 0)
        for r in range(k):
            past = jnp.where(row == r, before[k - 1 - r], past)
        same.append(past == here)
    firsts, lasts = [], []
    for c in range(rows // Q):
        end = jnp.broadcast_to(here[c * Q + Q - 1 : c * Q + Q, 0:1], (Q, 8))
        start = jnp.broadcast_to(here[c * Q - 1 : c * Q, 0:1], (Q, 8)) if c else before[0][:Q]
        firsts.append(start)
        lasts.append(end)
    first, last = jnp.concatenate(firsts, axis=0), jnp.concatenate(lasts, axis=0)
    marks = same + [None, here == first, here == last, here == before[0], first == last]
    result = here
    for i, mark in enumerate(marks):
        if mark is not None:
            result = jnp.where(lane == i, jnp.where(mark, 1.0, 0.0), result)
    return result


def proj_kernel(tok, halo, gain, ids, halo_ids, weight, x_out, misc_out, normed, turned, info):
    @pl.when(pl.program_id(0) == 0)
    def _():
        for rows, at in ((halo, slice(0, HALO)), (tok, slice(HALO, None))):
            raw = rows[...].astype(F32)
            inv = lax.rsqrt(jnp.mean(raw * raw, axis=-1, keepdims=True) + EPS)
            normed[at] = (raw * inv * gain[...]).astype(BF)
        turned[...] = normed[HALO:].T
        info[...] = marks_of(ids[...], halo_ids[...])

    depth, cols = tok.shape[1], weight.shape[3]
    result = mm(normed[...], weight[...].reshape(depth, cols))
    block = x_out.shape[1]
    x_out[...] = result[:, :block].astype(BF)
    misc_out[0] = result[:, block:].astype(BF)


def project(tokens, halo_rows, gain, ids, halo_ids, weights):
    rows, depth = tokens.shape
    rows = rows + HALO
    nw, nt, k, cols = weights.shape
    block = INNER // nt
    misc = cols - block
    return pl.pallas_call(
        proj_kernel,
        grid=(nt,),
        in_specs=[
            whole_spec(tokens.shape),
            whole_spec(halo_rows.shape),
            whole_spec((1, depth)),
            whole_spec(ids.shape),
            whole_spec(halo_ids.shape),
            pl.BlockSpec((nw, 1, k, cols), lambda t: (0, t, 0, 0)),
        ],
        out_specs=[
            pl.BlockSpec((rows, block), lambda t: (0, t)),
            pl.BlockSpec((1, rows, misc), lambda t: (t, 0, 0)),
            pl.BlockSpec((rows, depth), lambda t: (0, 0)),
            pl.BlockSpec((depth, rows - HALO), lambda t: (0, 0)),
            whole_spec((rows - HALO, 8)),
        ],
        out_shape=[
            SDS((rows, INNER), BF),
            SDS((nt, rows, misc), BF),
            SDS((rows, depth), BF),
            SDS((depth, rows - HALO), BF),
            SDS((rows - HALO, 8), F32),
        ],
        compiler_params=params(),
        cost_estimate=cost(2 * rows * depth * nt * cols, 2 * depth * nt * cols),
        name="project",
    )(tokens, halo_rows, gain, ids, halo_ids, weights)


def plain_kernel(left, weight, out, *turned, first):
    depth, cols = left.shape[1], weight.shape[3]
    if turned:
        @pl.when(pl.program_id(0) == 0)
        def _():
            turned[0][...] = left[...].T

    out[...] = mm(left[first:], weight[...].reshape(depth, cols)).astype(BF)


def plain(left, weights, first, turned):
    rows, depth = left.shape
    rows = rows - first
    nw, nt, k, _ = weights.shape
    block = INNER // nt
    out_specs = [pl.BlockSpec((rows, block), lambda t: (0, t))]
    out_shape = [SDS((rows, INNER), BF)]
    if turned:
        out_specs.append(pl.BlockSpec((depth, rows), lambda t: (0, 0)))
        out_shape.append(SDS((depth, rows), BF))
    return pl.pallas_call(
        functools.partial(plain_kernel, first=first),
        grid=(nt,),
        in_specs=[
            pl.BlockSpec(left.shape, lambda t: (0, 0)),
            pl.BlockSpec((nw, 1, k, block), lambda t: (0, t, 0, 0)),
        ],
        out_specs=out_specs,
        out_shape=out_shape,
        compiler_params=params(),
        cost_estimate=cost(2 * rows * depth * INNER, 2 * depth * INNER),
    )(left, weights)


def select_columns(t, heads, bc_cols, rows, cols):
    lane, col = iota((rows, cols), 0), iota((rows, cols), 1)
    first = (lane < bc_cols) & (col == lane + t * bc_cols)
    second = (
        (lane >= bc_cols)
        & (lane < bc_cols + heads)
        & (col == lane - bc_cols + 2 * STATE + t * heads)
    )
    return jnp.where(first | second, 1.0, 0.0).astype(BF)


def conv_of(ext, taps, bias, info):
    total = bias + taps[0:1] * ext[HALO:]
    for k in range(1, CONV):
        total = total + taps[k : k + 1] * pltpu.roll(ext, k, 0)[HALO:] * info[:, k - 1 : k]
    return total


def head_lanes(group, lanes):
    return jnp.where(
        iota((128, lanes), 0) == group * GROUP_HEADS + iota((128, lanes), 1) // HEAD_DIM, 1.0, 0.0
    ).astype(BF)


def expand(values, selection):
    high = values.astype(BF)
    low = (values - high.astype(F32)).astype(BF)
    return mm(high, selection) + mm(low, selection)


def prepare(misc, info, row_ids, small_rows, bcu, bc, bt, ct, scores, pre, step, rate, cum, cum_t, enter, leave, factor):
    nt, rows_ext, width = misc.shape
    rows = rows_ext - HALO
    chunks = rows // Q
    bc_cols, heads = 2 * STATE // nt, HEADS // nt
    total = None
    for t in range(nt):
        part = mm(misc[t], select_columns(t, heads, bc_cols, width, 2 * STATE + 128))
        total = part if total is None else total + part
    marks = info[...]
    bc_ext = total[:, : 2 * STATE]
    u = conv_of(bc_ext, small_rows[0:CONV], small_rows[CONV : CONV + 1], marks)
    if bcu is not None:
        bcu[...] = bc_ext
    act = (u * sigmoid(u)).astype(BF)
    bc[...] = act
    before = total[HALO:, 2 * STATE :] + small_rows[CONV + 1 : CONV + 2, 0:128]
    steps = jnp.maximum(before, 0.0) + jnp.log1p(jnp.exp(-jnp.abs(before)))
    rates = -jnp.exp(small_rows[CONV + 2 : CONV + 3, 0:128]) * steps
    rates = jnp.where(iota(rates.shape, 1) < HEADS, rates, 0.0)
    if pre is not None:
        pre[...] = before
        rate[...] = rates
    step[...] = steps
    upper = iota((Q, Q), 0) >= iota((Q, Q), 1)
    lower = jnp.where(upper, 1.0, 0.0)
    for c in range(chunks):
        at = slice(c * Q, (c + 1) * Q)
        sums = mm(lower, rates[at], NN, HIGH)
        cum[at] = sums
        cum_t[c] = sums.T
        last = sums[Q - 1 : Q]
        enter[at] = jnp.exp(sums) * marks[at, 4:5]
        leave[at] = jnp.exp(last - sums) * marks[at, 5:6]
        factor[c : c + 1] = jnp.exp(last) * marks[c * Q : c * Q + 1, 7:8]
        bb, cc = act[at, :STATE], act[at, STATE:]
        within = upper & (marks[at, 3:4] == row_ids[0:1, at])
        scores[c] = jnp.where(within, mm(cc, bb, NT), 0.0)
        bt[c] = bb.T
        if ct is not None:
            ct[c] = cc.T


def decay_of(turned, cum_t, c, group, k):
    row = cum_t[c, pl.ds(group * GROUP_HEADS + k, 1), :]
    return jnp.exp(jnp.minimum(turned[:, k : k + 1] - row, 0.0))


def turned_sums(cum, at, group):
    return pltpu.roll(cum[at], (128 - group * GROUP_HEADS) % 128, 1)


def halves(pair):
    left = iota(pair.shape, 1) < HEAD_DIM
    zero = jnp.zeros_like(pair)
    return jnp.concatenate([jnp.where(left, pair, zero), jnp.where(left, zero, pair)], axis=0)


def ssd_kernel(x, misc, info, row_ids, wide_rows, small_rows, signal, y, state, ent, bc_out, bt, scores, step, cum, cum_t, enter, leave, factor):
    group = pl.program_id(0)
    rows = signal.shape[0]
    chunks = rows // Q

    @pl.when(group == 0)
    def _():
        factor[...] = jnp.zeros_like(factor)
        prepare(misc, info, row_ids, small_rows, None, bc_out, bt, None, scores, None, step, None, cum, cum_t, enter, leave, factor)
        base = jnp.zeros((1, 128), F32)
        for c in range(chunks):
            at = slice(c * Q, (c + 1) * Q)
            ent[at] = jnp.exp(cum[at] + base) * info[at, 6:7]
            base = base + cum[c * Q + Q - 1 : c * Q + Q]

    u = conv_of(x[...].astype(F32), wide_rows[0:CONV], wide_rows[CONV : CONV + 1], info[...])
    act = (u * sigmoid(u)).astype(BF)
    signal[...] = act
    pick = head_lanes(group, LANES)
    inputs = act.astype(F32) * expand(step[...], pick)
    inputs_b = inputs.astype(BF)
    weighted = (inputs * expand(leave[...], pick)).astype(BF)
    entering = expand(enter[...], pick)
    factors = expand(factor[...], pick)
    now = jnp.zeros((STATE, LANES), F32)
    whole = jnp.ones((1, LANES), F32)
    for c in range(chunks):
        at = slice(c * Q, (c + 1) * Q)
        turned = turned_sums(cum, at, group)
        pieces = []
        for p in range(LANES // 128):
            ma = (scores[c] * decay_of(turned, cum_t, c, group, 2 * p)).astype(BF)
            mb = (scores[c] * decay_of(turned, cum_t, c, group, 2 * p + 1)).astype(BF)
            pieces.append(mm(jnp.concatenate([ma, mb], axis=1), halves(inputs_b[at, p * 128 : p * 128 + 128])))
        result = jnp.concatenate(pieces, axis=1)
        if c:
            result = result + entering[at] * mm(bc_out[at, STATE:], now.astype(BF))
        y[at] = result.astype(BF)
        now = factors[c : c + 1] * now + mm(bt[c], weighted[at])
        whole = whole * factors[c : c + 1]
    state[0:STATE] = now.astype(BF)
    state[STATE:] = jnp.broadcast_to(whole, (16, LANES)).astype(BF)


def whole_spec(shape):
    return pl.BlockSpec(shape, lambda *_: (0,) * len(shape))


def column_spec(rows):
    return pl.BlockSpec((rows, LANES), lambda g: (0, g))


def ssd_forward(x_ext, misc, info, row_ids, wide_rows, small_rows):
    rows = x_ext.shape[0] - HALO
    chunks = rows // Q
    return pl.pallas_call(
        ssd_kernel,
        grid=(INNER // LANES,),
        in_specs=[
            column_spec(rows + HALO),
            whole_spec(misc.shape),
            whole_spec(info.shape),
            whole_spec(row_ids.shape),
            column_spec(8),
            whole_spec(small_rows.shape),
        ],
        out_specs=[
            column_spec(rows),
            column_spec(rows),
            column_spec(STATE + 16),
            whole_spec((rows, 128)),
            whole_spec((rows, 2 * STATE)),
        ],
        out_shape=[
            SDS((rows, INNER), BF),
            SDS((rows, INNER), BF),
            SDS((STATE + 16, INNER), BF),
            SDS((rows, 128), F32),
            SDS((rows, 2 * STATE), BF),
        ],
        scratch_shapes=[
            pltpu.VMEM((chunks, STATE, Q), BF),
            pltpu.VMEM((chunks, Q, Q), F32),
            pltpu.VMEM((rows, 128), F32),
            pltpu.VMEM((rows, 128), F32),
            pltpu.VMEM((chunks, 128, Q), F32),
            pltpu.VMEM((rows, 128), F32),
            pltpu.VMEM((rows, 128), F32),
            pltpu.VMEM((8, 128), F32),
        ],
        compiler_params=params(),
        cost_estimate=cost(20e9, 12e6),
        name="ssd_forward",
    )(x_ext, misc, info, row_ids, wide_rows, small_rows)


GATE_LANES = 1024


def gate_kernel(y, signal, gate, dno, bc, ent, incoming, wide_rows, pair, d_y, adjoint, sums, y_sum, gated_sum, acc):
    block = pl.program_id(0)
    rows = y.shape[0]
    width = GATE_LANES
    pieces = INNER // width

    @pl.when(block == 0)
    def _():
        acc[...] = jnp.zeros_like(acc)
        sums[...] = jnp.zeros_like(sums)

    cc = bc[:, STATE:]
    cc_t = cc.T
    ent_hi = ent[...].astype(BF)
    ent_lo = (ent[...] - ent_hi.astype(F32)).astype(BF)

    def lanes_of(i):
        pick = jnp.where(
            iota((128, width), 0) == i * (width // HEAD_DIM) + iota((128, width), 1) // HEAD_DIM, 1.0, 0.0
        ).astype(BF)
        return mm(ent_hi, pick) + mm(ent_lo, pick)

    def first(i, carry):
        squares, dots = carry
        at = pl.ds(pl.multiple_of(i * width, width), width)
        total = y[:, at].astype(F32) + wide_rows[CONV + 1 : CONV + 2, at] * signal[:, at].astype(F32)
        total = total + lanes_of(i) * mm(cc, incoming[0:STATE, at])
        z = gate[:, at].astype(F32)
        gated = total * (z * sigmoid(z))
        y_sum[:, at] = total
        gated_sum[:, at] = gated
        squares = squares + jnp.sum(gated * gated, axis=-1, keepdims=True)
        dots = dots + jnp.sum(dno[:, at].astype(F32) * wide_rows[CONV + 2 : CONV + 3, at] * gated, axis=-1, keepdims=True)
        return squares, dots

    zero = jnp.zeros((rows, 1), F32)
    squares, dots = lax.fori_loop(0, pieces, first, (zero, zero))
    inv = lax.rsqrt(squares / INNER + EPS)
    pull = inv * inv * inv * (dots / INNER)

    def second(i, carry):
        at = pl.ds(pl.multiple_of(i * width, width), width)
        total, gated = y_sum[:, at], gated_sum[:, at]
        z = gate[:, at].astype(F32)
        logistic = sigmoid(z)
        d_out = dno[:, at].astype(F32)
        scaled = gated * inv
        pair[1, :, at] = (scaled * wide_rows[CONV + 2 : CONV + 3, at]).astype(BF)
        d_gated = inv * (d_out * wide_rows[CONV + 2 : CONV + 3, at]) - gated * pull
        dy = d_gated * (z * logistic)
        d_y[:, at] = dy.astype(BF)
        pair[0, :, at] = (d_gated * total * logistic * (1.0 + z * (1.0 - logistic))).astype(BF)
        acc[:, at] += mm(cc_t, (dy * lanes_of(i)).astype(BF))
        sums[0:1, at] += jnp.sum(d_out * scaled, axis=0, keepdims=True)
        sums[1:2, at] += jnp.sum(dy * signal[:, at].astype(F32), axis=0, keepdims=True)
        return carry

    lax.fori_loop(0, pieces, second, 0)

    @pl.when(block == pl.num_programs(0) - 1)
    def _():
        adjoint[...] = acc[...].astype(BF)


def gate_norm(y, signal, gate, dno, bc, ent, incoming, wide_rows):
    rows = y.shape[0]
    size = min(rows, 256)
    row = lambda cols: pl.BlockSpec((size, cols), lambda i: (i, 0))
    return pl.pallas_call(
        gate_kernel,
        grid=(rows // size,),
        in_specs=[
            row(INNER), row(INNER), row(INNER), row(INNER), row(2 * STATE), row(128),
            whole_spec(incoming.shape), whole_spec(wide_rows.shape),
        ],
        out_specs=[
            pl.BlockSpec((2, size, INNER), lambda i: (0, i, 0)), row(INNER), whole_spec((STATE, INNER)), whole_spec((8, INNER)),
        ],
        out_shape=[
            SDS((2, rows, INNER), BF), SDS((rows, INNER), BF), SDS((STATE, INNER), BF), SDS((8, INNER), F32),
        ],
        scratch_shapes=[
            pltpu.VMEM((size, INNER), F32), pltpu.VMEM((size, INNER), F32), pltpu.VMEM((STATE, INNER), F32),
        ],
        compiler_params=params(),
        cost_estimate=cost(10e9, 25e6),
        name="gate_norm",
    )(y, signal, gate, dno, bc, ent, incoming, wide_rows)


def conv_back(du, ext, taps, info):
    grads = []
    zero = jnp.zeros((HALO, du.shape[1]), F32)
    back = None
    for k in range(CONV):
        part = du if k == 0 else du * info[:, k - 1 : k]
        moved = ext if k == 0 else pltpu.roll(ext, k, 0)
        grads.append(jnp.sum(part * moved[HALO:], axis=0, keepdims=True))
        term = jnp.concatenate([zero, part * taps[k : k + 1]], axis=0)
        if k:
            term = pltpu.roll(term, term.shape[0] - k, 0)
        back = term if back is None else back + term
    grads.append(jnp.sum(du, axis=0, keepdims=True))
    grads.append(jnp.zeros((3, du.shape[1]), F32))
    return back, jnp.concatenate(grads, axis=0)


def slope_of(u):
    logistic = sigmoid(u)
    return logistic * (1.0 + u * (1.0 - logistic))


def ssd_back_kernel(
    x, signal, dy, misc, info, row_ids, wide_rows, small_rows, incoming, after,
    dx, tail, rim, conv_grad, small, tail_bc, rim_bc, bc_grad, head_grad,
    bcu, bc, bt, ct, scores, pre, step, rate, cum, cum_t, enter, leave, factor,
    d_scores, d_b, d_c, d_direct, d_enter, d_leave, d_rows, d_cols, d_factor,
):
    group = pl.program_id(0)
    rows = signal.shape[0]
    chunks = rows // Q

    @pl.when(group == 0)
    def _():
        factor[...] = jnp.zeros_like(factor)
        prepare(misc, info, row_ids, small_rows, bcu, bc, bt, ct, scores, pre, step, rate, cum, cum_t, enter, leave, factor)
        for ref in (d_scores, d_b, d_c, d_direct, d_enter, d_leave, d_rows, d_cols, d_factor):
            ref[...] = jnp.zeros_like(ref)

    pick = head_lanes(group, LANES)
    gather = jnp.where(
        iota((LANES, 128), 1) == group * GROUP_HEADS + iota((LANES, 128), 0) // HEAD_DIM, 1.0, 0.0
    ).astype(BF)
    act = signal[...].astype(F32)
    steps = expand(step[...], pick)
    inputs = act * steps
    inputs_b = inputs.astype(BF)
    leaving = expand(leave[...], pick)
    weighted = inputs * leaving
    weighted_b = weighted.astype(BF)
    cot = dy[...].astype(F32)
    cot_in = cot * expand(enter[...], pick)
    cot_in_b = cot_in.astype(BF)
    factors = expand(factor[...], pick)
    now = incoming[0:STATE].astype(F32)
    states = []
    for c in range(chunks):
        at = slice(c * Q, (c + 1) * Q)
        states.append(now.astype(BF))
        if c < chunks - 1:
            now = factors[c : c + 1] * now + mm(bt[c], weighted_b[at])
    adj = after[0:STATE].astype(F32)
    lane = iota((Q, 128), 1)
    d_signal = [None] * chunks
    for c in reversed(range(chunks)):
        at = slice(c * Q, (c + 1) * Q)
        bb, cc = bc[at, :STATE], bc[at, STATE:]
        adj_b = adj.astype(BF)
        from_state = mm(cc, states[c])
        from_adj = mm(bb, adj_b)
        d_c[at] += mm(cot_in_b[at], states[c], NT)
        d_b[at] += mm(weighted_b[at], adj_b, NT)
        crossing = factors[c : c + 1] * jnp.sum(adj * states[c].astype(F32), axis=0, keepdims=True)
        d_factor[c] += mm(jnp.broadcast_to(crossing, (8, LANES)).astype(BF), gather)
        turned = turned_sums(cum, at, group)
        masked = scores[c]
        pieces = []
        score_sum = None
        row_sum = jnp.zeros((Q, 128), F32)
        for p in range(LANES // 128):
            lanes = slice(p * 128, p * 128 + 128)
            cots = halves(dy[at, lanes])
            d_pair = mm(cots, inputs_b[at, lanes], NT)
            both = []
            for j in range(2):
                k = 2 * p + j
                decays = decay_of(turned, cum_t, c, group, k)
                both.append((masked * decays).astype(BF))
                through = d_pair[j * Q : (j + 1) * Q] * decays
                score_sum = through if score_sum is None else score_sum + through
                product = through * masked
                row_sum = jnp.where(
                    lane == group * GROUP_HEADS + k, jnp.sum(product, axis=1, keepdims=True), row_sum
                )
                d_cols[c, pl.ds(group * GROUP_HEADS + k, 1), :] = jnp.sum(product, axis=0, keepdims=True)
            pieces.append(mm(jnp.concatenate(both, axis=0), cots, TN))
        d_scores[c] += score_sum
        d_rows[at] += row_sum
        d_inputs = jnp.concatenate(pieces, axis=1) + leaving[at] * from_adj
        d_direct[at] += mm((act[at] * d_inputs).astype(BF), gather)
        d_enter[at] += mm((cot_in[at] * from_state).astype(BF), gather)
        d_leave[at] += mm((weighted[at] * from_adj).astype(BF), gather)
        d_signal[c] = steps[at] * d_inputs + wide_rows[CONV + 1 : CONV + 2] * cot[at]
        if c:
            adj = factors[c : c + 1] * adj + mm(ct[c], cot_in_b[at])
    ext = x[...].astype(F32)
    du = jnp.concatenate(d_signal, axis=0) * slope_of(conv_of(ext, wide_rows[0:CONV], wide_rows[CONV : CONV + 1], info[...]))
    back, grads = conv_back(du, ext, wide_rows[0:CONV], info[...])
    dx[...] = back[HALO:].astype(BF)
    tail[...] = back[rows + HALO - 8 :]
    rim[...] = back[HALO - 8 : HALO]
    conv_grad[...] = grads

    @pl.when(group == pl.num_programs(0) - 1)
    def _():
        after_eq = jnp.where(iota((Q, Q), 1) >= iota((Q, Q), 0), 1.0, 0.0)
        before_ne = jnp.where(iota((Q, Q), 1) < iota((Q, Q), 0), 1.0, 0.0)
        grow = -jnp.exp(small_rows[CONV + 2 : CONV + 3, 0:128])
        dec_sum = jnp.zeros((1, 128), F32)
        bias_sum = jnp.zeros((1, 128), F32)
        valid = iota((Q, 128), 1) < HEADS
        parts = []
        for c in range(chunks):
            at = slice(c * Q, (c + 1) * Q)
            bb, cc = bc[at, :STATE], bc[at, STATE:]
            within = (iota((Q, Q), 0) >= iota((Q, Q), 1)) & (info[at, 3:4] == row_ids[0:1, at])
            ds = jnp.where(within, d_scores[c], 0.0).astype(BF)
            parts.append(jnp.concatenate([d_b[at] + mm(ds, cc, TN), d_c[at] + mm(ds, bb)], axis=1))
            d_rate = mm(after_eq, d_rows[at] + d_enter[at] - d_cols[c].T, NN, HIGH)
            d_rate = d_rate + mm(before_ne, d_leave[at], NN, HIGH) + d_factor[c][0:1]
            d_step = d_direct[at] + grow * d_rate
            d_pre = jnp.where(valid, d_step * sigmoid(pre[at]), 0.0)
            small[at, 2 * STATE :] = d_pre.astype(BF)
            bias_sum = bias_sum + jnp.sum(d_pre, axis=0, keepdims=True)
            dec_sum = dec_sum + jnp.sum(jnp.where(valid, d_rate * rate[at], 0.0), axis=0, keepdims=True)
        ext_bc = bcu[...]
        du_bc = jnp.concatenate(parts, axis=0)
        du_bc = du_bc * slope_of(conv_of(ext_bc, small_rows[0:CONV], small_rows[CONV : CONV + 1], info[...]))
        back_bc, grads_bc = conv_back(du_bc, ext_bc, small_rows[0:CONV], info[...])
        small[:, : 2 * STATE] = back_bc[HALO:].astype(BF)
        tail_bc[...] = back_bc[rows + HALO - 8 :]
        rim_bc[...] = back_bc[HALO - 8 : HALO]
        bc_grad[...] = grads_bc
        head_grad[...] = jnp.concatenate([bias_sum, dec_sum, jnp.zeros((6, 128), F32)], axis=0)


def ssd_backward(x_ext, signal, dy, misc, info, row_ids, wide_rows, small_rows, incoming, after):
    rows = signal.shape[0]
    chunks = rows // Q
    vm = pltpu.VMEM
    return pl.pallas_call(
        ssd_back_kernel,
        grid=(INNER // LANES,),
        in_specs=[
            column_spec(rows + HALO),
            column_spec(rows),
            column_spec(rows),
            whole_spec(misc.shape),
            whole_spec(info.shape),
            whole_spec(row_ids.shape),
            column_spec(8),
            whole_spec(small_rows.shape),
            column_spec(incoming.shape[0]),
            column_spec(after.shape[0]),
        ],
        out_specs=[
            column_spec(rows),
            column_spec(8),
            column_spec(8),
            column_spec(8),
            whole_spec((rows, 2 * STATE + 128)),
            whole_spec((8, 2 * STATE)),
            whole_spec((8, 2 * STATE)),
            whole_spec((8, 2 * STATE)),
            whole_spec((8, 128)),
        ],
        out_shape=[
            SDS((rows, INNER), BF),
            SDS((8, INNER), F32),
            SDS((8, INNER), F32),
            SDS((8, INNER), F32),
            SDS((rows, 2 * STATE + 128), BF),
            SDS((8, 2 * STATE), F32),
            SDS((8, 2 * STATE), F32),
            SDS((8, 2 * STATE), F32),
            SDS((8, 128), F32),
        ],
        scratch_shapes=[
            vm((rows + HALO, 2 * STATE), F32),
            vm((rows, 2 * STATE), BF),
            vm((chunks, STATE, Q), BF),
            vm((chunks, STATE, Q), BF),
            vm((chunks, Q, Q), F32),
            vm((rows, 128), F32),
            vm((rows, 128), F32),
            vm((rows, 128), F32),
            vm((rows, 128), F32),
            vm((chunks, 128, Q), F32),
            vm((rows, 128), F32),
            vm((rows, 128), F32),
            vm((8, 128), F32),
            vm((chunks, Q, Q), F32),
            vm((rows, 128), F32),
            vm((rows, 128), F32),
            vm((rows, 128), F32),
            vm((rows, 128), F32),
            vm((rows, 128), F32),
            vm((rows, 128), F32),
            vm((chunks, 128, Q), F32),
            vm((chunks, 8, 128), F32),
        ],
        compiler_params=params(),
        cost_estimate=cost(40e9, 15e6),
        name="ssd_backward",
    )(x_ext, signal, dy, misc, info, row_ids, wide_rows, small_rows, incoming, after)


def slot_of(piece, order):
    slot = 0
    for j, bit in enumerate(order[1:], 2):
        slot = slot + (((piece >> bit) & 1) << (len(order) - j))
    return slot


def weight_grad_body(where, own_z, next_z, own_o, next_o, own, other, *outs, cols, top):
    kind, piece = pl.program_id(0), pl.program_id(1)
    keep_a, send_a, keep_b, send_b = outs
    half = keep_a.shape[3]
    per = half // cols
    nt = 2 * per
    block = INNER // nt
    mine = jnp.where(kind == 0, own_z[0], own_o[0])
    theirs = jnp.where(kind == 0, next_z[0], next_o[0])
    parts = []
    for turn in range(nt):
        t = jnp.bitwise_xor(where[1], turn)
        at = pl.ds(pl.multiple_of(t * block, block), block)
        parts.append((mm(mine, own[0, :, at]) + mm(theirs, other[0, :, at])).astype(BF))
    for keep, send, order, chosen in (
        (keep_a, send_a, list(range(top + 1)), parts[:per]),
        (keep_b, send_b, list(range(top, -1, -1)), parts[per:]),
    ):
        slot = slot_of(piece, order)
        away = (piece >> order[0]) & 1

        @pl.when(away == 0)
        def _(keep=keep, slot=slot, chosen=chosen):
            for i, value in enumerate(chosen):
                keep[0, slot, :, i * cols : (i + 1) * cols] = value

        @pl.when(away == 1)
        def _(send=send, slot=slot, chosen=chosen):
            for i, value in enumerate(chosen):
                send[0, slot, :, i * cols : (i + 1) * cols] = value


def weight_grad(where, lefts, own, other, nt, cols):
    nw, k, rows = lefts[0].shape
    nm = nw // 2
    half = nt // 2 * cols
    left = pl.BlockSpec((1, k, rows), lambda q, r, s: (2 * jnp.bitwise_xor(r, s[0]) + s[2], 0, 0))
    right = pl.BlockSpec((1, rows, INNER), lambda q, r, s: (q, 0, 0))
    out = pl.BlockSpec((1, nm // 2, k, half), lambda q, r, s: (q, 0, 0, 0))
    return pl.pallas_call(
        functools.partial(weight_grad_body, cols=cols, top=nm.bit_length() - 2),
        grid_spec=pltpu.PrefetchScalarGridSpec(
            num_scalar_prefetch=1,
            grid=(2, nm),
            in_specs=[left] * 4 + [right] * 2,
            out_specs=[out] * 4,
        ),
        out_shape=[SDS((2, nm // 2, k, half), BF)] * 4,
        compiler_params=params(),
        cost_estimate=cost(8 * nm * k * rows * INNER, 12 * nm * k * INNER),
    )(where, *lefts, own, other)


def out_kernel(left, weight, tokens, out, acc):
    t = pl.program_id(0)
    depth = out.shape[1]
    part = mm(left[0], weight[...].reshape(depth, weight.shape[3]), NT)

    @pl.when(t == 0)
    def _():
        acc[...] = tokens[...].astype(F32) + part

    @pl.when(t > 0)
    def _():
        acc[...] += part

    @pl.when(t == pl.num_programs(0) - 1)
    def _():
        out[...] = acc[...].astype(BF)


def out_project(left, weights, which, tokens):
    rows, depth = tokens.shape
    nw, nt, k, _ = weights.shape
    block = INNER // nt
    return pl.pallas_call(
        out_kernel,
        grid=(nt,),
        in_specs=[
            pl.BlockSpec((1, rows, block), lambda t: (1, 0, t)),
            pl.BlockSpec((nw, 1, k, block), lambda t: (0, t, 0, which)),
            whole_spec(tokens.shape),
        ],
        out_specs=whole_spec(tokens.shape),
        out_shape=SDS(tokens.shape, BF),
        scratch_shapes=[pltpu.VMEM((rows, depth), F32)],
        compiler_params=params(),
        cost_estimate=cost(2 * rows * depth * INNER, 2 * depth * INNER),
        name="out_project",
    )(left, weights, tokens)


def gate_part_kernel(left, weight, out):
    t = pl.program_id(0)
    depth = out.shape[1]
    part = mm(left[0], weight[...].reshape(depth, weight.shape[3]), NT)

    @pl.when(t == 0)
    def _():
        out[...] = part

    @pl.when(t > 0)
    def _():
        out[...] += part


def gate_part(left, weights, which, depth):
    rows = left.shape[1]
    nw, nt, k, _ = weights.shape
    block = INNER // nt
    return pl.pallas_call(
        gate_part_kernel,
        grid=(nt,),
        in_specs=[
            pl.BlockSpec((1, rows, block), lambda t: (0, 0, t)),
            pl.BlockSpec((nw, 1, k, block), lambda t: (0, t, 0, which)),
        ],
        out_specs=whole_spec((rows, depth)),
        out_shape=SDS((rows, depth), F32),
        compiler_params=params(),
        cost_estimate=cost(2 * rows * depth * INNER, 2 * depth * INNER),
        name="gate_part",
    )(left, weights)


MESH = pl.DeviceIdType.MESH
SPLIT = 4
RATE = 2
LAG = 2


def remote(src, dst, send, recv, peer):
    return pltpu.make_async_remote_copy(src, dst, send, recv, device_id=peer, device_id_type=MESH)


def greet(peers):
    barrier = pltpu.get_barrier_semaphore()
    for peer in peers:
        pl.semaphore_signal(barrier, inc=1, device_id=peer, device_id_type=MESH)
    pl.semaphore_wait(barrier, len(peers))


class Line:
    def __init__(self, own, slot, send, recv, count):
        self.own, self.slot, self.send, self.recv, self.count = own, slot, send, recv, count
        self.t = lax.axis_index("tp")

    def each(self, distance, leaving, act):
        t, last = self.t, self.count - 1
        for way, sign in ((0, 1), (1, -1)):
            origin = t - sign * distance
            ahead = t + sign
            fine = (origin >= 0) & (origin <= last)
            if leaving:
                fine = fine & (ahead >= 0) & (ahead <= last)
            step = distance + 1 if leaving else distance

            @pl.when(fine)
            def _(origin=origin, ahead=ahead, way=way, step=step):
                there = self.slot(jnp.clip(origin, 0, last))
                source = self.own if leaving and distance == 0 else there
                act(
                    remote(source, there, self.send.at[way, step], self.recv.at[way, step], {"tp": jnp.clip(ahead, 0, last)})
                )

    def start(self, distance):
        self.each(distance, True, lambda copy: copy.start())

    def arrive(self, distance):
        self.each(distance, False, lambda copy: copy.wait_recv())

    def finish(self):
        for distance in range(self.count - 1):
            self.each(distance, True, lambda copy: copy.wait_send())


def gather_kernel(own, z_own, o_own, whole, z_line, o_line, send_x, recv_x, send_z, recv_z, send_o, recv_o, send_p, recv_p, send_c, recv_c, local):
    nw, nt = whole.shape[0], whole.shape[1]
    k = own.shape[0]
    w, t = lax.axis_index("wide"), lax.axis_index("tp")
    bits = nw.bit_length() - 2
    rows = k // SPLIT
    half = nt // 2
    greet(
        [{"tp": lax.rem(t + 1, nt)}, {"tp": lax.rem(t + nt - 1, nt)}]
        + [{"wide": jnp.bitwise_xor(w, 1 << b)} for b in range(bits + 1)]
    )
    part = lambda s: pl.ds(s * rows, rows)
    mine = []
    for s in range(SPLIT):
        mine.append(pltpu.make_async_copy(own.at[part(s)], whole.at[w, t, part(s)], local.at[0, s]))
        mine.append(pltpu.make_async_copy(z_own.at[part(s)], z_line.at[t, part(s)], local.at[1, s]))
        mine.append(pltpu.make_async_copy(o_own.at[part(s)], o_line.at[t, part(s)], local.at[2, s]))
    first = [Line(own.at[part(s)], lambda o, s=s: whole.at[w, o, part(s)], send_x.at[s], recv_x.at[s], nt) for s in range(SPLIT)]
    later = [Line(z_own.at[part(s)], lambda o, s=s: z_line.at[o, part(s)], send_z.at[s], recv_z.at[s], nt) for s in range(SPLIT)]
    later += [Line(o_own.at[part(s)], lambda o, s=s: o_line.at[o, part(s)], send_o.at[s], recv_o.at[s], nt) for s in range(SPLIT)]
    for line in first:
        line.start(0)
    for copy in mine:
        copy.start()
    sent, crossing, have, coming = [], [], {}, {}

    def exchange(index, h, s, mask, send, recv):
        at = (pl.ds(h * half, half), part(s))
        peer = {"wide": jnp.bitwise_xor(w, mask)}
        ref = whole.at[(index,) + at]
        copy = remote(ref, ref, send, recv, peer)
        copy.start()
        sent.append(copy)
        other = whole.at[(jnp.bitwise_xor(index, mask),) + at]
        return remote(other, other, send, recv, peer)

    def cross(index, h, s, number):
        crossing.append(exchange(index, h, s, 1, send_c.at[s, h, number], recv_c.at[s, h, number]))

    def begin(s, p):
        for h in range(2):
            mask = 2 << (p if h == 0 else bits - 1 - p)
            coming[s, p, h] = []
            for n, index in enumerate(list(have[s, h])):
                slot = (1 << p) - 1 + n
                copy = exchange(index, h, s, mask, send_p.at[s, h, slot], recv_p.at[s, h, slot])
                coming[s, p, h].append((jnp.bitwise_xor(index, mask), copy))

    hops = nt - 1
    pending = len(later)
    for tick in range(max(SPLIT + hops - 1 + bits, (pending + RATE - 1) // RATE + hops + LAG)):
        for d in range(hops, 0, -1):
            s = tick - d + 1
            if 0 <= s < SPLIT:
                first[s].arrive(d)
                if d < hops:
                    first[s].start(d)
        s = tick - hops + 1
        if 0 <= s < SPLIT:
            mine[3 * s].wait()
            for h in range(2):
                have[s, h] = [w]
            begin(s, 0)
            for h in range(2):
                cross(w, h, s, 0)
        for p in range(bits):
            s = tick - hops - p
            if 0 <= s < SPLIT:
                for h in range(2):
                    for index, copy in coming[s, p, h]:
                        copy.wait_recv()
                        have[s, h].append(index)
                if p + 1 < bits:
                    begin(s, p + 1)
                for h in range(2):
                    for n in range(1 << p):
                        cross(coming[s, p, h][n][0], h, s, (1 << p) + n)
        for d in range(hops, -1, -1):
            for n in range(RATE * (tick - LAG - d), RATE * (tick - LAG - d + 1)):
                if 0 <= n < pending:
                    if d:
                        later[n].arrive(d)
                    if d < hops:
                        later[n].start(d)
    for copy in crossing:
        copy.wait_recv()
    for s in range(SPLIT):
        mine[3 * s + 1].wait()
        mine[3 * s + 2].wait()
    for line in first + later:
        line.finish()
    for copy in sent:
        copy.wait_send()


def gather(own, z_own, o_own, nw, nt):
    k, cols = own.shape
    nm = nw // 2
    dma = pltpu.SemaphoreType.DMA
    return pl.pallas_call(
        gather_kernel,
        in_specs=[pl.BlockSpec(memory_space=pltpu.VMEM)] * 3,
        out_specs=[pl.BlockSpec(memory_space=pl.ANY)] * 3,
        out_shape=[SDS((nw, nt, k, cols), BF), SDS((nt,) + z_own.shape, BF), SDS((nt,) + o_own.shape, BF)],
        scratch_shapes=[dma((SPLIT, 2, nt))] * 6 + [dma((SPLIT, 2, nm))] * 4 + [dma((3, SPLIT))],
        compiler_params=params(32, collective_id=0, has_side_effects=True),
        cost_estimate=cost(60e9, 1e6),
        name="gather",
    )(own, z_own, o_own)


def span_shifts(span):
    reach = (DOC_MAX - 2) // span + 1
    size, steps = 1, []
    while 2 * size < reach:
        steps.append(size)
        size *= 2
    return steps, (1 + size if size < reach else 0)


STATE_PARTS = 4
EARLY = 1


def join(near, far):
    decay = near[STATE : STATE + 1].astype(F32)
    state = near[:STATE].astype(F32) + decay * far[:STATE].astype(F32)
    whole = near[STATE:].astype(F32) * far[STATE:].astype(F32)
    return jnp.concatenate([state, whole], axis=0).astype(BF)


class Passing:
    def __init__(self, source, target, send, recv, steps):
        nt = lax.axis_size("tp")
        count = lax.axis_size("wide") * nt
        place = lax.axis_index("wide") * nt + lax.axis_index("tp")
        ahead = place + steps
        behind = place - steps
        self.sends = (ahead < count) & (ahead >= 0)
        self.gets = (behind < count) & (behind >= 0)
        to = jnp.clip(ahead, 0, count - 1)
        self.peer = {"wide": to // nt, "tp": lax.rem(to, nt)}
        self.source, self.target, self.send, self.recv = source, target, send, recv

    def copy(self, j):
        width = INNER // STATE_PARTS
        at = pl.ds(j * width, width)
        return remote(self.source.at[:, at], self.target.at[:, at], self.send.at[j], self.recv.at[j], self.peer)

    def clear(self):
        @pl.when(jnp.logical_not(self.gets))
        def _():
            self.target[...] = jnp.zeros_like(self.target)

    def start(self, j):
        @pl.when(self.sends)
        def _():
            self.copy(j).start()

    def arrive(self, j):
        @pl.when(self.gets)
        def _():
            self.copy(j).wait_recv()

    def finish(self):
        @pl.when(self.sends)
        def _():
            for j in range(STATE_PARTS):
                self.copy(j).wait_send()


def shift_peers(shifts):
    nt = lax.axis_size("tp")
    count = lax.axis_size("wide") * nt
    place = lax.axis_index("wide") * nt + lax.axis_index("tp")
    peers = []
    for steps in shifts:
        for sign in (1, -1):
            to = lax.rem(place + count + sign * steps, count)
            peers.append({"wide": to // nt, "tp": lax.rem(to, nt)})
    return peers


def spread_kernel(state, z_line, z_first, o_line, o_first, incoming, z_whole, o_whole, *scratch, span):
    steps, far_step = span_shifts(span)
    levels = len(steps) + 1 + (1 if far_step else 0)
    buffers, scratch = scratch[:levels], scratch[levels:]
    helds, scratch = scratch[: len(steps)], scratch[len(steps) :]
    send_s, recv_s, send_p, recv_p, send_c, recv_c, local = scratch
    nw, nt = z_whole.shape[0], z_whole.shape[1]
    w = lax.axis_index("wide")
    bits = nw.bit_length() - 2
    shifts = sorted(set(steps) | {1} | ({far_step} if far_step else set()))
    width = INNER // STATE_PARTS

    def columns(j):
        return slice(j * width, (j + 1) * width)

    sources = [state] + list(helds)
    passes = [Passing(sources[i], buffers[i], send_s.at[i], recv_s.at[i], steps[i]) for i in range(len(steps))]
    last = sources[len(steps)]
    near = Passing(last, buffers[len(steps)], send_s.at[len(steps)], recv_s.at[len(steps)], 1)
    ends = [near]
    if far_step:
        ends.append(Passing(last, buffers[len(steps) + 1], send_s.at[len(steps) + 1], recv_s.at[len(steps) + 1], far_step))
    for item in passes + ends:
        item.clear()
    greet(shift_peers(shifts) + [{"wide": jnp.bitwise_xor(w, 1 << b)} for b in range(bits + 1)])
    for j in range(STATE_PARTS):
        (passes + ends)[0].start(j)
    if not passes and far_step:
        for j in range(STATE_PARTS):
            ends[1].start(j)

    sent, copies, crossing = [], [], []
    kinds = ((z_line, z_first, z_whole, [2 << p for p in range(bits)]), (o_line, o_first, o_whole, [2 << (bits - 1 - p) for p in range(bits)]))

    def exchange(source, whole, index, c, mask, send, recv):
        peer = {"wide": jnp.bitwise_xor(w, mask)}
        copy = remote(source, whole.at[index, c], send, recv, peer)
        copy.start()
        sent.append(copy)
        other = whole.at[jnp.bitwise_xor(index, mask), c]
        return remote(other, other, send, recv, peer)

    waiting = {}
    for kind, (line, first, whole, masks) in enumerate(kinds):
        waiting[kind] = {c: [(w, line.at[c]), (jnp.bitwise_xor(w, masks[0]), first.at[c])] for c in range(nt)}
    rounds = {}

    def begin(kind, p, c):
        whole, masks = kinds[kind][2], kinds[kind][3]
        rounds[kind, p, c] = [
            (jnp.bitwise_xor(index, masks[p]), exchange(source, whole, index, c, masks[p], send_p.at[kind, c, (1 << p) - 2 + n], recv_p.at[kind, c, (1 << p) - 2 + n]))
            for n, (index, source) in enumerate(waiting[kind][c])
        ]

    def cross(kind, index, source, c, number):
        crossing.append(exchange(source, kinds[kind][2], index, c, 1, send_c.at[kind, c, number], recv_c.at[kind, c, number]))

    def begin_some(some):
        for c in some:
            for kind in range(2):
                if bits > 1:
                    begin(kind, 1, c)

    begin_some(range(EARLY))
    for c in range(nt):
        for kind in range(2):
            for n, (index, source) in enumerate(waiting[kind][c]):
                copy = pltpu.make_async_copy(source, kinds[kind][2].at[index, c], local.at[kind, c, n])
                copy.start()
                copies.append(copy)
                cross(kind, index, source, c, n)
    for i, item in enumerate(passes):
        for j in range(STATE_PARTS):
            item.arrive(j)
            helds[i][:, columns(j)] = join(sources[i][:, columns(j)], buffers[i][:, columns(j)])
        following = passes[i + 1 : i + 2] or ends
        for j in range(STATE_PARTS):
            for other in following:
                other.start(j)
    begin_some(range(EARLY, nt))
    for p in range(1, bits):
        for c in range(nt):
            for kind in range(2):
                for n, (index, copy) in enumerate(rounds[kind, p, c]):
                    copy.wait_recv()
                    source = kinds[kind][2].at[index, c]
                    waiting[kind][c].append((index, source))
                    cross(kind, index, source, c, (1 << p) + n)
                if p + 1 < bits:
                    begin(kind, p + 1, c)
    for j in range(STATE_PARTS):
        for item in ends:
            item.arrive(j)
        value = buffers[len(steps)][:, columns(j)]
        if far_step:
            value = join(value, buffers[len(steps) + 1][:, columns(j)])
        incoming[:, columns(j)] = value
    for copy in crossing:
        copy.wait_recv()
    for copy in copies:
        copy.wait()
    for item in passes + ends:
        item.finish()
    for copy in sent:
        copy.wait_send()


def spread(state, z_line, z_first, o_line, o_first, nw, span):
    nt, k, cols = z_line.shape
    nm = nw // 2
    steps, far_step = span_shifts(span)
    levels = len(steps) + 1 + (1 if far_step else 0)
    dma = pltpu.SemaphoreType.DMA
    vmem, anywhere = pl.BlockSpec(memory_space=pltpu.VMEM), pl.BlockSpec(memory_space=pl.ANY)
    return pl.pallas_call(
        functools.partial(spread_kernel, span=span),
        in_specs=[vmem] * 5,
        out_specs=[vmem, anywhere, anywhere],
        out_shape=[SDS(state.shape, BF), SDS((nw, nt, k, cols), BF), SDS((nw, nt, k, cols), BF)],
        scratch_shapes=[pltpu.VMEM(state.shape, BF)] * (levels + len(steps))
        + [dma((levels, STATE_PARTS))] * 2
        + [dma((2, nt, max(nm - 2, 1)))] * 2
        + [dma((2, nt, nm))] * 2
        + [dma((2, nt, 2))],
        compiler_params=params(48, collective_id=1, has_side_effects=True),
        cost_estimate=cost(60e9, 1e6),
        name="spread",
    )(state, z_line, z_first, o_line, o_first)


ROW_PARTS = 2
STEP_LAG = 4
SUM_GAP = 2


class Unit:
    def __init__(self, order, first, keep, kept, sends, recvs, send_sem, recv_sem, done):
        self.order, self.first, self.keep, self.kept, self.sends, self.recvs = order, first, keep, kept, sends, recvs
        self.send_sem, self.recv_sem, self.done = send_sem, recv_sem, done

    def copy(self, p):
        peer = {"wide": jnp.bitwise_xor(lax.axis_index("wide"), 2 << self.order[p])}
        return remote(self.sends[p], self.recvs[p], self.send_sem.at[p], self.recv_sem.at[p], peer)

    def merge(self, p):
        self.copy(p).wait_recv()
        keep = self.keep if p == self.first else self.kept
        count = self.recvs[p].shape[0]
        if p == len(self.order) - 1:
            self.done(keep[0].astype(F32) + self.recvs[p][0].astype(F32))
            return
        for i in range(count // 2):
            self.kept[i] = keep[i].astype(F32) + self.recvs[p][i].astype(F32)
        for i in range(count // 2, count):
            self.sends[p + 1][i - count // 2] = (keep[i].astype(F32) + self.recvs[p][i].astype(F32)).astype(BF)


def finish_kernel(
    dx, small, tail, tail_bc, rim, rim_bc, left, left_next, keep_a, send_a, keep_b, send_b, wx, so_far, tokens, cot, gain, conv_grad, gate_sums, bc_grad, head_grad,
    x_out, bc_out, dt_out, z_out, o_out, grad, sums_out, gain_out,
    dxs, dxn, smalls, smalln, rims, rims_bc, extra, weights,
    keep_x, send_x, recv_x, turn_x, own_x, got_x, kept_zo, send_zo, recv_zo, turn_zo, own_zo, got_zo, sums_to, sums_from, gain_to, gain_from,
    sem_flip, sem_rim, sem_local, sem_xs, sem_xr, sem_zs, sem_zr, sem_txs, sem_txr, sem_tzs, sem_tzr, sem_ss, sem_sr, sem_gs, sem_gr,
):
    nw, nt, k, cols = wx.shape
    rows, depth = tokens.shape
    block = INNER // nt
    nm = nw // 2
    bits = nm.bit_length() - 1
    per = nt // 2
    w, rank = lax.axis_index("wide"), lax.axis_index("tp")
    chip, core = w // 2, lax.rem(w, 2)
    count = nw * nt
    place = w * nt + rank
    before, behind = lax.rem(place + count - 1, count), lax.rem(place + 1, count)
    sibling = {"wide": jnp.bitwise_xor(w, 1)}
    tp_bits = nt.bit_length() - 1
    across = [{"tp": jnp.bitwise_xor(rank, 1 << b)} for b in range(tp_bits)]
    has_next = place < count - 1
    has_last = place > 0
    to_last = {"wide": before // nt, "tp": lax.rem(before, nt)}
    to_next = {"wide": behind // nt, "tp": lax.rem(behind, nt)}
    orders = (list(range(bits)), list(range(bits - 1, -1, -1)))

    @pl.when(jnp.logical_not(has_next))
    def _():
        rims[...] = jnp.zeros_like(rims)
        rims_bc[...] = jnp.zeros_like(rims_bc)

    greet([sibling, to_last, to_next] + across + [{"wide": jnp.bitwise_xor(w, 2 << b)} for b in range(bits)])
    rim_copies = [
        remote(rim, rims, sem_rim.at[0], sem_rim.at[1], to_last),
        remote(rim_bc, rims_bc, sem_rim.at[2], sem_rim.at[3], to_last),
    ]

    @pl.when(has_last)
    def _():
        for copy in rim_copies:
            copy.start()

    started = []

    def start(copy):
        copy.start()
        started.append(copy)

    body = pl.ds(0, rows - HALO)
    flips, locals_ = [], []
    order_of_turns = [turn for pair in zip(range(per - 1, -1, -1), range(nt - 1, per - 1, -1)) for turn in pair]
    small_copy = remote(small.at[body], smalln.at[body], sem_flip.at[0, 0], sem_flip.at[1, 0], sibling)
    start(small_copy)
    own_small = pltpu.make_async_copy(small, smalls, sem_local.at[nt])
    own_small.start()
    for n, turn in enumerate(order_of_turns):
        at = pl.ds(pl.multiple_of(jnp.bitwise_xor(rank, turn) * block, block), block)
        flips.append(remote(dx.at[body, at], dxn.at[body, at], sem_flip.at[0, 1 + n], sem_flip.at[1, 1 + n], sibling))
        start(flips[n])
        locals_.append(pltpu.make_async_copy(dx.at[:, at], dxs.at[:, at], sem_local.at[n]))
        locals_[n].start()
    initial = pltpu.make_async_copy(so_far, grad, sem_local.at[nt + 1])
    initial.start()

    def weight_copy(t):
        return pltpu.make_async_copy(wx.at[:, t], weights.at[t % 2], sem_local.at[nt + 2 + t % 2])

    weight_copy(0).start()

    def level(turn):
        return (turn & -turn).bit_length() - 1

    def finished(total, turn, own, leaving):
        if turn % 2:
            leaving[turn] = total.astype(BF)
        else:
            own[turn // 2] = total

    units_zo = []
    for q in range(2):
        for h, (keep, send) in enumerate(((keep_a, send_a), (keep_b, send_b))):
            def done(total, q=q, h=h):
                for i in range(per):
                    finished(total[:, i * block : (i + 1) * block], h * per + i, own_zo.at[q], turn_zo.at[q])

            number = 2 * q + h
            sends = {p: (send.at[q] if p == 1 else send_zo.at[number, pl.ds(0, nm >> (p + 1))]) for p in range(1, bits)}
            recvs = {p: recv_zo.at[number, pl.ds((nm >> 1) - (nm >> p), nm >> (p + 1))] for p in range(1, bits)}
            units_zo.append(
                Unit(orders[h], 1, keep.at[q], kept_zo.at[number], sends, recvs, sem_zs.at[number], sem_zr.at[number], done)
            )
    for unit in units_zo:
        start(unit.copy(1))

    part = k // ROW_PARTS
    units_x = []
    for s in range(ROW_PARTS):
        for turn in order_of_turns:
            number = len(units_x)

            def done(total, turn=turn, s=s):
                at = pl.ds(s * part, part)
                finished(total, turn, own_x.at[:, at], turn_x.at[:, at])

            sends = {p: send_x.at[number, pl.ds(nm - (nm >> p), nm >> (p + 1))] for p in range(bits)}
            recvs = {p: recv_x.at[number, pl.ds(nm - (nm >> p), nm >> (p + 1))] for p in range(bits)}
            unit = Unit(
                orders[0 if turn < per else 1], 0, keep_x.at[number], keep_x.at[number], sends, recvs, sem_xs.at[number], sem_xr.at[number], done
            )
            unit.turn, unit.s = turn, s
            units_x.append(unit)

    for copy in locals_:
        copy.wait()
    own_small.wait()

    @pl.when(has_next)
    def _():
        for copy in rim_copies:
            copy.wait_recv()

    last = slice(rows - HALO, rows)
    old = dxs[last].astype(F32)
    dxs[last] = jnp.concatenate([old[: HALO - 8], tail[...] + rims[...]], axis=0).astype(BF)
    old = smalls[last].astype(F32)
    fixed = jnp.concatenate([old[: HALO - 8, : 2 * STATE], tail_bc[...] + rims_bc[...]], axis=0)
    smalls[last] = jnp.concatenate([fixed, old[:, 2 * STATE :]], axis=1).astype(BF)

    end = pl.ds(rows - HALO, HALO)
    ends = [
        remote(smalls.at[end], smalln.at[end], sem_flip.at[0, nt + 1], sem_flip.at[1, nt + 1], sibling),
        remote(dxs.at[end], dxn.at[end], sem_flip.at[0, nt + 2], sem_flip.at[1, nt + 2], sibling),
    ]

    def members(order):
        found = []
        for index in range(nm // 2):
            r = 0
            for j, bit in enumerate(order[1:], 2):
                r |= ((index >> (len(order) - j)) & 1) << bit
            found.append(r)
        return found

    def compute(unit):
        order = unit.order
        kept = members(order)
        away = [r | (1 << order[0]) for r in kept]
        t = jnp.bitwise_xor(rank, unit.turn)
        at = pl.ds(pl.multiple_of(t * block, block), block)
        at_rows = pl.ds(unit.s * part, part)
        chips = [jnp.bitwise_xor(chip, r) for r in away + kept]
        places = [2 * m + core for m in chips]
        mine = jnp.concatenate([left[m, at_rows, :] for m in places], axis=0)
        theirs = jnp.concatenate([left_next[m, at_rows, :] for m in places], axis=0)
        result = mm(mine, dxs[:, at]) + mm(theirs, dxn[:, at])
        pick = select_columns(t, HEADS // nt, 2 * STATE // nt, cols - block, 2 * STATE + 128)
        picked = mm(jnp.concatenate([extra[m, at_rows, :] for m in chips], axis=0), pick, NT)
        value = jnp.concatenate([result, picked], axis=1)
        for i in range(nm // 2):
            unit.sends[0][i] = value[i * part : (i + 1) * part].astype(BF)
            unit.keep[i] = value[(nm // 2 + i) * part : (nm // 2 + i + 1) * part]

    def row_part(t):
        weight_copy(t).wait()
        if t + 1 < nt:
            weight_copy(t + 1).start()
        if t == 0:
            initial.wait()
        pick = select_columns(t, HEADS // nt, 2 * STATE // nt, cols - block, 2 * STATE + 128)
        extra_columns = mm(smalls[...], pick, NT).astype(BF)
        values = jnp.concatenate([dxs[:, t * block : (t + 1) * block], extra_columns], axis=1)
        grad[...] += mm(values, weights[t % 2].reshape(depth, cols), NT)

    def row_end():
        raw = tokens[...].astype(F32)
        inv = lax.rsqrt(jnp.mean(raw * raw, axis=-1, keepdims=True) + EPS)
        unit = raw * inv
        d_normed = grad[...]
        gain_grad = jnp.sum(d_normed * unit, axis=0, keepdims=True)
        gain_to[0] = gain_grad
        d_unit = d_normed * gain[...]
        grad[...] = cot[...].astype(F32) + inv * (d_unit - unit * jnp.mean(d_unit * unit, axis=-1, keepdims=True))

    partners = [{"wide": jnp.bitwise_xor(w, 1 << b)} for b in range(bits + 1)]
    partners += across

    def sum_start():
        sums_to[0, 0:5] = conv_grad[0:5]
        sums_to[0, 5:7] = gate_sums[0:2]
        for i in range(CONV + 1):
            sums_to[0, 7:8, i * 2 * STATE : (i + 1) * 2 * STATE] = bc_grad[i : i + 1]
        at = (CONV + 1) * 2 * STATE
        for i in range(2):
            sums_to[0, 7:8, at + i * 128 : at + (i + 1) * 128] = head_grad[i : i + 1]
        sums_to[0, 7:8, at + 256 :] = jnp.zeros((1, INNER - at - 256), F32)

    def butterfly(to, source, out, send, recv):
        def copy(i):
            return remote(to.at[i], source.at[i], send.at[i], recv.at[i], partners[i])

        def join(i):
            copy(i).wait_recv()
            total = to[i] + source[i]
            if i + 1 < len(partners):
                to[i + 1] = total
            else:
                out[...] = total

        return copy, join

    flies = [butterfly(sums_to, sums_from, sums_out, sem_ss, sem_sr), butterfly(gain_to, gain_from, gain_out, sem_gs, sem_gr)]

    def parcels(unit):
        if unit in units_zo:
            number = units_zo.index(unit)
            q, h = number // 2, number % 2
            for turn in range((h + 1) * per - 1, h * per - 1, -1):
                yield turn, own_zo.at[q], turn_zo.at[q], got_zo.at[q], sem_tzs.at[q], sem_tzr.at[q]
        else:
            at = pl.ds(unit.s * part, part)
            yield unit.turn, own_x.at[:, at], turn_x.at[:, at], got_x.at[:, :, at], sem_txs.at[unit.s], sem_txr.at[unit.s]

    def joined(turn, own, got, send, recv, upto):
        total = own[turn // 2]
        for b in range(upto):
            source = got.at[turn // 2, b]
            remote(source, source, send.at[turn], recv.at[turn // 2, b], across[b]).wait_recv()
            total = total + source[...].astype(F32)
        return total

    def pass_on(unit, odd):
        found = []
        for turn, own, leaving, got, send, recv in parcels(unit):
            if turn == 0 or bool(turn % 2) != odd:
                continue
            b = level(turn)
            if b:
                leaving[turn] = joined(turn, own, got, send, recv, b).astype(BF)
            target = turn ^ (1 << b)
            found.append(remote(leaving.at[turn], got.at[target // 2, b], send.at[turn], recv.at[target // 2, b], across[b]))
        return found

    side = [functools.partial(row_part, t) for t in range(nt)] + [row_end]
    total_x = len(units_x)
    steps = total_x + STEP_LAG * bits
    first_job = 1
    fly_steps = [
        [1 + SUM_GAP * i for i in range(len(partners) + 1)],
        [first_job + len(side) + i for i in range(len(partners) + 1)],
    ]
    steps = max(steps, fly_steps[0][-1], fly_steps[1][-1])
    later = {step: [] for step in range(steps + 2)}
    for step in range(steps + 1):
        ready = []
        leaving_now = [copy for unit in later[step] for copy in pass_on(unit, False)]
        if step < total_x:
            if step == 0:
                for copy in ends:
                    start(copy)
                small_copy.wait_recv()
                for copy in ends:
                    copy.wait_recv()
                small_all = [smalls[...], smalln[...]]
                for m in range(nm):
                    extra[m] = (mm(left[2 * m + core], small_all[0]) + mm(left_next[2 * m + core], small_all[1])).astype(BF)
            if step < len(flips):
                flips[step].wait_recv()
            compute(units_x[step])
        for p in range(bits - 1, -1, -1):
            u = step - STEP_LAG * (p + 1)
            if 0 <= u < total_x:
                units_x[u].merge(p)
                ready.append((units_x[u], p + 1))
        for p in range(bits - 1, 0, -1):
            u = step - 1 - STEP_LAG * (p - 1)
            if 0 <= u < len(units_zo):
                units_zo[u].merge(p)
                ready.append((units_zo[u], p + 1))
        if step == 0:
            sum_start()
        job = step - first_job
        if 0 <= job < len(side):
            side[job]()
        leaving_sums = []
        for (copy, join), when in zip(flies, fly_steps):
            if step in when:
                i = when.index(step)
                if i:
                    join(i - 1)
                if i < len(partners):
                    leaving_sums.append(copy(i))
        if step < total_x:
            start(units_x[step].copy(0))
        for unit, p in ready:
            if p < bits:
                start(unit.copy(p))
            else:
                for copy in pass_on(unit, True):
                    start(copy)
                later[step + 1].append(unit)
        for copy in leaving_now:
            start(copy)
        for copy in leaving_sums:
            start(copy)
    zo_total = []
    for q in range(2):
        unit = units_zo[2 * q]
        for turn, own, leaving, got, send, recv in parcels(unit):
            if turn == 0:
                zo_total.append(joined(0, own, got, send, recv, tp_bits))
    z_out[...] = zo_total[0]
    o_out[...] = zo_total[1].T
    for unit in units_x:
        for turn, own, leaving, got, send, recv in parcels(unit):
            if turn == 0:
                total = joined(0, own, got, send, recv, tp_bits)
                at = slice(unit.s * part, (unit.s + 1) * part)
                x_out[at] = total[:, :block]
                bc_out[at] = total[:, block : block + bc_out.shape[1]]
                dt_out[at] = total[:, block + bc_out.shape[1] : block + bc_out.shape[1] + dt_out.shape[1]]
    for copy in started:
        copy.wait_send()

    @pl.when(has_last)
    def _():
        for copy in rim_copies:
            copy.wait_send()


def finish(dx, small, tail, tail_bc, rim, rim_bc, left, left_next, keep_a, send_a, keep_b, send_b, wx, so_far, tokens, cot, gain, conv_grad, gate_sums, bc_grad, head_grad):
    nw, nt, k, cols = wx.shape
    rows, depth = tokens.shape
    nm = nw // 2
    bits = nm.bit_length() - 1
    block = INNER // nt
    half = nt // 2 * block
    part = k // ROW_PARTS
    units = ROW_PARTS * nt
    tp_bits = nt.bit_length() - 1
    partners = bits + 1 + tp_bits
    dma, vm = pltpu.SemaphoreType.DMA, pltpu.VMEM
    vmem, anywhere = pl.BlockSpec(memory_space=pltpu.VMEM), pl.BlockSpec(memory_space=pl.ANY)
    return pl.pallas_call(
        finish_kernel,
        in_specs=[anywhere, anywhere] + [vmem] * 6 + [vmem] * 4 + [anywhere, anywhere] + [vmem] * 7,
        out_specs=[vmem] * 8,
        out_shape=[
            SDS((k, block), F32), SDS((k, 2 * STATE // nt), F32), SDS((k, HEADS // nt), F32),
            SDS((k, block), F32), SDS((block, k), F32), SDS((rows, depth), F32), SDS((8, INNER), F32), SDS((1, depth), F32),
        ],
        scratch_shapes=[
            vm((rows, INNER), BF), vm((rows, INNER), BF), vm(small.shape, BF), vm(small.shape, BF),
            vm((8, INNER), F32), vm((8, 2 * STATE), F32), vm((nm, k, small.shape[1]), BF), vm((2, nw, k, cols), BF),
            vm((units, nm // 2, part, cols), F32), vm((units, nm - 1, part, cols), BF), vm((units, nm - 1, part, cols), BF),
            vm((nt, k, cols), BF), vm((nt // 2, k, cols), F32), vm((nt // 2, tp_bits, k, cols), BF),
            vm((4, nm // 4, k, half) if bits > 2 else (4, 1, 8, 128), F32),
            vm((4, nm // 8, k, half) if bits > 2 else (4, 1, 16, 128), BF),
            vm((4, max(nm // 2 - 1, 1), k, half), BF),
            vm((2, nt, k, block), BF), vm((2, nt // 2, k, block), F32), vm((2, nt // 2, tp_bits, k, block), BF),
            vm((partners, 8, INNER), F32), vm((partners, 8, INNER), F32), vm((partners, 1, depth), F32), vm((partners, 1, depth), F32),
            dma((2, nt + 3)), dma((4,)), dma((nt + 4,)),
            dma((units, bits)), dma((units, bits)), dma((4, bits)), dma((4, bits)),
            dma((ROW_PARTS, nt)), dma((ROW_PARTS, nt // 2, tp_bits)), dma((2, nt)), dma((2, nt // 2, tp_bits)),
            dma((partners,)), dma((partners,)), dma((partners,)), dma((partners,)),
        ],
        compiler_params=params(63, collective_id=2, has_side_effects=True),
        cost_estimate=cost(60e9, 1e6),
        name="finish",
    )(dx, small, tail, tail_bc, rim, rim_bc, left, left_next, keep_a, send_a, keep_b, send_b, wx, so_far, tokens, cot, gain, conv_grad, gate_sums, bc_grad, head_grad)


BOTH = ("wide", "tp")


def shift(value, steps):
    count = lax.axis_size("wide") * lax.axis_size("tp")
    first, last = max(0, -steps), min(count, count - steps)
    return lax.ppermute(value, BOTH, [(i, i + steps) for i in range(first, last)])


def carry_states(own, span, direction):
    reach = (DOC_MAX - 2) // span + 1
    held, size = own, 1
    while 2 * size < reach:
        other = shift(held, direction * size)
        held = combine(held, other)
        size *= 2
    near = shift(held, direction)
    if size >= reach:
        return near
    far = shift(held, direction * (1 + size))
    return combine(near, far)


def combine(near, far):
    decay = near[STATE : STATE + 1].astype(F32)
    state = near[:STATE].astype(F32) + decay * far[:STATE].astype(F32)
    whole = near[STATE:].astype(F32) * far[STATE:].astype(F32)
    return jnp.concatenate([state, whole], axis=0).astype(BF)


def flip(value, mask):
    return lax.ppermute(value, "wide", [(i, i ^ mask) for i in range(lax.axis_size("wide"))])


def add(a, b):
    return (a.astype(F32) + b.astype(F32)).astype(BF)


def first_exchange(keep_a, send_a, keep_b, send_b):
    top = keep_a.shape[1].bit_length() - 1
    size = keep_a.shape[1] // 2
    got_a, got_b = flip(send_a, 2), flip(send_b, 2 << top)
    result = []
    for keep, got in ((keep_a, got_a), (keep_b, got_b)):
        result += [add(keep[:, :size], got[:, :size]), add(keep[:, size:], got[:, size:])]
    return result


def per_device(
    tokens, segment_ids, out_cotangent, norm_gain, z_weight, x_weight, bc_weight, dt_weight, x_conv, x_bias,
    bc_conv, bc_bias, dt_bias, decay_log, skip_gain, gate_gain, out_weight,
):
    nw, nt = lax.axis_size("wide"), lax.axis_size("tp")
    rank = lax.axis_index("tp")
    rows, depth = tokens.shape
    k = depth // nw
    block = INNER // nt
    small = jnp.concatenate([bc_weight, dt_weight], axis=1)
    small = jnp.pad(small, ((0, 0), (0, 128 - small.shape[1])))
    own_x = jnp.concatenate([x_weight, small], axis=1)
    wx, z_line, o_line = gather(own_x, z_weight, out_weight.T, nw, nt)
    z_first, o_first = flip(z_line, 2), flip(o_line, nw // 2)

    own_ids = lax.dynamic_slice_in_dim(segment_ids, rank * rows, rows, 0)
    halo_rows = shift(tokens[rows - HALO :], 1)
    halo_ids = (shift(own_ids[rows - 128 :] + 1, 1) - 1).astype(F32)[None, :]
    row_ids = jnp.broadcast_to(own_ids.astype(F32)[None, :], (8, rows))

    def padded(v, width):
        v = v if v.ndim == 2 else v[None, :]
        return jnp.pad(v, ((0, 0), (0, width - v.shape[1])))

    wide_rows = jnp.concatenate(
        [x_conv, x_bias[None, :], jnp.repeat(skip_gain, HEAD_DIM)[None, :], gate_gain[None, :], x_bias[None, :]], axis=0
    ).astype(F32)
    small_rows = jnp.concatenate(
        [bc_conv, bc_bias[None, :], padded(dt_bias, 2 * STATE), padded(decay_log, 2 * STATE), bc_bias[None, :]], axis=0
    ).astype(F32)
    in_gain = norm_gain.astype(F32)[None, :]

    x_ext, misc, normed_ext, normed_t, info = project(tokens, halo_rows, in_gain, row_ids, halo_ids, wx)
    signal, y, own_state, ent, bc = ssd_forward(
        x_ext, misc, info, row_ids, wide_rows, small_rows
    )
    incoming, wz, wo = spread(own_state, z_line, z_first, o_line, o_first, nw, rows)
    core = lax.rem(lax.axis_index("wide"), 2)
    where = jnp.stack([lax.axis_index("wide") // 2, rank, core]).astype(jnp.int32)
    normed_next = flip(normed_t, 1).reshape(nw, k, rows)
    (gate,) = plain(normed_ext, wz, HALO, False)
    dno, cot_t = plain(out_cotangent, wo, 0, True)
    cot_next = flip(cot_t, 1).reshape(nw, k, rows)
    left = [normed_t.reshape(nw, k, rows), normed_next, cot_t.reshape(nw, k, rows), cot_next]
    pair, dy, adjoint, sums = gate_norm(y, signal, gate, dno, bc, ent, incoming, wide_rows)
    own_adjoint = jnp.concatenate([adjoint, own_state[STATE:]], axis=0)
    after = carry_states(own_adjoint, rows, -1)
    pair_next = flip(pair, 1)
    block_out = out_project(pair, wo, 0, tokens)
    so_far = gate_part(pair, wz, 0, depth)
    zo = weight_grad(where, left, pair, pair_next, nt, block)
    zo = first_exchange(*zo)
    dx, tail, rim, conv_grad, small_grad, tail_bc, rim_bc, bc_grad, head_grad = ssd_backward(
        x_ext, signal, dy, misc, info, row_ids, wide_rows, small_rows, incoming, after
    )
    x_weight_grad, bc_weight_grad, dt_weight_grad, z_weight_grad, out_weight_grad, grad_x, small_sums, gain_sum = finish(
        dx, small_grad, tail, tail_bc, rim, rim_bc, left[0], left[1], *zo, wx, so_far, tokens, out_cotangent, in_gain,
        conv_grad, sums, bc_grad, head_grad,
    )
    wide_bc = (CONV + 1) * 2 * STATE
    bc_all = small_sums[7, :wide_bc].reshape(CONV + 1, 2 * STATE)
    head_all = small_sums[7, wide_bc : wide_bc + 256]
    return (
        block_out,
        grad_x,
        gain_sum[0],
        z_weight_grad,
        x_weight_grad,
        bc_weight_grad,
        dt_weight_grad,
        small_sums[:CONV],
        small_sums[CONV],
        bc_all[:CONV],
        bc_all[CONV],
        head_all[:HEADS],
        head_all[128 : 128 + HEADS],
        small_sums[6].reshape(HEADS, HEAD_DIM).sum(axis=1),
        small_sums[5],
        out_weight_grad,
    )


def solution(mesh):
    rows, shard, out_shard = P(("wide", "tp"), None), P("wide", "tp"), P("tp", "wide")
    return jax.shard_map(
        per_device,
        mesh=mesh,
        in_specs=(rows, P("wide"), rows, P(), shard, shard, shard, shard) + (P(),) * 8 + (out_shard,),
        out_specs=(rows, rows, P(), shard, shard, shard, shard) + (P(),) * 8 + (out_shard,),
        check_vma=False,
    )
```

```python
import functools

import jax
import jax.numpy as jnp
from jax import lax
from jax.experimental import pallas as pl
from jax.experimental.pallas import tpu as pltpu
from jax.sharding import PartitionSpec as P


HEADS = 48
HEAD_DIM = 64
STATE = 128
CONV = 4
INNER = 3072
DOC_MAX = 2048
EPS = 1e-05
HALO = 16
Q = 128
LANES = 256
GROUP_HEADS = LANES // HEAD_DIM
F32 = jnp.float32
BF = jnp.bfloat16
HIGH = lax.Precision.HIGHEST
NN = ((1,), (0,))
NT = ((1,), (1,))
TN = ((0,), (0,))
SDS = jax.ShapeDtypeStruct


def mm(a, b, dims=NN, precision=None):
    return lax.dot_general(a, b, (dims, ((), ())), precision=precision, preferred_element_type=F32)


def sigmoid(v):
    return 1.0 / (1.0 + jnp.exp(-v))


def iota(shape, axis):
    return lax.broadcasted_iota(jnp.int32, shape, axis)


def params(vmem_mb=60, **kw):
    return pltpu.CompilerParams(vmem_limit_bytes=vmem_mb * 1024 * 1024, **kw)


def cost(flops, read):
    return pl.CostEstimate(flops=int(flops), bytes_accessed=int(read), transcendentals=0)


def marks_of(ids, halo_ids):
    rows = ids.shape[1]
    here = ids.T
    row, lane = iota(here.shape, 0), iota(here.shape, 1)
    before = [jnp.broadcast_to(halo_ids[0:1, 128 - j : 129 - j], here.shape) for j in range(1, CONV)]
    same = []
    for k in range(1, CONV):
        past = pltpu.roll(here, k, 0)
        for r in range(k):
            past = jnp.where(row == r, before[k - 1 - r], past)
        same.append(past == here)
    firsts, lasts = [], []
    for c in range(rows // Q):
        end = jnp.broadcast_to(here[c * Q + Q - 1 : c * Q + Q, 0:1], (Q, 8))
        start = jnp.broadcast_to(here[c * Q - 1 : c * Q, 0:1], (Q, 8)) if c else before[0][:Q]
        firsts.append(start)
        lasts.append(end)
    first, last = jnp.concatenate(firsts, axis=0), jnp.concatenate(lasts, axis=0)
    marks = same + [None, here == first, here == last, here == before[0], first == last]
    result = here
    for i, mark in enumerate(marks):
        if mark is not None:
            result = jnp.where(lane == i, jnp.where(mark, 1.0, 0.0), result)
    return result


def proj_kernel(tok, halo, gain, ids, weight, x_out, misc_out, normed, turned, info):
    @pl.when(pl.program_id(0) == 0)
    def _():
        for rows, at in ((halo, slice(0, HALO)), (tok, slice(HALO, None))):
            raw = rows[...].astype(F32)[: rows.shape[0] if rows is tok else HALO]
            inv = lax.rsqrt(jnp.mean(raw * raw, axis=-1, keepdims=True) + EPS)
            normed[at] = (raw * inv * gain[...]).astype(BF)
        turned[...] = normed[HALO:].T
        info[...] = marks_of(ids[...], halo[HALO:, 0:128].astype(F32)[0:1] - 1.0)

    depth, cols = tok.shape[1], weight.shape[3]
    result = mm(normed[...], weight[...].reshape(depth, cols))
    block = x_out.shape[1]
    x_out[...] = result[:, :block].astype(BF)
    misc_out[0] = result[:, block:].astype(BF)


def project(tokens, halo_rows, gain, ids, weights):
    rows, depth = tokens.shape
    rows = rows + HALO
    nw, nt, k, cols = weights.shape
    block = INNER // nt
    misc = cols - block
    return pl.pallas_call(
        proj_kernel,
        grid=(nt,),
        in_specs=[
            whole_spec(tokens.shape),
            whole_spec(halo_rows.shape),
            whole_spec((1, depth)),
            whole_spec(ids.shape),
            pl.BlockSpec((nw, 1, k, cols), lambda t: (0, t, 0, 0)),
        ],
        out_specs=[
            pl.BlockSpec((rows, block), lambda t: (0, t)),
            pl.BlockSpec((1, rows, misc), lambda t: (t, 0, 0)),
            pl.BlockSpec((rows, depth), lambda t: (0, 0)),
            pl.BlockSpec((depth, rows - HALO), lambda t: (0, 0)),
            whole_spec((rows - HALO, 8)),
        ],
        out_shape=[
            SDS((rows, INNER), BF),
            SDS((nt, rows, misc), BF),
            SDS((rows, depth), BF),
            SDS((depth, rows - HALO), BF),
            SDS((rows - HALO, 8), F32),
        ],
        compiler_params=params(),
        cost_estimate=cost(2 * rows * depth * nt * cols, 2 * depth * nt * cols),
        name="project",
    )(tokens, halo_rows, gain, ids, weights)


def plain_kernel(left, weight, out, *turned, first):
    depth, cols = left.shape[1], weight.shape[3]
    if turned:
        @pl.when(pl.program_id(0) == 0)
        def _():
            turned[0][...] = left[...].T

    out[...] = mm(left[first:], weight[...].reshape(depth, cols)).astype(BF)


def plain(left, weights, first, turned):
    rows, depth = left.shape
    rows = rows - first
    nw, nt, k, _ = weights.shape
    block = INNER // nt
    out_specs = [pl.BlockSpec((rows, block), lambda t: (0, t))]
    out_shape = [SDS((rows, INNER), BF)]
    if turned:
        out_specs.append(pl.BlockSpec((depth, rows), lambda t: (0, 0)))
        out_shape.append(SDS((depth, rows), BF))
    return pl.pallas_call(
        functools.partial(plain_kernel, first=first),
        grid=(nt,),
        in_specs=[
            pl.BlockSpec(left.shape, lambda t: (0, 0)),
            pl.BlockSpec((nw, 1, k, block), lambda t: (0, t, 0, 0)),
        ],
        out_specs=out_specs,
        out_shape=out_shape,
        compiler_params=params(),
        cost_estimate=cost(2 * rows * depth * INNER, 2 * depth * INNER),
    )(left, weights)


def select_columns(t, heads, bc_cols, rows, cols):
    lane, col = iota((rows, cols), 0), iota((rows, cols), 1)
    first = (lane < bc_cols) & (col == lane + t * bc_cols)
    second = (
        (lane >= bc_cols)
        & (lane < bc_cols + heads)
        & (col == lane - bc_cols + 2 * STATE + t * heads)
    )
    return jnp.where(first | second, 1.0, 0.0).astype(BF)


def conv_of(ext, taps, bias, info):
    total = bias + taps[0:1] * ext[HALO:]
    for k in range(1, CONV):
        total = total + taps[k : k + 1] * pltpu.roll(ext, k, 0)[HALO:] * info[:, k - 1 : k]
    return total


def head_lanes(group, lanes):
    return jnp.where(
        iota((128, lanes), 0) == group * GROUP_HEADS + iota((128, lanes), 1) // HEAD_DIM, 1.0, 0.0
    ).astype(BF)


def expand(values, selection):
    high = values.astype(BF)
    low = (values - high.astype(F32)).astype(BF)
    return mm(high, selection) + mm(low, selection)


def prepare(misc, info, row_ids, small_rows, bcu, bc, bt, ct, scores, pre, step, rate, cum, cum_t, enter, leave, factor):
    nt, rows_ext, width = misc.shape
    rows = rows_ext - HALO
    chunks = rows // Q
    bc_cols, heads = 2 * STATE // nt, HEADS // nt
    total = None
    for t in range(nt):
        part = mm(misc[t], select_columns(t, heads, bc_cols, width, 2 * STATE + 128))
        total = part if total is None else total + part
    marks = info[...]
    bc_ext = total[:, : 2 * STATE]
    u = conv_of(bc_ext, small_rows[0:CONV], small_rows[CONV : CONV + 1], marks)
    if bcu is not None:
        bcu[...] = bc_ext
    act = (u * sigmoid(u)).astype(BF)
    bc[...] = act
    before = total[HALO:, 2 * STATE :] + small_rows[CONV + 1 : CONV + 2, 0:128]
    steps = jnp.maximum(before, 0.0) + jnp.log1p(jnp.exp(-jnp.abs(before)))
    rates = -jnp.exp(small_rows[CONV + 2 : CONV + 3, 0:128]) * steps
    rates = jnp.where(iota(rates.shape, 1) < HEADS, rates, 0.0)
    if pre is not None:
        pre[...] = before
        rate[...] = rates
    step[...] = steps
    upper = iota((Q, Q), 0) >= iota((Q, Q), 1)
    lower = jnp.where(upper, 1.0, 0.0)
    for c in range(chunks):
        at = slice(c * Q, (c + 1) * Q)
        sums = mm(lower, rates[at], NN, HIGH)
        cum[at] = sums
        cum_t[c] = sums.T
        last = sums[Q - 1 : Q]
        enter[at] = jnp.exp(sums) * marks[at, 4:5]
        leave[at] = jnp.exp(last - sums) * marks[at, 5:6]
        factor[c : c + 1] = jnp.exp(last) * marks[c * Q : c * Q + 1, 7:8]
        bb, cc = act[at, :STATE], act[at, STATE:]
        within = upper & (marks[at, 3:4] == row_ids[0:1, at])
        scores[c] = jnp.where(within, mm(cc, bb, NT), 0.0)
        bt[c] = bb.T
        if ct is not None:
            ct[c] = cc.T


def decay_of(turned, cum_t, c, group, k):
    row = cum_t[c, pl.ds(group * GROUP_HEADS + k, 1), :]
    return jnp.exp(jnp.minimum(turned[:, k : k + 1] - row, 0.0))


def turned_sums(cum, at, group):
    return pltpu.roll(cum[at], (128 - group * GROUP_HEADS) % 128, 1)


def halves(pair):
    left = iota(pair.shape, 1) < HEAD_DIM
    zero = jnp.zeros_like(pair)
    return jnp.concatenate([jnp.where(left, pair, zero), jnp.where(left, zero, pair)], axis=0)


def ssd_kernel(x, misc, info, row_ids, wide_rows, small_rows, signal, y, state, ent, bc_out, bt, scores, step, cum, cum_t, enter, leave, factor):
    group = pl.program_id(0)
    rows = signal.shape[0]
    chunks = rows // Q

    @pl.when(group == 0)
    def _():
        factor[...] = jnp.zeros_like(factor)
        prepare(misc, info, row_ids, small_rows, None, bc_out, bt, None, scores, None, step, None, cum, cum_t, enter, leave, factor)
        base = jnp.zeros((1, 128), F32)
        for c in range(chunks):
            at = slice(c * Q, (c + 1) * Q)
            ent[at] = jnp.exp(cum[at] + base) * info[at, 6:7]
            base = base + cum[c * Q + Q - 1 : c * Q + Q]

    u = conv_of(x[...].astype(F32), wide_rows[0:CONV], wide_rows[CONV : CONV + 1], info[...])
    act = (u * sigmoid(u)).astype(BF)
    signal[...] = act
    pick = head_lanes(group, LANES)
    inputs = act.astype(F32) * expand(step[...], pick)
    inputs_b = inputs.astype(BF)
    weighted = (inputs * expand(leave[...], pick)).astype(BF)
    entering = expand(enter[...], pick)
    factors = expand(factor[...], pick)
    now = jnp.zeros((STATE, LANES), F32)
    whole = jnp.ones((1, LANES), F32)
    for c in range(chunks):
        at = slice(c * Q, (c + 1) * Q)
        turned = turned_sums(cum, at, group)
        pieces = []
        for p in range(LANES // 128):
            ma = (scores[c] * decay_of(turned, cum_t, c, group, 2 * p)).astype(BF)
            mb = (scores[c] * decay_of(turned, cum_t, c, group, 2 * p + 1)).astype(BF)
            pieces.append(mm(jnp.concatenate([ma, mb], axis=1), halves(inputs_b[at, p * 128 : p * 128 + 128])))
        result = jnp.concatenate(pieces, axis=1)
        if c:
            result = result + entering[at] * mm(bc_out[at, STATE:], now.astype(BF))
        y[at] = result.astype(BF)
        now = factors[c : c + 1] * now + mm(bt[c], weighted[at])
        whole = whole * factors[c : c + 1]
    state[0:STATE] = now.astype(BF)
    state[STATE:] = jnp.broadcast_to(whole, (16, LANES)).astype(BF)


def whole_spec(shape):
    return pl.BlockSpec(shape, lambda *_: (0,) * len(shape))


def column_spec(rows):
    return pl.BlockSpec((rows, LANES), lambda g: (0, g))


def ssd_forward(x_ext, misc, info, row_ids, wide_rows, small_rows):
    rows = x_ext.shape[0] - HALO
    chunks = rows // Q
    return pl.pallas_call(
        ssd_kernel,
        grid=(INNER // LANES,),
        in_specs=[
            column_spec(rows + HALO),
            whole_spec(misc.shape),
            whole_spec(info.shape),
            whole_spec(row_ids.shape),
            column_spec(8),
            whole_spec(small_rows.shape),
        ],
        out_specs=[
            column_spec(rows),
            column_spec(rows),
            column_spec(STATE + 16),
            whole_spec((rows, 128)),
            whole_spec((rows, 2 * STATE)),
        ],
        out_shape=[
            SDS((rows, INNER), BF),
            SDS((rows, INNER), BF),
            SDS((STATE + 16, INNER), BF),
            SDS((rows, 128), F32),
            SDS((rows, 2 * STATE), BF),
        ],
        scratch_shapes=[
            pltpu.VMEM((chunks, STATE, Q), BF),
            pltpu.VMEM((chunks, Q, Q), F32),
            pltpu.VMEM((rows, 128), F32),
            pltpu.VMEM((rows, 128), F32),
            pltpu.VMEM((chunks, 128, Q), F32),
            pltpu.VMEM((rows, 128), F32),
            pltpu.VMEM((rows, 128), F32),
            pltpu.VMEM((8, 128), F32),
        ],
        compiler_params=params(),
        cost_estimate=cost(20e9, 12e6),
        name="ssd_forward",
    )(x_ext, misc, info, row_ids, wide_rows, small_rows)


GATE_LANES = 1024


def gate_kernel(y, signal, gate, dno, bc, ent, incoming, wide_rows, pair, d_y, adjoint, sums, y_sum, gated_sum, acc):
    block = pl.program_id(0)
    rows = y.shape[0]
    width = GATE_LANES
    pieces = INNER // width

    @pl.when(block == 0)
    def _():
        acc[...] = jnp.zeros_like(acc)
        sums[...] = jnp.zeros_like(sums)

    cc = bc[:, STATE:]
    cc_t = cc.T
    ent_hi = ent[...].astype(BF)
    ent_lo = (ent[...] - ent_hi.astype(F32)).astype(BF)

    def lanes_of(i):
        pick = jnp.where(
            iota((128, width), 0) == i * (width // HEAD_DIM) + iota((128, width), 1) // HEAD_DIM, 1.0, 0.0
        ).astype(BF)
        return mm(ent_hi, pick) + mm(ent_lo, pick)

    def first(i, carry):
        squares, dots = carry
        at = pl.ds(pl.multiple_of(i * width, width), width)
        total = y[:, at].astype(F32) + wide_rows[CONV + 1 : CONV + 2, at] * signal[:, at].astype(F32)
        total = total + lanes_of(i) * mm(cc, incoming[0:STATE, at])
        z = gate[:, at].astype(F32)
        gated = total * (z * sigmoid(z))
        y_sum[:, at] = total
        gated_sum[:, at] = gated
        squares = squares + jnp.sum(gated * gated, axis=-1, keepdims=True)
        dots = dots + jnp.sum(dno[:, at].astype(F32) * wide_rows[CONV + 2 : CONV + 3, at] * gated, axis=-1, keepdims=True)
        return squares, dots

    zero = jnp.zeros((rows, 1), F32)
    squares, dots = lax.fori_loop(0, pieces, first, (zero, zero))
    inv = lax.rsqrt(squares / INNER + EPS)
    pull = inv * inv * inv * (dots / INNER)

    def second(i, carry):
        at = pl.ds(pl.multiple_of(i * width, width), width)
        total, gated = y_sum[:, at], gated_sum[:, at]
        z = gate[:, at].astype(F32)
        logistic = sigmoid(z)
        d_out = dno[:, at].astype(F32)
        scaled = gated * inv
        pair[1, :, at] = (scaled * wide_rows[CONV + 2 : CONV + 3, at]).astype(BF)
        d_gated = inv * (d_out * wide_rows[CONV + 2 : CONV + 3, at]) - gated * pull
        dy = d_gated * (z * logistic)
        d_y[:, at] = dy.astype(BF)
        pair[0, :, at] = (d_gated * total * logistic * (1.0 + z * (1.0 - logistic))).astype(BF)
        acc[:, at] += mm(cc_t, (dy * lanes_of(i)).astype(BF))
        sums[0:1, at] += jnp.sum(d_out * scaled, axis=0, keepdims=True)
        sums[1:2, at] += jnp.sum(dy * signal[:, at].astype(F32), axis=0, keepdims=True)
        return carry

    lax.fori_loop(0, pieces, second, 0)

    @pl.when(block == pl.num_programs(0) - 1)
    def _():
        adjoint[...] = acc[...].astype(BF)


def gate_norm(y, signal, gate, dno, bc, ent, incoming, wide_rows):
    rows = y.shape[0]
    size = min(rows, 256)
    row = lambda cols: pl.BlockSpec((size, cols), lambda i: (i, 0))
    return pl.pallas_call(
        gate_kernel,
        grid=(rows // size,),
        in_specs=[
            row(INNER), row(INNER), row(INNER), row(INNER), row(2 * STATE), row(128),
            whole_spec(incoming.shape), whole_spec(wide_rows.shape),
        ],
        out_specs=[
            pl.BlockSpec((2, size, INNER), lambda i: (0, i, 0)), row(INNER), whole_spec((STATE, INNER)), whole_spec((8, INNER)),
        ],
        out_shape=[
            SDS((2, rows, INNER), BF), SDS((rows, INNER), BF), SDS((STATE, INNER), BF), SDS((8, INNER), F32),
        ],
        scratch_shapes=[
            pltpu.VMEM((size, INNER), F32), pltpu.VMEM((size, INNER), F32), pltpu.VMEM((STATE, INNER), F32),
        ],
        compiler_params=params(),
        cost_estimate=cost(10e9, 25e6),
        name="gate_norm",
    )(y, signal, gate, dno, bc, ent, incoming, wide_rows)


def conv_back(du, ext, taps, info):
    grads = []
    zero = jnp.zeros((HALO, du.shape[1]), F32)
    back = None
    for k in range(CONV):
        part = du if k == 0 else du * info[:, k - 1 : k]
        moved = ext if k == 0 else pltpu.roll(ext, k, 0)
        grads.append(jnp.sum(part * moved[HALO:], axis=0, keepdims=True))
        term = jnp.concatenate([zero, part * taps[k : k + 1]], axis=0)
        if k:
            term = pltpu.roll(term, term.shape[0] - k, 0)
        back = term if back is None else back + term
    grads.append(jnp.sum(du, axis=0, keepdims=True))
    grads.append(jnp.zeros((3, du.shape[1]), F32))
    return back, jnp.concatenate(grads, axis=0)


def slope_of(u):
    logistic = sigmoid(u)
    return logistic * (1.0 + u * (1.0 - logistic))


def ssd_back_kernel(
    x, signal, dy, misc, info, row_ids, wide_rows, small_rows, incoming, after,
    dx, tail, rim, conv_grad, small, tail_bc, rim_bc, bc_grad, head_grad,
    bcu, bc, bt, ct, scores, pre, step, rate, cum, cum_t, enter, leave, factor,
    d_scores, d_b, d_c, d_direct, d_enter, d_leave, d_rows, d_cols, d_factor,
):
    group = pl.program_id(0)
    rows = signal.shape[0]
    chunks = rows // Q

    @pl.when(group == 0)
    def _():
        factor[...] = jnp.zeros_like(factor)
        prepare(misc, info, row_ids, small_rows, bcu, bc, bt, ct, scores, pre, step, rate, cum, cum_t, enter, leave, factor)
        for ref in (d_scores, d_b, d_c, d_direct, d_enter, d_leave, d_rows, d_cols, d_factor):
            ref[...] = jnp.zeros_like(ref)

    pick = head_lanes(group, LANES)
    gather = jnp.where(
        iota((LANES, 128), 1) == group * GROUP_HEADS + iota((LANES, 128), 0) // HEAD_DIM, 1.0, 0.0
    ).astype(BF)
    act = signal[...].astype(F32)
    steps = expand(step[...], pick)
    inputs = act * steps
    inputs_b = inputs.astype(BF)
    leaving = expand(leave[...], pick)
    weighted = inputs * leaving
    weighted_b = weighted.astype(BF)
    cot = dy[...].astype(F32)
    cot_in = cot * expand(enter[...], pick)
    cot_in_b = cot_in.astype(BF)
    factors = expand(factor[...], pick)
    now = incoming[0:STATE].astype(F32)
    states = []
    for c in range(chunks):
        at = slice(c * Q, (c + 1) * Q)
        states.append(now.astype(BF))
        if c < chunks - 1:
            now = factors[c : c + 1] * now + mm(bt[c], weighted_b[at])
    adj = after[0:STATE].astype(F32)
    lane = iota((Q, 128), 1)
    d_signal = [None] * chunks
    for c in reversed(range(chunks)):
        at = slice(c * Q, (c + 1) * Q)
        bb, cc = bc[at, :STATE], bc[at, STATE:]
        adj_b = adj.astype(BF)
        from_state = mm(cc, states[c])
        from_adj = mm(bb, adj_b)
        d_c[at] += mm(cot_in_b[at], states[c], NT)
        d_b[at] += mm(weighted_b[at], adj_b, NT)
        crossing = factors[c : c + 1] * jnp.sum(adj * states[c].astype(F32), axis=0, keepdims=True)
        d_factor[c] += mm(jnp.broadcast_to(crossing, (8, LANES)).astype(BF), gather)
        turned = turned_sums(cum, at, group)
        masked = scores[c]
        pieces = []
        score_sum = None
        row_sum = jnp.zeros((Q, 128), F32)
        for p in range(LANES // 128):
            lanes = slice(p * 128, p * 128 + 128)
            cots = halves(dy[at, lanes])
            d_pair = mm(cots, inputs_b[at, lanes], NT)
            both = []
            for j in range(2):
                k = 2 * p + j
                decays = decay_of(turned, cum_t, c, group, k)
                both.append((masked * decays).astype(BF))
                through = d_pair[j * Q : (j + 1) * Q] * decays
                score_sum = through if score_sum is None else score_sum + through
                product = through * masked
                row_sum = jnp.where(
                    lane == group * GROUP_HEADS + k, jnp.sum(product, axis=1, keepdims=True), row_sum
                )
                d_cols[c, pl.ds(group * GROUP_HEADS + k, 1), :] = jnp.sum(product, axis=0, keepdims=True)
            pieces.append(mm(jnp.concatenate(both, axis=0), cots, TN))
        d_scores[c] += score_sum
        d_rows[at] += row_sum
        d_inputs = jnp.concatenate(pieces, axis=1) + leaving[at] * from_adj
        d_direct[at] += mm((act[at] * d_inputs).astype(BF), gather)
        d_enter[at] += mm((cot_in[at] * from_state).astype(BF), gather)
        d_leave[at] += mm((weighted[at] * from_adj).astype(BF), gather)
        d_signal[c] = steps[at] * d_inputs + wide_rows[CONV + 1 : CONV + 2] * cot[at]
        if c:
            adj = factors[c : c + 1] * adj + mm(ct[c], cot_in_b[at])
    ext = x[...].astype(F32)
    du = jnp.concatenate(d_signal, axis=0) * slope_of(conv_of(ext, wide_rows[0:CONV], wide_rows[CONV : CONV + 1], info[...]))
    back, grads = conv_back(du, ext, wide_rows[0:CONV], info[...])
    dx[...] = back[HALO:].astype(BF)
    tail[...] = back[rows + HALO - 8 :]
    rim[...] = back[HALO - 8 : HALO]
    conv_grad[...] = grads

    @pl.when(group == pl.num_programs(0) - 1)
    def _():
        after_eq = jnp.where(iota((Q, Q), 1) >= iota((Q, Q), 0), 1.0, 0.0)
        before_ne = jnp.where(iota((Q, Q), 1) < iota((Q, Q), 0), 1.0, 0.0)
        grow = -jnp.exp(small_rows[CONV + 2 : CONV + 3, 0:128])
        dec_sum = jnp.zeros((1, 128), F32)
        bias_sum = jnp.zeros((1, 128), F32)
        valid = iota((Q, 128), 1) < HEADS
        parts = []
        for c in range(chunks):
            at = slice(c * Q, (c + 1) * Q)
            bb, cc = bc[at, :STATE], bc[at, STATE:]
            within = (iota((Q, Q), 0) >= iota((Q, Q), 1)) & (info[at, 3:4] == row_ids[0:1, at])
            ds = jnp.where(within, d_scores[c], 0.0).astype(BF)
            parts.append(jnp.concatenate([d_b[at] + mm(ds, cc, TN), d_c[at] + mm(ds, bb)], axis=1))
            d_rate = mm(after_eq, d_rows[at] + d_enter[at] - d_cols[c].T, NN, HIGH)
            d_rate = d_rate + mm(before_ne, d_leave[at], NN, HIGH) + d_factor[c][0:1]
            d_step = d_direct[at] + grow * d_rate
            d_pre = jnp.where(valid, d_step * sigmoid(pre[at]), 0.0)
            small[at, 2 * STATE :] = d_pre.astype(BF)
            bias_sum = bias_sum + jnp.sum(d_pre, axis=0, keepdims=True)
            dec_sum = dec_sum + jnp.sum(jnp.where(valid, d_rate * rate[at], 0.0), axis=0, keepdims=True)
        ext_bc = bcu[...]
        du_bc = jnp.concatenate(parts, axis=0)
        du_bc = du_bc * slope_of(conv_of(ext_bc, small_rows[0:CONV], small_rows[CONV : CONV + 1], info[...]))
        back_bc, grads_bc = conv_back(du_bc, ext_bc, small_rows[0:CONV], info[...])
        small[:, : 2 * STATE] = back_bc[HALO:].astype(BF)
        tail_bc[...] = back_bc[rows + HALO - 8 :]
        rim_bc[...] = back_bc[HALO - 8 : HALO]
        bc_grad[...] = grads_bc
        head_grad[...] = jnp.concatenate([bias_sum, dec_sum, jnp.zeros((6, 128), F32)], axis=0)


def ssd_backward(x_ext, signal, dy, misc, info, row_ids, wide_rows, small_rows, incoming, after):
    rows = signal.shape[0]
    chunks = rows // Q
    vm = pltpu.VMEM
    return pl.pallas_call(
        ssd_back_kernel,
        grid=(INNER // LANES,),
        in_specs=[
            column_spec(rows + HALO),
            column_spec(rows),
            column_spec(rows),
            whole_spec(misc.shape),
            whole_spec(info.shape),
            whole_spec(row_ids.shape),
            column_spec(8),
            whole_spec(small_rows.shape),
            column_spec(incoming.shape[0]),
            column_spec(after.shape[0]),
        ],
        out_specs=[
            column_spec(rows),
            column_spec(8),
            column_spec(8),
            column_spec(8),
            whole_spec((rows, 2 * STATE + 128)),
            whole_spec((8, 2 * STATE)),
            whole_spec((8, 2 * STATE)),
            whole_spec((8, 2 * STATE)),
            whole_spec((8, 128)),
        ],
        out_shape=[
            SDS((rows, INNER), BF),
            SDS((8, INNER), F32),
            SDS((8, INNER), F32),
            SDS((8, INNER), F32),
            SDS((rows, 2 * STATE + 128), BF),
            SDS((8, 2 * STATE), F32),
            SDS((8, 2 * STATE), F32),
            SDS((8, 2 * STATE), F32),
            SDS((8, 128), F32),
        ],
        scratch_shapes=[
            vm((rows + HALO, 2 * STATE), F32),
            vm((rows, 2 * STATE), BF),
            vm((chunks, STATE, Q), BF),
            vm((chunks, STATE, Q), BF),
            vm((chunks, Q, Q), F32),
            vm((rows, 128), F32),
            vm((rows, 128), F32),
            vm((rows, 128), F32),
            vm((rows, 128), F32),
            vm((chunks, 128, Q), F32),
            vm((rows, 128), F32),
            vm((rows, 128), F32),
            vm((8, 128), F32),
            vm((chunks, Q, Q), F32),
            vm((rows, 128), F32),
            vm((rows, 128), F32),
            vm((rows, 128), F32),
            vm((rows, 128), F32),
            vm((rows, 128), F32),
            vm((rows, 128), F32),
            vm((chunks, 128, Q), F32),
            vm((chunks, 8, 128), F32),
        ],
        compiler_params=params(),
        cost_estimate=cost(40e9, 15e6),
        name="ssd_backward",
    )(x_ext, signal, dy, misc, info, row_ids, wide_rows, small_rows, incoming, after)


def slot_of(piece, order):
    slot = 0
    for j, bit in enumerate(order[1:], 2):
        slot = slot + (((piece >> bit) & 1) << (len(order) - j))
    return slot


def weight_grad_body(where, own_z, next_z, own_o, next_o, own, other, *outs, cols, top):
    kind, piece = pl.program_id(0), pl.program_id(1)
    keep_a, send_a, keep_b, send_b = outs
    half = keep_a.shape[3]
    per = half // cols
    nt = 2 * per
    block = INNER // nt
    mine = jnp.where(kind == 0, own_z[0], own_o[0])
    theirs = jnp.where(kind == 0, next_z[0], next_o[0])
    parts = []
    for turn in range(nt):
        t = jnp.bitwise_xor(where[1], turn)
        at = pl.ds(pl.multiple_of(t * block, block), block)
        parts.append((mm(mine, own[0, :, at]) + mm(theirs, other[0, :, at])).astype(BF))
    for keep, send, order, chosen in (
        (keep_a, send_a, list(range(top + 1)), parts[:per]),
        (keep_b, send_b, list(range(top, -1, -1)), parts[per:]),
    ):
        slot = slot_of(piece, order)
        away = (piece >> order[0]) & 1

        @pl.when(away == 0)
        def _(keep=keep, slot=slot, chosen=chosen):
            for i, value in enumerate(chosen):
                keep[0, slot, :, i * cols : (i + 1) * cols] = value

        @pl.when(away == 1)
        def _(send=send, slot=slot, chosen=chosen):
            for i, value in enumerate(chosen):
                send[0, slot, :, i * cols : (i + 1) * cols] = value


def weight_grad(where, lefts, own, other, nt, cols):
    nw, k, rows = lefts[0].shape
    nm = nw // 2
    half = nt // 2 * cols
    left = pl.BlockSpec((1, k, rows), lambda q, r, s: (2 * jnp.bitwise_xor(r, s[0]) + s[2], 0, 0))
    right = pl.BlockSpec((1, rows, INNER), lambda q, r, s: (q, 0, 0))
    out = pl.BlockSpec((1, nm // 2, k, half), lambda q, r, s: (q, 0, 0, 0))
    return pl.pallas_call(
        functools.partial(weight_grad_body, cols=cols, top=nm.bit_length() - 2),
        grid_spec=pltpu.PrefetchScalarGridSpec(
            num_scalar_prefetch=1,
            grid=(2, nm),
            in_specs=[left] * 4 + [right] * 2,
            out_specs=[out] * 4,
        ),
        out_shape=[SDS((2, nm // 2, k, half), BF)] * 4,
        compiler_params=params(),
        cost_estimate=cost(8 * nm * k * rows * INNER, 12 * nm * k * INNER),
    )(where, *lefts, own, other)


def out_kernel(left, weight, tokens, out, acc):
    t = pl.program_id(0)
    depth = out.shape[1]
    part = mm(left[0], weight[...].reshape(depth, weight.shape[3]), NT)

    @pl.when(t == 0)
    def _():
        acc[...] = tokens[...].astype(F32) + part

    @pl.when(t > 0)
    def _():
        acc[...] += part

    @pl.when(t == pl.num_programs(0) - 1)
    def _():
        out[...] = acc[...].astype(BF)


def out_project(left, weights, which, tokens):
    rows, depth = tokens.shape
    nw, nt, k, _ = weights.shape
    block = INNER // nt
    return pl.pallas_call(
        out_kernel,
        grid=(nt,),
        in_specs=[
            pl.BlockSpec((1, rows, block), lambda t: (1, 0, t)),
            pl.BlockSpec((nw, 1, k, block), lambda t: (0, t, 0, which)),
            whole_spec(tokens.shape),
        ],
        out_specs=whole_spec(tokens.shape),
        out_shape=SDS(tokens.shape, BF),
        scratch_shapes=[pltpu.VMEM((rows, depth), F32)],
        compiler_params=params(),
        cost_estimate=cost(2 * rows * depth * INNER, 2 * depth * INNER),
        name="out_project",
    )(left, weights, tokens)


def gate_part_kernel(left, weight, out):
    t = pl.program_id(0)
    depth = out.shape[1]
    part = mm(left[0], weight[...].reshape(depth, weight.shape[3]), NT)

    @pl.when(t == 0)
    def _():
        out[...] = part

    @pl.when(t > 0)
    def _():
        out[...] += part


def gate_part(left, weights, which, depth):
    rows = left.shape[1]
    nw, nt, k, _ = weights.shape
    block = INNER // nt
    return pl.pallas_call(
        gate_part_kernel,
        grid=(nt,),
        in_specs=[
            pl.BlockSpec((1, rows, block), lambda t: (0, 0, t)),
            pl.BlockSpec((nw, 1, k, block), lambda t: (0, t, 0, which)),
        ],
        out_specs=whole_spec((rows, depth)),
        out_shape=SDS((rows, depth), F32),
        compiler_params=params(),
        cost_estimate=cost(2 * rows * depth * INNER, 2 * depth * INNER),
        name="gate_part",
    )(left, weights)


MESH = pl.DeviceIdType.MESH
SPLIT = 4
RATE = 2
LAG = 2


def remote(src, dst, send, recv, peer):
    return pltpu.make_async_remote_copy(src, dst, send, recv, device_id=peer, device_id_type=MESH)


def greet(peers):
    barrier = pltpu.get_barrier_semaphore()
    for peer in peers:
        pl.semaphore_signal(barrier, inc=1, device_id=peer, device_id_type=MESH)
    pl.semaphore_wait(barrier, len(peers))


class Line:
    def __init__(self, own, slot, send, recv, count):
        self.own, self.slot, self.send, self.recv, self.count = own, slot, send, recv, count
        self.t = lax.axis_index("tp")

    def each(self, distance, leaving, act):
        t, last = self.t, self.count - 1
        for way, sign in ((0, 1), (1, -1)):
            origin = t - sign * distance
            ahead = t + sign
            fine = (origin >= 0) & (origin <= last)
            if leaving:
                fine = fine & (ahead >= 0) & (ahead <= last)
            step = distance + 1 if leaving else distance

            @pl.when(fine)
            def _(origin=origin, ahead=ahead, way=way, step=step):
                there = self.slot(jnp.clip(origin, 0, last))
                source = self.own if leaving and distance == 0 else there
                act(
                    remote(source, there, self.send.at[way, step], self.recv.at[way, step], {"tp": jnp.clip(ahead, 0, last)})
                )

    def start(self, distance):
        self.each(distance, True, lambda copy: copy.start())

    def arrive(self, distance):
        self.each(distance, False, lambda copy: copy.wait_recv())

    def finish(self):
        for distance in range(self.count - 1):
            self.each(distance, True, lambda copy: copy.wait_send())


def gather_kernel(own, z_own, o_own, whole, z_line, o_line, send_x, recv_x, send_z, recv_z, send_o, recv_o, send_p, recv_p, send_c, recv_c, local):
    nw, nt = whole.shape[0], whole.shape[1]
    k = own.shape[0]
    w, t = lax.axis_index("wide"), lax.axis_index("tp")
    bits = nw.bit_length() - 2
    rows = k // SPLIT
    half = nt // 2
    greet(
        [{"tp": lax.rem(t + 1, nt)}, {"tp": lax.rem(t + nt - 1, nt)}]
        + [{"wide": jnp.bitwise_xor(w, 1 << b)} for b in range(bits + 1)]
    )
    part = lambda s: pl.ds(s * rows, rows)
    mine = []
    for s in range(SPLIT):
        mine.append(pltpu.make_async_copy(own.at[part(s)], whole.at[w, t, part(s)], local.at[0, s]))
        mine.append(pltpu.make_async_copy(z_own.at[part(s)], z_line.at[t, part(s)], local.at[1, s]))
        mine.append(pltpu.make_async_copy(o_own.at[part(s)], o_line.at[t, part(s)], local.at[2, s]))
    first = [Line(own.at[part(s)], lambda o, s=s: whole.at[w, o, part(s)], send_x.at[s], recv_x.at[s], nt) for s in range(SPLIT)]
    later = [Line(z_own.at[part(s)], lambda o, s=s: z_line.at[o, part(s)], send_z.at[s], recv_z.at[s], nt) for s in range(SPLIT)]
    later += [Line(o_own.at[part(s)], lambda o, s=s: o_line.at[o, part(s)], send_o.at[s], recv_o.at[s], nt) for s in range(SPLIT)]
    for line in first:
        line.start(0)
    for copy in mine:
        copy.start()
    sent, crossing, have, coming = [], [], {}, {}

    def exchange(index, h, s, mask, send, recv):
        at = (pl.ds(h * half, half), part(s))
        peer = {"wide": jnp.bitwise_xor(w, mask)}
        ref = whole.at[(index,) + at]
        copy = remote(ref, ref, send, recv, peer)
        copy.start()
        sent.append(copy)
        other = whole.at[(jnp.bitwise_xor(index, mask),) + at]
        return remote(other, other, send, recv, peer)

    def cross(index, h, s, number):
        crossing.append(exchange(index, h, s, 1, send_c.at[s, h, number], recv_c.at[s, h, number]))

    def begin(s, p):
        for h in range(2):
            mask = 2 << (p if h == 0 else bits - 1 - p)
            coming[s, p, h] = []
            for n, index in enumerate(list(have[s, h])):
                slot = (1 << p) - 1 + n
                copy = exchange(index, h, s, mask, send_p.at[s, h, slot], recv_p.at[s, h, slot])
                coming[s, p, h].append((jnp.bitwise_xor(index, mask), copy))

    hops = nt - 1
    pending = len(later)
    for tick in range(max(SPLIT + hops - 1 + bits, (pending + RATE - 1) // RATE + hops + LAG)):
        for d in range(hops, 0, -1):
            s = tick - d + 1
            if 0 <= s < SPLIT:
                first[s].arrive(d)
                if d < hops:
                    first[s].start(d)
        s = tick - hops + 1
        if 0 <= s < SPLIT:
            mine[3 * s].wait()
            for h in range(2):
                have[s, h] = [w]
            begin(s, 0)
            for h in range(2):
                cross(w, h, s, 0)
        for p in range(bits):
            s = tick - hops - p
            if 0 <= s < SPLIT:
                for h in range(2):
                    for index, copy in coming[s, p, h]:
                        copy.wait_recv()
                        have[s, h].append(index)
                if p + 1 < bits:
                    begin(s, p + 1)
                for h in range(2):
                    for n in range(1 << p):
                        cross(coming[s, p, h][n][0], h, s, (1 << p) + n)
        for d in range(hops, -1, -1):
            for n in range(RATE * (tick - LAG - d), RATE * (tick - LAG - d + 1)):
                if 0 <= n < pending:
                    if d:
                        later[n].arrive(d)
                    if d < hops:
                        later[n].start(d)
    for copy in crossing:
        copy.wait_recv()
    for s in range(SPLIT):
        mine[3 * s + 1].wait()
        mine[3 * s + 2].wait()
    for line in first + later:
        line.finish()
    for copy in sent:
        copy.wait_send()


def gather(own, z_own, o_own, nw, nt):
    k, cols = own.shape
    nm = nw // 2
    dma = pltpu.SemaphoreType.DMA
    return pl.pallas_call(
        gather_kernel,
        in_specs=[pl.BlockSpec(memory_space=pltpu.VMEM)] * 3,
        out_specs=[pl.BlockSpec(memory_space=pl.ANY)] * 3,
        out_shape=[SDS((nw, nt, k, cols), BF), SDS((nt,) + z_own.shape, BF), SDS((nt,) + o_own.shape, BF)],
        scratch_shapes=[dma((SPLIT, 2, nt))] * 6 + [dma((SPLIT, 2, nm))] * 4 + [dma((3, SPLIT))],
        compiler_params=params(32, collective_id=0, has_side_effects=True),
        cost_estimate=cost(60e9, 1e6),
        name="gather",
    )(own, z_own, o_own)


def span_shifts(span):
    reach = (DOC_MAX - 2) // span + 1
    size, steps = 1, []
    while 2 * size < reach:
        steps.append(size)
        size *= 2
    return steps, (1 + size if size < reach else 0)


STATE_PARTS = 4
EARLY = 1


def join(near, far):
    decay = near[STATE : STATE + 1].astype(F32)
    state = near[:STATE].astype(F32) + decay * far[:STATE].astype(F32)
    whole = near[STATE:].astype(F32) * far[STATE:].astype(F32)
    return jnp.concatenate([state, whole], axis=0).astype(BF)


class Passing:
    def __init__(self, source, target, send, recv, steps):
        nt = lax.axis_size("tp")
        count = lax.axis_size("wide") * nt
        place = lax.axis_index("wide") * nt + lax.axis_index("tp")
        ahead = place + steps
        behind = place - steps
        self.sends = (ahead < count) & (ahead >= 0)
        self.gets = (behind < count) & (behind >= 0)
        to = jnp.clip(ahead, 0, count - 1)
        self.peer = {"wide": to // nt, "tp": lax.rem(to, nt)}
        self.source, self.target, self.send, self.recv = source, target, send, recv

    def copy(self, j):
        width = INNER // STATE_PARTS
        at = pl.ds(j * width, width)
        return remote(self.source.at[:, at], self.target.at[:, at], self.send.at[j], self.recv.at[j], self.peer)

    def clear(self):
        @pl.when(jnp.logical_not(self.gets))
        def _():
            self.target[...] = jnp.zeros_like(self.target)

    def start(self, j):
        @pl.when(self.sends)
        def _():
            self.copy(j).start()

    def arrive(self, j):
        @pl.when(self.gets)
        def _():
            self.copy(j).wait_recv()

    def finish(self):
        @pl.when(self.sends)
        def _():
            for j in range(STATE_PARTS):
                self.copy(j).wait_send()


def shift_peers(shifts):
    nt = lax.axis_size("tp")
    count = lax.axis_size("wide") * nt
    place = lax.axis_index("wide") * nt + lax.axis_index("tp")
    peers = []
    for steps in shifts:
        for sign in (1, -1):
            to = lax.rem(place + count + sign * steps, count)
            peers.append({"wide": to // nt, "tp": lax.rem(to, nt)})
    return peers


def spread_kernel(state, z_line, z_first, o_line, o_first, incoming, z_whole, o_whole, *scratch, span):
    steps, far_step = span_shifts(span)
    levels = len(steps) + 1 + (1 if far_step else 0)
    buffers, scratch = scratch[:levels], scratch[levels:]
    helds, scratch = scratch[: len(steps)], scratch[len(steps) :]
    send_s, recv_s, send_p, recv_p, send_c, recv_c, local = scratch
    nw, nt = z_whole.shape[0], z_whole.shape[1]
    w = lax.axis_index("wide")
    bits = nw.bit_length() - 2
    shifts = sorted(set(steps) | {1} | ({far_step} if far_step else set()))
    width = INNER // STATE_PARTS

    def columns(j):
        return slice(j * width, (j + 1) * width)

    sources = [state] + list(helds)
    passes = [Passing(sources[i], buffers[i], send_s.at[i], recv_s.at[i], steps[i]) for i in range(len(steps))]
    last = sources[len(steps)]
    near = Passing(last, buffers[len(steps)], send_s.at[len(steps)], recv_s.at[len(steps)], 1)
    ends = [near]
    if far_step:
        ends.append(Passing(last, buffers[len(steps) + 1], send_s.at[len(steps) + 1], recv_s.at[len(steps) + 1], far_step))
    for item in passes + ends:
        item.clear()
    greet(shift_peers(shifts) + [{"wide": jnp.bitwise_xor(w, 1 << b)} for b in range(bits + 1)])
    for j in range(STATE_PARTS):
        (passes + ends)[0].start(j)
    if not passes and far_step:
        for j in range(STATE_PARTS):
            ends[1].start(j)

    sent, copies, crossing = [], [], []
    kinds = ((z_line, z_first, z_whole, [2 << p for p in range(bits)]), (o_line, o_first, o_whole, [2 << (bits - 1 - p) for p in range(bits)]))

    def exchange(source, whole, index, c, mask, send, recv):
        peer = {"wide": jnp.bitwise_xor(w, mask)}
        copy = remote(source, whole.at[index, c], send, recv, peer)
        copy.start()
        sent.append(copy)
        other = whole.at[jnp.bitwise_xor(index, mask), c]
        return remote(other, other, send, recv, peer)

    waiting = {}
    for kind, (line, first, whole, masks) in enumerate(kinds):
        waiting[kind] = {c: [(w, line.at[c]), (jnp.bitwise_xor(w, masks[0]), first.at[c])] for c in range(nt)}
    rounds = {}

    def begin(kind, p, c):
        whole, masks = kinds[kind][2], kinds[kind][3]
        rounds[kind, p, c] = [
            (jnp.bitwise_xor(index, masks[p]), exchange(source, whole, index, c, masks[p], send_p.at[kind, c, (1 << p) - 2 + n], recv_p.at[kind, c, (1 << p) - 2 + n]))
            for n, (index, source) in enumerate(waiting[kind][c])
        ]

    def cross(kind, index, source, c, number):
        crossing.append(exchange(source, kinds[kind][2], index, c, 1, send_c.at[kind, c, number], recv_c.at[kind, c, number]))

    def begin_some(some):
        for c in some:
            for kind in range(2):
                if bits > 1:
                    begin(kind, 1, c)

    begin_some(range(EARLY))
    for c in range(nt):
        for kind in range(2):
            for n, (index, source) in enumerate(waiting[kind][c]):
                copy = pltpu.make_async_copy(source, kinds[kind][2].at[index, c], local.at[kind, c, n])
                copy.start()
                copies.append(copy)
                cross(kind, index, source, c, n)
    for i, item in enumerate(passes):
        for j in range(STATE_PARTS):
            item.arrive(j)
            helds[i][:, columns(j)] = join(sources[i][:, columns(j)], buffers[i][:, columns(j)])
        following = passes[i + 1 : i + 2] or ends
        for j in range(STATE_PARTS):
            for other in following:
                other.start(j)
    begin_some(range(EARLY, nt))
    for p in range(1, bits):
        for c in range(nt):
            for kind in range(2):
                for n, (index, copy) in enumerate(rounds[kind, p, c]):
                    copy.wait_recv()
                    source = kinds[kind][2].at[index, c]
                    waiting[kind][c].append((index, source))
                    cross(kind, index, source, c, (1 << p) + n)
                if p + 1 < bits:
                    begin(kind, p + 1, c)
    for j in range(STATE_PARTS):
        for item in ends:
            item.arrive(j)
        value = buffers[len(steps)][:, columns(j)]
        if far_step:
            value = join(value, buffers[len(steps) + 1][:, columns(j)])
        incoming[:, columns(j)] = value
    for copy in crossing:
        copy.wait_recv()
    for copy in copies:
        copy.wait()
    for item in passes + ends:
        item.finish()
    for copy in sent:
        copy.wait_send()


def spread(state, z_line, z_first, o_line, o_first, nw, span):
    nt, k, cols = z_line.shape
    nm = nw // 2
    steps, far_step = span_shifts(span)
    levels = len(steps) + 1 + (1 if far_step else 0)
    dma = pltpu.SemaphoreType.DMA
    vmem, anywhere = pl.BlockSpec(memory_space=pltpu.VMEM), pl.BlockSpec(memory_space=pl.ANY)
    return pl.pallas_call(
        functools.partial(spread_kernel, span=span),
        in_specs=[vmem] * 5,
        out_specs=[vmem, anywhere, anywhere],
        out_shape=[SDS(state.shape, BF), SDS((nw, nt, k, cols), BF), SDS((nw, nt, k, cols), BF)],
        scratch_shapes=[pltpu.VMEM(state.shape, BF)] * (levels + len(steps))
        + [dma((levels, STATE_PARTS))] * 2
        + [dma((2, nt, max(nm - 2, 1)))] * 2
        + [dma((2, nt, nm))] * 2
        + [dma((2, nt, 2))],
        compiler_params=params(48, collective_id=1, has_side_effects=True),
        cost_estimate=cost(60e9, 1e6),
        name="spread",
    )(state, z_line, z_first, o_line, o_first)


ROW_PARTS = 2
STEP_LAG = 4
SUM_GAP = 2


class Unit:
    def __init__(self, order, first, keep, kept, sends, recvs, send_sem, recv_sem, done):
        self.order, self.first, self.keep, self.kept, self.sends, self.recvs = order, first, keep, kept, sends, recvs
        self.send_sem, self.recv_sem, self.done = send_sem, recv_sem, done

    def copy(self, p):
        peer = {"wide": jnp.bitwise_xor(lax.axis_index("wide"), 2 << self.order[p])}
        return remote(self.sends[p], self.recvs[p], self.send_sem.at[p], self.recv_sem.at[p], peer)

    def merge(self, p):
        self.copy(p).wait_recv()
        keep = self.keep if p == self.first else self.kept
        count = self.recvs[p].shape[0]
        if p == len(self.order) - 1:
            self.done(keep[0].astype(F32) + self.recvs[p][0].astype(F32))
            return
        for i in range(count // 2):
            self.kept[i] = keep[i].astype(F32) + self.recvs[p][i].astype(F32)
        for i in range(count // 2, count):
            self.sends[p + 1][i - count // 2] = (keep[i].astype(F32) + self.recvs[p][i].astype(F32)).astype(BF)


def finish_kernel(
    dx, small, tail, tail_bc, rim, rim_bc, left, left_next, keep_a, send_a, keep_b, send_b, wx, so_far, tokens, cot, gain, conv_grad, gate_sums, bc_grad, head_grad,
    x_out, bc_out, dt_out, z_out, o_out, grad, sums_out, gain_out,
    dxs, dxn, smalls, smalln, rims, rims_bc, extra, weights,
    keep_x, send_x, recv_x, turn_x, own_x, got_x, kept_zo, send_zo, recv_zo, turn_zo, own_zo, got_zo, sums_to, sums_from, gain_to, gain_from,
    sem_flip, sem_rim, sem_local, sem_xs, sem_xr, sem_zs, sem_zr, sem_txs, sem_txr, sem_tzs, sem_tzr, sem_ss, sem_sr, sem_gs, sem_gr,
):
    nw, nt, k, cols = wx.shape
    rows, depth = tokens.shape
    block = INNER // nt
    nm = nw // 2
    bits = nm.bit_length() - 1
    per = nt // 2
    w, rank = lax.axis_index("wide"), lax.axis_index("tp")
    chip, core = w // 2, lax.rem(w, 2)
    count = nw * nt
    place = w * nt + rank
    before, behind = lax.rem(place + count - 1, count), lax.rem(place + 1, count)
    sibling = {"wide": jnp.bitwise_xor(w, 1)}
    tp_bits = nt.bit_length() - 1
    across = [{"tp": jnp.bitwise_xor(rank, 1 << b)} for b in range(tp_bits)]
    has_next = place < count - 1
    has_last = place > 0
    to_last = {"wide": before // nt, "tp": lax.rem(before, nt)}
    to_next = {"wide": behind // nt, "tp": lax.rem(behind, nt)}
    orders = (list(range(bits)), list(range(bits - 1, -1, -1)))

    @pl.when(jnp.logical_not(has_next))
    def _():
        rims[...] = jnp.zeros_like(rims)
        rims_bc[...] = jnp.zeros_like(rims_bc)

    greet([sibling, to_last, to_next] + across + [{"wide": jnp.bitwise_xor(w, 2 << b)} for b in range(bits)])
    rim_copies = [
        remote(rim, rims, sem_rim.at[0], sem_rim.at[1], to_last),
        remote(rim_bc, rims_bc, sem_rim.at[2], sem_rim.at[3], to_last),
    ]

    @pl.when(has_last)
    def _():
        for copy in rim_copies:
            copy.start()

    started = []

    def start(copy):
        copy.start()
        started.append(copy)

    body = pl.ds(0, rows - HALO)
    flips, locals_ = [], []
    order_of_turns = [turn for pair in zip(range(per - 1, -1, -1), range(nt - 1, per - 1, -1)) for turn in pair]
    small_copy = remote(small.at[body], smalln.at[body], sem_flip.at[0, 0], sem_flip.at[1, 0], sibling)
    start(small_copy)
    own_small = pltpu.make_async_copy(small, smalls, sem_local.at[nt])
    own_small.start()
    for n, turn in enumerate(order_of_turns):
        at = pl.ds(pl.multiple_of(jnp.bitwise_xor(rank, turn) * block, block), block)
        flips.append(remote(dx.at[body, at], dxn.at[body, at], sem_flip.at[0, 1 + n], sem_flip.at[1, 1 + n], sibling))
        start(flips[n])
        locals_.append(pltpu.make_async_copy(dx.at[:, at], dxs.at[:, at], sem_local.at[n]))
        locals_[n].start()
    initial = pltpu.make_async_copy(so_far, grad, sem_local.at[nt + 1])
    initial.start()

    def weight_copy(t):
        return pltpu.make_async_copy(wx.at[:, t], weights.at[t % 2], sem_local.at[nt + 2 + t % 2])

    weight_copy(0).start()

    def level(turn):
        return (turn & -turn).bit_length() - 1

    def finished(total, turn, own, leaving):
        if turn % 2:
            leaving[turn] = total.astype(BF)
        else:
            own[turn // 2] = total

    units_zo = []
    for q in range(2):
        for h, (keep, send) in enumerate(((keep_a, send_a), (keep_b, send_b))):
            def done(total, q=q, h=h):
                for i in range(per):
                    finished(total[:, i * block : (i + 1) * block], h * per + i, own_zo.at[q], turn_zo.at[q])

            number = 2 * q + h
            sends = {p: (send.at[q] if p == 1 else send_zo.at[number, pl.ds(0, nm >> (p + 1))]) for p in range(1, bits)}
            recvs = {p: recv_zo.at[number, pl.ds((nm >> 1) - (nm >> p), nm >> (p + 1))] for p in range(1, bits)}
            units_zo.append(
                Unit(orders[h], 1, keep.at[q], kept_zo.at[number], sends, recvs, sem_zs.at[number], sem_zr.at[number], done)
            )
    for unit in units_zo:
        start(unit.copy(1))

    part = k // ROW_PARTS
    units_x = []
    for s in range(ROW_PARTS):
        for turn in order_of_turns:
            number = len(units_x)

            def done(total, turn=turn, s=s):
                at = pl.ds(s * part, part)
                finished(total, turn, own_x.at[:, at], turn_x.at[:, at])

            sends = {p: send_x.at[number, pl.ds(nm - (nm >> p), nm >> (p + 1))] for p in range(bits)}
            recvs = {p: recv_x.at[number, pl.ds(nm - (nm >> p), nm >> (p + 1))] for p in range(bits)}
            unit = Unit(
                orders[0 if turn < per else 1], 0, keep_x.at[number], keep_x.at[number], sends, recvs, sem_xs.at[number], sem_xr.at[number], done
            )
            unit.turn, unit.s = turn, s
            units_x.append(unit)

    for copy in locals_:
        copy.wait()
    own_small.wait()

    @pl.when(has_next)
    def _():
        for copy in rim_copies:
            copy.wait_recv()

    last = slice(rows - HALO, rows)
    old = dxs[last].astype(F32)
    dxs[last] = jnp.concatenate([old[: HALO - 8], tail[...] + rims[...]], axis=0).astype(BF)
    old = smalls[last].astype(F32)
    fixed = jnp.concatenate([old[: HALO - 8, : 2 * STATE], tail_bc[...] + rims_bc[...]], axis=0)
    smalls[last] = jnp.concatenate([fixed, old[:, 2 * STATE :]], axis=1).astype(BF)

    end = pl.ds(rows - HALO, HALO)
    ends = [
        remote(smalls.at[end], smalln.at[end], sem_flip.at[0, nt + 1], sem_flip.at[1, nt + 1], sibling),
        remote(dxs.at[end], dxn.at[end], sem_flip.at[0, nt + 2], sem_flip.at[1, nt + 2], sibling),
    ]

    def members(order):
        found = []
        for index in range(nm // 2):
            r = 0
            for j, bit in enumerate(order[1:], 2):
                r |= ((index >> (len(order) - j)) & 1) << bit
            found.append(r)
        return found

    def compute(unit):
        order = unit.order
        kept = members(order)
        away = [r | (1 << order[0]) for r in kept]
        t = jnp.bitwise_xor(rank, unit.turn)
        at = pl.ds(pl.multiple_of(t * block, block), block)
        at_rows = pl.ds(unit.s * part, part)
        chips = [jnp.bitwise_xor(chip, r) for r in away + kept]
        places = [2 * m + core for m in chips]
        mine = jnp.concatenate([left[m, at_rows, :] for m in places], axis=0)
        theirs = jnp.concatenate([left_next[m, at_rows, :] for m in places], axis=0)
        result = mm(mine, dxs[:, at]) + mm(theirs, dxn[:, at])
        pick = select_columns(t, HEADS // nt, 2 * STATE // nt, cols - block, 2 * STATE + 128)
        picked = mm(jnp.concatenate([extra[m, at_rows, :] for m in chips], axis=0), pick, NT)
        value = jnp.concatenate([result, picked], axis=1)
        for i in range(nm // 2):
            unit.sends[0][i] = value[i * part : (i + 1) * part].astype(BF)
            unit.keep[i] = value[(nm // 2 + i) * part : (nm // 2 + i + 1) * part]

    def row_part(t):
        weight_copy(t).wait()
        if t + 1 < nt:
            weight_copy(t + 1).start()
        if t == 0:
            initial.wait()
        pick = select_columns(t, HEADS // nt, 2 * STATE // nt, cols - block, 2 * STATE + 128)
        extra_columns = mm(smalls[...], pick, NT).astype(BF)
        values = jnp.concatenate([dxs[:, t * block : (t + 1) * block], extra_columns], axis=1)
        grad[...] += mm(values, weights[t % 2].reshape(depth, cols), NT)

    def row_end():
        raw = tokens[...].astype(F32)
        inv = lax.rsqrt(jnp.mean(raw * raw, axis=-1, keepdims=True) + EPS)
        unit = raw * inv
        d_normed = grad[...]
        gain_grad = jnp.sum(d_normed * unit, axis=0, keepdims=True)
        gain_to[0] = gain_grad
        d_unit = d_normed * gain[...]
        grad[...] = cot[...].astype(F32) + inv * (d_unit - unit * jnp.mean(d_unit * unit, axis=-1, keepdims=True))

    partners = [{"wide": jnp.bitwise_xor(w, 1 << b)} for b in range(bits + 1)]
    partners += across

    def sum_start():
        sums_to[0, 0:5] = conv_grad[0:5]
        sums_to[0, 5:7] = gate_sums[0:2]
        for i in range(CONV + 1):
            sums_to[0, 7:8, i * 2 * STATE : (i + 1) * 2 * STATE] = bc_grad[i : i + 1]
        at = (CONV + 1) * 2 * STATE
        for i in range(2):
            sums_to[0, 7:8, at + i * 128 : at + (i + 1) * 128] = head_grad[i : i + 1]
        sums_to[0, 7:8, at + 256 :] = jnp.zeros((1, INNER - at - 256), F32)

    def butterfly(to, source, out, send, recv):
        def copy(i):
            return remote(to.at[i], source.at[i], send.at[i], recv.at[i], partners[i])

        def join(i):
            copy(i).wait_recv()
            total = to[i] + source[i]
            if i + 1 < len(partners):
                to[i + 1] = total
            else:
                out[...] = total

        return copy, join

    flies = [butterfly(sums_to, sums_from, sums_out, sem_ss, sem_sr), butterfly(gain_to, gain_from, gain_out, sem_gs, sem_gr)]

    def parcels(unit):
        if unit in units_zo:
            number = units_zo.index(unit)
            q, h = number // 2, number % 2
            for turn in range((h + 1) * per - 1, h * per - 1, -1):
                yield turn, own_zo.at[q], turn_zo.at[q], got_zo.at[q], sem_tzs.at[q], sem_tzr.at[q]
        else:
            at = pl.ds(unit.s * part, part)
            yield unit.turn, own_x.at[:, at], turn_x.at[:, at], got_x.at[:, :, at], sem_txs.at[unit.s], sem_txr.at[unit.s]

    def joined(turn, own, got, send, recv, upto):
        total = own[turn // 2]
        for b in range(upto):
            source = got.at[turn // 2, b]
            remote(source, source, send.at[turn], recv.at[turn // 2, b], across[b]).wait_recv()
            total = total + source[...].astype(F32)
        return total

    def pass_on(unit, odd):
        found = []
        for turn, own, leaving, got, send, recv in parcels(unit):
            if turn == 0 or bool(turn % 2) != odd:
                continue
            b = level(turn)
            if b:
                leaving[turn] = joined(turn, own, got, send, recv, b).astype(BF)
            target = turn ^ (1 << b)
            found.append(remote(leaving.at[turn], got.at[target // 2, b], send.at[turn], recv.at[target // 2, b], across[b]))
        return found

    side = [functools.partial(row_part, t) for t in range(nt)] + [row_end]
    total_x = len(units_x)
    steps = total_x + STEP_LAG * bits
    first_job = 1
    fly_steps = [
        [1 + SUM_GAP * i for i in range(len(partners) + 1)],
        [first_job + len(side) + i for i in range(len(partners) + 1)],
    ]
    steps = max(steps, fly_steps[0][-1], fly_steps[1][-1])
    later = {step: [] for step in range(steps + 2)}
    for step in range(steps + 1):
        ready = []
        leaving_now = [copy for unit in later[step] for copy in pass_on(unit, False)]
        if step < total_x:
            if step == 0:
                for copy in ends:
                    start(copy)
                small_copy.wait_recv()
                for copy in ends:
                    copy.wait_recv()
                small_all = [smalls[...], smalln[...]]
                for m in range(nm):
                    extra[m] = (mm(left[2 * m + core], small_all[0]) + mm(left_next[2 * m + core], small_all[1])).astype(BF)
            if step < len(flips):
                flips[step].wait_recv()
            compute(units_x[step])
        for p in range(bits - 1, -1, -1):
            u = step - STEP_LAG * (p + 1)
            if 0 <= u < total_x:
                units_x[u].merge(p)
                ready.append((units_x[u], p + 1))
        for p in range(bits - 1, 0, -1):
            u = step - 1 - STEP_LAG * (p - 1)
            if 0 <= u < len(units_zo):
                units_zo[u].merge(p)
                ready.append((units_zo[u], p + 1))
        if step == 0:
            sum_start()
        job = step - first_job
        if 0 <= job < len(side):
            side[job]()
        leaving_sums = []
        for (copy, join), when in zip(flies, fly_steps):
            if step in when:
                i = when.index(step)
                if i:
                    join(i - 1)
                if i < len(partners):
                    leaving_sums.append(copy(i))
        if step < total_x:
            start(units_x[step].copy(0))
        for unit, p in ready:
            if p < bits:
                start(unit.copy(p))
            else:
                for copy in pass_on(unit, True):
                    start(copy)
                later[step + 1].append(unit)
        for copy in leaving_now:
            start(copy)
        for copy in leaving_sums:
            start(copy)
    zo_total = []
    for q in range(2):
        unit = units_zo[2 * q]
        for turn, own, leaving, got, send, recv in parcels(unit):
            if turn == 0:
                zo_total.append(joined(0, own, got, send, recv, tp_bits))
    z_out[...] = zo_total[0]
    o_out[...] = zo_total[1].T
    for unit in units_x:
        for turn, own, leaving, got, send, recv in parcels(unit):
            if turn == 0:
                total = joined(0, own, got, send, recv, tp_bits)
                at = slice(unit.s * part, (unit.s + 1) * part)
                x_out[at] = total[:, :block]
                bc_out[at] = total[:, block : block + bc_out.shape[1]]
                dt_out[at] = total[:, block + bc_out.shape[1] : block + bc_out.shape[1] + dt_out.shape[1]]
    for copy in started:
        copy.wait_send()

    @pl.when(has_last)
    def _():
        for copy in rim_copies:
            copy.wait_send()


def finish(dx, small, tail, tail_bc, rim, rim_bc, left, left_next, keep_a, send_a, keep_b, send_b, wx, so_far, tokens, cot, gain, conv_grad, gate_sums, bc_grad, head_grad):
    nw, nt, k, cols = wx.shape
    rows, depth = tokens.shape
    nm = nw // 2
    bits = nm.bit_length() - 1
    block = INNER // nt
    half = nt // 2 * block
    part = k // ROW_PARTS
    units = ROW_PARTS * nt
    tp_bits = nt.bit_length() - 1
    partners = bits + 1 + tp_bits
    dma, vm = pltpu.SemaphoreType.DMA, pltpu.VMEM
    vmem, anywhere = pl.BlockSpec(memory_space=pltpu.VMEM), pl.BlockSpec(memory_space=pl.ANY)
    return pl.pallas_call(
        finish_kernel,
        in_specs=[anywhere, anywhere] + [vmem] * 6 + [vmem] * 4 + [anywhere, anywhere] + [vmem] * 7,
        out_specs=[vmem] * 8,
        out_shape=[
            SDS((k, block), F32), SDS((k, 2 * STATE // nt), F32), SDS((k, HEADS // nt), F32),
            SDS((k, block), F32), SDS((block, k), F32), SDS((rows, depth), F32), SDS((8, INNER), F32), SDS((1, depth), F32),
        ],
        scratch_shapes=[
            vm((rows, INNER), BF), vm((rows, INNER), BF), vm(small.shape, BF), vm(small.shape, BF),
            vm((8, INNER), F32), vm((8, 2 * STATE), F32), vm((nm, k, small.shape[1]), BF), vm((2, nw, k, cols), BF),
            vm((units, nm // 2, part, cols), F32), vm((units, nm - 1, part, cols), BF), vm((units, nm - 1, part, cols), BF),
            vm((nt, k, cols), BF), vm((nt // 2, k, cols), F32), vm((nt // 2, tp_bits, k, cols), BF),
            vm((4, nm // 4, k, half) if bits > 2 else (4, 1, 8, 128), F32),
            vm((4, nm // 8, k, half) if bits > 2 else (4, 1, 16, 128), BF),
            vm((4, max(nm // 2 - 1, 1), k, half), BF),
            vm((2, nt, k, block), BF), vm((2, nt // 2, k, block), F32), vm((2, nt // 2, tp_bits, k, block), BF),
            vm((partners, 8, INNER), F32), vm((partners, 8, INNER), F32), vm((partners, 1, depth), F32), vm((partners, 1, depth), F32),
            dma((2, nt + 3)), dma((4,)), dma((nt + 4,)),
            dma((units, bits)), dma((units, bits)), dma((4, bits)), dma((4, bits)),
            dma((ROW_PARTS, nt)), dma((ROW_PARTS, nt // 2, tp_bits)), dma((2, nt)), dma((2, nt // 2, tp_bits)),
            dma((partners,)), dma((partners,)), dma((partners,)), dma((partners,)),
        ],
        compiler_params=params(63, collective_id=2, has_side_effects=True),
        cost_estimate=cost(60e9, 1e6),
        name="finish",
    )(dx, small, tail, tail_bc, rim, rim_bc, left, left_next, keep_a, send_a, keep_b, send_b, wx, so_far, tokens, cot, gain, conv_grad, gate_sums, bc_grad, head_grad)


BOTH = ("wide", "tp")


def shift(value, steps):
    count = lax.axis_size("wide") * lax.axis_size("tp")
    first, last = max(0, -steps), min(count, count - steps)
    return lax.ppermute(value, BOTH, [(i, i + steps) for i in range(first, last)])


def carry_states(own, span, direction):
    reach = (DOC_MAX - 2) // span + 1
    held, size = own, 1
    while 2 * size < reach:
        other = shift(held, direction * size)
        held = combine(held, other)
        size *= 2
    near = shift(held, direction)
    if size >= reach:
        return near
    far = shift(held, direction * (1 + size))
    return combine(near, far)


def combine(near, far):
    decay = near[STATE : STATE + 1].astype(F32)
    state = near[:STATE].astype(F32) + decay * far[:STATE].astype(F32)
    whole = near[STATE:].astype(F32) * far[STATE:].astype(F32)
    return jnp.concatenate([state, whole], axis=0).astype(BF)


def flip(value, mask):
    return lax.ppermute(value, "wide", [(i, i ^ mask) for i in range(lax.axis_size("wide"))])


def add(a, b):
    return (a.astype(F32) + b.astype(F32)).astype(BF)


def first_exchange(keep_a, send_a, keep_b, send_b):
    top = keep_a.shape[1].bit_length() - 1
    size = keep_a.shape[1] // 2
    got_a, got_b = flip(send_a, 2), flip(send_b, 2 << top)
    result = []
    for keep, got in ((keep_a, got_a), (keep_b, got_b)):
        result += [add(keep[:, :size], got[:, :size]), add(keep[:, size:], got[:, size:])]
    return result


def per_device(
    tokens, segment_ids, out_cotangent, norm_gain, z_weight, x_weight, bc_weight, dt_weight, x_conv, x_bias,
    bc_conv, bc_bias, dt_bias, decay_log, skip_gain, gate_gain, out_weight,
):
    nw, nt = lax.axis_size("wide"), lax.axis_size("tp")
    rank = lax.axis_index("tp")
    rows, depth = tokens.shape
    k = depth // nw
    block = INNER // nt
    small = jnp.concatenate([bc_weight, dt_weight], axis=1)
    small = jnp.pad(small, ((0, 0), (0, 128 - small.shape[1])))
    own_x = jnp.concatenate([x_weight, small], axis=1)
    wx, z_line, o_line = gather(own_x, z_weight, out_weight.T, nw, nt)
    z_first, o_first = flip(z_line, 2), flip(o_line, nw // 2)

    own_ids = lax.dynamic_slice_in_dim(segment_ids, rank * rows, rows, 0)
    last_ids = jnp.pad((own_ids[rows - 128 :] + 1).astype(BF)[None, :], ((0, HALO - 1), (0, depth - 128)))
    halo_rows = shift(jnp.concatenate([tokens[rows - HALO :], last_ids], axis=0), 1)
    row_ids = jnp.broadcast_to(own_ids.astype(F32)[None, :], (8, rows))

    def padded(v, width):
        v = v if v.ndim == 2 else v[None, :]
        return jnp.pad(v, ((0, 0), (0, width - v.shape[1])))

    wide_rows = jnp.concatenate(
        [x_conv, x_bias[None, :], jnp.repeat(skip_gain, HEAD_DIM)[None, :], gate_gain[None, :], x_bias[None, :]], axis=0
    ).astype(F32)
    small_rows = jnp.concatenate(
        [bc_conv, bc_bias[None, :], padded(dt_bias, 2 * STATE), padded(decay_log, 2 * STATE), bc_bias[None, :]], axis=0
    ).astype(F32)
    in_gain = norm_gain.astype(F32)[None, :]

    x_ext, misc, normed_ext, normed_t, info = project(tokens, halo_rows, in_gain, row_ids, wx)
    signal, y, own_state, ent, bc = ssd_forward(
        x_ext, misc, info, row_ids, wide_rows, small_rows
    )
    incoming, wz, wo = spread(own_state, z_line, z_first, o_line, o_first, nw, rows)
    core = lax.rem(lax.axis_index("wide"), 2)
    where = jnp.stack([lax.axis_index("wide") // 2, rank, core]).astype(jnp.int32)
    normed_next = flip(normed_t, 1).reshape(nw, k, rows)
    (gate,) = plain(normed_ext, wz, HALO, False)
    dno, cot_t = plain(out_cotangent, wo, 0, True)
    cot_next = flip(cot_t, 1).reshape(nw, k, rows)
    left = [normed_t.reshape(nw, k, rows), normed_next, cot_t.reshape(nw, k, rows), cot_next]
    pair, dy, adjoint, sums = gate_norm(y, signal, gate, dno, bc, ent, incoming, wide_rows)
    own_adjoint = jnp.concatenate([adjoint, own_state[STATE:]], axis=0)
    after = carry_states(own_adjoint, rows, -1)
    pair_next = flip(pair, 1)
    block_out = out_project(pair, wo, 0, tokens)
    so_far = gate_part(pair, wz, 0, depth)
    zo = weight_grad(where, left, pair, pair_next, nt, block)
    zo = first_exchange(*zo)
    dx, tail, rim, conv_grad, small_grad, tail_bc, rim_bc, bc_grad, head_grad = ssd_backward(
        x_ext, signal, dy, misc, info, row_ids, wide_rows, small_rows, incoming, after
    )
    x_weight_grad, bc_weight_grad, dt_weight_grad, z_weight_grad, out_weight_grad, grad_x, small_sums, gain_sum = finish(
        dx, small_grad, tail, tail_bc, rim, rim_bc, left[0], left[1], *zo, wx, so_far, tokens, out_cotangent, in_gain,
        conv_grad, sums, bc_grad, head_grad,
    )
    wide_bc = (CONV + 1) * 2 * STATE
    bc_all = small_sums[7, :wide_bc].reshape(CONV + 1, 2 * STATE)
    head_all = small_sums[7, wide_bc : wide_bc + 256]
    return (
        block_out,
        grad_x,
        gain_sum[0],
        z_weight_grad,
        x_weight_grad,
        bc_weight_grad,
        dt_weight_grad,
        small_sums[:CONV],
        small_sums[CONV],
        bc_all[:CONV],
        bc_all[CONV],
        head_all[:HEADS],
        head_all[128 : 128 + HEADS],
        small_sums[6].reshape(HEADS, HEAD_DIM).sum(axis=1),
        small_sums[5],
        out_weight_grad,
    )


def solution(mesh):
    rows, shard, out_shard = P(("wide", "tp"), None), P("wide", "tp"), P("tp", "wide")
    return jax.shard_map(
        per_device,
        mesh=mesh,
        in_specs=(rows, P("wide"), rows, P(), shard, shard, shard, shard) + (P(),) * 8 + (out_shard,),
        out_specs=(rows, rows, P(), shard, shard, shard, shard) + (P(),) * 8 + (out_shard,),
        check_vma=False,
    )
```
